32 devices in a mesh: lat: 4 (over z), dom: 2 (over y), ens: 4 (over x, core).
Axes of the slice: x: 2, y: 2, z: 4, core: 2. Of those that a mesh axis runs over, the one named last changes fastest.
Arguments:
- ens_state: bfloat16 [256, 32, 1024, 32], P('ens', 'lat', 'dom')
- w_in: bfloat16 [64, 128], replicated
- w_out: bfloat16 [128, 32], replicated
- obs_op: bfloat16 [32, 16], replicated
- obs_val: float32 [32, 4, 256, 16], P('lat', 'dom')
- obs_wt: float32 [32, 4, 256, 16], P('lat', 'dom')
Outputs:
- output: bfloat16 [256, 32, 1024, 32], P('ens', 'lat', 'dom')
All inputs are finite; a program needn't handle non-finite values.
Results may differ from the reference program's by a relative error of at most 0.001.
Values are sent between devices in bfloat16 or wider.
A program may use at most 1 GiB of HBM per device.

```python
import jax
import jax.numpy as jnp
from jax import lax

MEMBERS = 256
CHANNELS = 32
HIDDEN = 128
OBS_CHAN = 16
PATCH_LEN = 256
GRID_ROWS = 32
GRID_COLS = 1024
NS_STEPS = 12
TOP_PRECISION = lax.Precision.HIGHEST


def setup_inputs(seed: int = 0) -> dict:
    key_list = jax.random.split(jax.random.key(seed), 7)
    patch_count = GRID_COLS // PATCH_LEN
    mean_field = jax.random.normal(key_list[0], (GRID_ROWS, GRID_COLS, CHANNELS), jnp.float32)
    member_dev = 0.3 * jax.random.normal(key_list[1], (MEMBERS, GRID_ROWS, GRID_COLS, CHANNELS), jnp.float32)
    ens_state = (mean_field[None] + member_dev).astype(jnp.bfloat16)
    w_in = (jax.random.normal(key_list[2], (2 * CHANNELS, HIDDEN), jnp.float32) * (2 * CHANNELS) ** -0.5).astype(jnp.bfloat16)
    w_out = (jax.random.normal(key_list[3], (HIDDEN, CHANNELS), jnp.float32) * (0.5 * HIDDEN ** -0.5)).astype(jnp.bfloat16)
    obs_op = (jax.random.normal(key_list[4], (CHANNELS, OBS_CHAN), jnp.float32) * CHANNELS ** -0.5).astype(jnp.bfloat16)
    obs_shape = (GRID_ROWS, patch_count, PATCH_LEN, OBS_CHAN)
    obs_val = 1.5 * jax.random.normal(key_list[5], obs_shape, jnp.float32)
    obs_wt = jax.random.uniform(key_list[6], obs_shape, jnp.float32, 0.25, 1.75) * (MEMBERS / (PATCH_LEN * OBS_CHAN))
    return {'ens_state': ens_state, 'w_in': w_in, 'w_out': w_out, 'obs_op': obs_op, 'obs_val': obs_val, 'obs_wt': obs_wt}


def forecast_member(member, w_in, w_out):
    x_f32 = member.astype(jnp.float32)
    row_above = jnp.concatenate([x_f32[:1], x_f32[:-1]], axis=0)
    row_below = jnp.concatenate([x_f32[1:], x_f32[-1:]], axis=0)
    col_west = jnp.roll(x_f32, 1, axis=1)
    col_east = jnp.roll(x_f32, -1, axis=1)
    laplace = (row_above + row_below + col_west + col_east - 4.0 * x_f32).astype(jnp.bfloat16)
    features = jnp.concatenate([member, laplace], axis=-1).reshape(GRID_ROWS * GRID_COLS, 2 * CHANNELS)
    pre_act = jnp.dot(features, w_in, preferred_element_type=jnp.float32)
    hidden = jax.nn.gelu(pre_act, approximate=False).astype(jnp.bfloat16)
    update = jnp.dot(hidden, w_out, preferred_element_type=jnp.float32)
    return (x_f32 + update.reshape(GRID_ROWS, GRID_COLS, CHANNELS)).astype(jnp.bfloat16)


def inverse_root(a_mat):
    eye_mat = jnp.eye(MEMBERS, dtype=jnp.float32)
    scale_f = jnp.sqrt(jnp.sum(a_mat * a_mat, axis=(-2, -1), keepdims=True))

    def step_fn(carry, step_in):
        y_mat, z_mat = carry
        t_mat = 1.5 * eye_mat - 0.5 * jnp.einsum('nij,njk->nik', z_mat, y_mat, precision=TOP_PRECISION)
        y_next = jnp.einsum('nij,njk->nik', y_mat, t_mat, precision=TOP_PRECISION)
        z_next = jnp.einsum('nij,njk->nik', t_mat, z_mat, precision=TOP_PRECISION)
        return (y_next, z_next), None

    z_init = jnp.broadcast_to(eye_mat, a_mat.shape)
    final_pair, step_out = lax.scan(step_fn, (a_mat / scale_f, z_init), None, length=NS_STEPS)
    return final_pair[1] / jnp.sqrt(scale_f)


def analyse_row(xf_row, obs_row, wt_row, obs_op):
    n_patch = GRID_COLS // PATCH_LEN
    obs_width = PATCH_LEN * OBS_CHAN
    xf_pts = xf_row.astype(jnp.float32).reshape(MEMBERS, n_patch, PATCH_LEN, CHANNELS)
    x_mean = jnp.mean(xf_pts, axis=0)
    x_anom = xf_pts - x_mean
    y_back = jnp.einsum('enbc,co->enbo', xf_pts, obs_op.astype(jnp.float32), precision=TOP_PRECISION)
    y_mean = jnp.mean(y_back, axis=0)
    y_anom = (y_back - y_mean).reshape(MEMBERS, n_patch, obs_width)
    c_mat = y_anom * wt_row.reshape(n_patch, obs_width)
    a_mat = jnp.einsum('enq,fnq->nef', c_mat, y_anom, precision=TOP_PRECISION) + (MEMBERS - 1) * jnp.eye(MEMBERS, dtype=jnp.float32)
    s_mat = inverse_root(a_mat)
    pa_mat = jnp.einsum('nij,njk->nik', s_mat, s_mat, precision=TOP_PRECISION)
    innovation = obs_row.reshape(n_patch, obs_width) - y_mean.reshape(n_patch, obs_width)
    c_innov = jnp.einsum('enq,nq->ne', c_mat, innovation, precision=TOP_PRECISION)
    w_mean = jnp.einsum('nef,nf->ne', pa_mat, c_innov, precision=TOP_PRECISION)
    t_mat = (MEMBERS - 1) ** 0.5 * s_mat + w_mean[:, :, None]
    x_anal = x_mean + jnp.einsum('knbc,nke->enbc', x_anom, t_mat, precision=TOP_PRECISION)
    return x_anal.reshape(MEMBERS, GRID_COLS, CHANNELS).astype(jnp.bfloat16)


def reference(ens_state, w_in, w_out, obs_op, obs_val, obs_wt):
    forecast = lax.map(lambda member: forecast_member(member, w_in, w_out), ens_state)
    by_row = jnp.swapaxes(forecast, 0, 1)
    analysed = lax.map(lambda row_args: analyse_row(row_args[0], row_args[1], row_args[2], obs_op), (by_row, obs_val, obs_wt))
    return jnp.swapaxes(analysed, 0, 1)
```

```python
import functools
import math

import jax
import jax.numpy as jnp
import numpy as np
from jax import lax
from jax.experimental import pallas as pl
from jax.experimental.pallas import tpu as pltpu
from jax.sharding import PartitionSpec as P

NS_STEPS = 12
MESH = pl.DeviceIdType.MESH
F32 = jnp.float32
BF16 = jnp.bfloat16
MEMBERS = 256
MINE = 64
ROWS = 8
COLS = 512
CHANS = 32
PATCH = 256
OBS = 16
CHUNKS = 4
OWNERS = 4
GROUP = 16
SUBS = MINE // GROUP
STAGE = CHUNKS * OWNERS


def split3(value):
    high = value.astype(BF16)
    rest = value - high.astype(F32)
    mid = rest.astype(BF16)
    low = (rest - mid.astype(F32)).astype(BF16)
    return high, mid, low


def dot(a, b):
    return jnp.dot(a, b, preferred_element_type=F32)


def dot_t(a, b):
    return lax.dot_general(a, b, (((1,), (1,)), ((), ())), preferred_element_type=F32)


def dot6(a, b):
    small = dot(a[2][...], b[0][...]) + dot(a[0][...], b[2][...]) + dot(a[1][...], b[1][...])
    return small + dot(a[1][...], b[0][...]) + dot(a[0][...], b[1][...]) + dot(a[0][...], b[0][...])


def chunk_row(chunk, which):
    last = chunk // (CHUNKS - 1)
    return (1 - last) * (1 + 2 * chunk + which) + last * (ROWS - 1) * which


def kernel(lat_count, dom_count, w1_ref, w2_ref, bd_ref, perm_ref, yo_ref, wt_ref, x_ref, out_ref,
           buf, xbuf, edge_out, edge_in, work, am, pm, zm, cif, sy, sz, st, xbar, ybar, sw_ref, sd_ref,
           x_sem, halo_send, halo_recv, halo_local, edge_send, edge_recv, f_send, f_recv, r_send, r_recv, own_sem):
    me = lax.axis_index('ens')
    lat = lax.axis_index('lat')
    dom = lax.axis_index('dom')
    my_row = me // 2
    my_half = me % 2
    lat_up = (lat + lat_count - 1) % lat_count
    lat_down = (lat + 1) % lat_count
    dom_other = (dom + 1) % dom_count

    row_copies = [pltpu.make_async_copy(x_ref.at[:, r], xbuf.at[r + 1], x_sem.at[r]) for r in range(ROWS)]
    for r in range(ROWS):
        row_copies[r].start()

    barrier = pltpu.get_barrier_semaphore()
    for t in range(1, OWNERS):
        pl.semaphore_signal(barrier, inc=1, device_id={'ens': (me + t) % OWNERS}, device_id_type=MESH)
    pl.semaphore_signal(barrier, inc=1, device_id={'lat': lat_up}, device_id_type=MESH)
    pl.semaphore_signal(barrier, inc=1, device_id={'lat': lat_down}, device_id_type=MESH)
    pl.semaphore_signal(barrier, inc=1, device_id={'dom': dom_other}, device_id_type=MESH)
    pl.semaphore_wait(barrier, OWNERS + 2)

    send_up = pltpu.make_async_remote_copy(x_ref.at[:, 0], xbuf.at[ROWS + 1], halo_send.at[0], halo_recv.at[1],
                                           device_id={'lat': lat_up}, device_id_type=MESH)
    send_down = pltpu.make_async_remote_copy(x_ref.at[:, ROWS - 1], xbuf.at[0], halo_send.at[1], halo_recv.at[0],
                                             device_id={'lat': lat_down}, device_id_type=MESH)
    top_copy = pltpu.make_async_copy(x_ref.at[:, 0], xbuf.at[0], halo_local.at[0])
    bottom_copy = pltpu.make_async_copy(x_ref.at[:, ROWS - 1], xbuf.at[ROWS + 1], halo_local.at[1])

    @pl.when(lat > 0)
    def _():
        send_up.start()

    @pl.when(lat < lat_count - 1)
    def _():
        send_down.start()

    @pl.when(lat == 0)
    def _():
        top_copy.start()

    @pl.when(lat == lat_count - 1)
    def _():
        bottom_copy.start()

    lane = lax.broadcasted_iota(jnp.int32, (CHANS, 128), 1)

    def edge_copy(chunk):
        return pltpu.make_async_remote_copy(edge_out.at[chunk], edge_in.at[chunk], edge_send.at[chunk], edge_recv.at[chunk],
                                            device_id={'dom': dom_other}, device_id_type=MESH)

    def pack(chunk, carry):
        def member(m, acc):
            first, last = acc
            for which in range(2):
                row = chunk_row(chunk, which) + 1
                spot = lane == which * MINE + m
                west = xbuf[row, m, :, 0:128].astype(F32)
                east = xbuf[row, m, :, COLS - 128:COLS].astype(F32)
                first = jnp.where(spot, west[:, 0:1], first)
                last = jnp.where(spot, east[:, 127:128], last)
            return first, last

        zero = jnp.zeros((CHANS, 128), F32)
        first, last = lax.fori_loop(0, MINE, member, (zero, zero))
        edge_out[chunk, 0] = first.astype(BF16)
        edge_out[chunk, 1] = last.astype(BF16)
        edge_copy(chunk).start()
        return carry

    for r in range(4):
        row_copies[r].wait()
    pack(0, 0)
    for r in range(4, ROWS):
        row_copies[r].wait()
    lax.fori_loop(1, CHUNKS, pack, 0)

    def f_copy(chunk, t, start, size):
        owner = (me + t) % OWNERS
        return pltpu.make_async_remote_copy(
            buf.at[STAGE + 3 * chunk + t - 1, pl.ds(start, size)], buf.at[OWNERS * chunk + me, pl.ds(start, size)],
            f_send.at[chunk, t - 1], f_recv.at[chunk, me], device_id={'ens': owner}, device_id_type=MESH)

    def forecast_chunk(chunk, carry):
        edge_copy(chunk).wait_recv()

        @pl.when((chunk == CHUNKS - 1) & (lat > 0))
        def _():
            send_down.wait_recv()

        @pl.when((chunk == CHUNKS - 1) & (lat == 0))
        def _():
            top_copy.wait()

        @pl.when((chunk == CHUNKS - 1) & (lat < lat_count - 1))
        def _():
            send_up.wait_recv()

        @pl.when((chunk == CHUNKS - 1) & (lat == lat_count - 1))
        def _():
            bottom_copy.wait()

        slots = []
        for owner in range(OWNERS):
            ahead = (owner - me + OWNERS) % OWNERS
            own = 1 - (ahead + OWNERS - 1) // OWNERS
            slots.append(own * (OWNERS * chunk + me) + (1 - own) * (STAGE + 3 * chunk + ahead - 1))

        def member(m, carry):
            from_east = edge_in[chunk, 0].astype(F32)
            from_west = edge_in[chunk, 1].astype(F32)
            for which in range(2):
                row = chunk_row(chunk, which) + 1
                spot = which * MINE + m
                halo_west = pltpu.roll(from_west, (128 - spot) % 128, 1)
                halo_east = pltpu.roll(from_east, 127 - spot, 1)
                here = xbuf[row, m]
                mid = here.astype(F32)
                above = xbuf[row - 1, m].astype(F32)
                below = xbuf[row + 1, m].astype(F32)
                west = pltpu.roll(mid, 1, 1)
                east = pltpu.roll(mid, COLS - 1, 1)
                west = jnp.concatenate([jnp.where(lane == 0, halo_west, west[:, :128]), west[:, 128:]], axis=1)
                east = jnp.concatenate([east[:, :COLS - 128], jnp.where(lane == 127, halo_east, east[:, COLS - 128:])], axis=1)
                laplace = (above + below + west + east - 4.0 * mid).astype(BF16)
                for half in range(2):
                    span = slice(half * PATCH, (half + 1) * PATCH)
                    features = jnp.concatenate([here[:, span], laplace[:, span]], axis=0)
                    pre_act = dot(w1_ref[...], features)
                    hidden = (0.5 * pre_act * (1.0 + lax.erf(pre_act * math.sqrt(0.5)))).astype(BF16)
                    update = dot(w2_ref[...], hidden)
                    buf[slots[2 * which + half], m] = (mid[:, span] + update).astype(BF16)
            return carry

        def sub(index, carry):
            start = index * GROUP
            lax.fori_loop(start, start + GROUP, member, 0)
            for t in (2, 1, 3):
                f_copy(chunk, t, start, GROUP).start()
            return carry

        lax.fori_loop(0, SUBS, sub, 0)
        return carry

    lax.fori_loop(0, CHUNKS, forecast_chunk, 0)

    def r_place(chunk, owner):
        return out_ref.at[:, chunk_row(chunk, owner // 2), :, pl.ds(pl.multiple_of((owner % 2) * PATCH, PATCH), PATCH)]

    def r_stage(chunk, target):
        return xbuf.at[2 * chunk + target // 2, :, :, (target % 2) * PATCH:(target % 2 + 1) * PATCH]

    def r_copy(chunk, target):
        return pltpu.make_async_remote_copy(
            r_stage(chunk, target), r_place(chunk, me), r_send.at[chunk, target], r_recv.at[chunk, me],
            device_id={'ens': target}, device_id_type=MESH)

    def own_copy(chunk, target):
        return pltpu.make_async_copy(r_stage(chunk, target), r_place(chunk, me), own_sem.at[chunk])

    row_id = lax.broadcasted_iota(jnp.int32, (MEMBERS, MEMBERS), 0)
    col_id = lax.broadcasted_iota(jnp.int32, (MEMBERS, MEMBERS), 1)

    def analyse(chunk, carry):
        for t in range(1, OWNERS):
            source = (me + t) % OWNERS
            pltpu.make_async_remote_copy(
                buf.at[STAGE], buf.at[OWNERS * chunk + source], f_send.at[chunk, 0], f_recv.at[chunk, source],
                device_id={'ens': source}, device_id_type=MESH).wait_recv()
        row = chunk_row(chunk, my_row)

        def block(group):
            return buf[OWNERS * chunk + group // SUBS, pl.ds((group % SUBS) * GROUP, GROUP)]

        def sums(group, acc):
            x_sum, y_sum = acc
            states = block(group)
            x_sum = x_sum + jnp.sum(states.astype(F32), axis=0)
            for part in range(2):
                y_sum = y_sum + dot(bd_ref[...], states[part * 8:part * 8 + 8].reshape(8 * CHANS, PATCH))
            return x_sum, y_sum

        x_sum, y_sum = lax.fori_loop(0, MEMBERS // GROUP, sums,
                                     (jnp.zeros((CHANS, PATCH), F32), jnp.zeros((8 * OBS, PATCH), F32)))
        xbar[...] = x_sum * (1.0 / MEMBERS)
        y_mean = jnp.sum(y_sum.reshape(OBS, 8, PATCH), axis=1) * (1.0 / MEMBERS)
        ybar[...] = y_mean
        root_wt = jnp.sqrt(wt_ref[row, my_half])
        sw_ref[...] = root_wt
        sd_ref[...] = root_wt * (yo_ref[row, my_half] - y_mean)

        def anomalies(group, carry):
            states = block(group)
            y_parts = [dot(bd_ref[...], states[part * 8:part * 8 + 8].reshape(8 * CHANS, PATCH)) for part in range(2)]
            spot = pl.ds(pl.multiple_of(group * GROUP, GROUP), GROUP)
            c_innov = jnp.zeros((GROUP, PATCH), F32)
            for o in range(OBS):
                y = jnp.concatenate([y_parts[0][o * 8:o * 8 + 8], y_parts[1][o * 8:o * 8 + 8]], axis=0)
                scaled = (y - ybar[o:o + 1]) * sw_ref[o:o + 1]
                c_innov = c_innov + scaled * sd_ref[o:o + 1]
                high, mid, low = split3(scaled)
                work[o, spot] = high
                work[OBS + o, spot] = mid
                work[2 * OBS + o, spot] = low
            cif[spot] = c_innov
            return carry

        lax.fori_loop(0, MEMBERS // GROUP, anomalies, 0)

        am[...] = jnp.zeros((MEMBERS, MEMBERS), F32)
        pm[...] = jnp.zeros((MEMBERS, MEMBERS), F32)

        def gram(o, carry):
            high = work[o]
            mid = work[OBS + o]
            pm[...] += dot_t(high, mid) + dot_t(high, work[2 * OBS + o])
            am[...] += dot_t(mid, mid) + dot_t(high, high)
            return carry

        lax.fori_loop(0, OBS, gram, 0)
        eye = jnp.where(row_id == col_id, 1.0, 0.0).astype(F32)
        cross = pm[...]
        a_mat = (MEMBERS - 1) * eye + (am[...] + (cross + cross.T))
        scale = jnp.sqrt(jnp.sum(jnp.sum(a_mat * a_mat, axis=0, keepdims=True), axis=1, keepdims=True))

        def put(refs, value):
            for index, part in enumerate(split3(value)):
                refs[index] = part

        def parts(refs):
            return [refs.at[index] for index in range(3)]

        put(sy, a_mat / scale)
        put(sz, eye)

        def newton(step, carry):
            unit = jnp.where(row_id == col_id, 1.5, 0.0).astype(F32)
            put(st, unit - 0.5 * dot6(parts(sz), parts(sy)))
            put(sy, dot6(parts(sy), parts(st)))
            z_next = dot6(parts(st), parts(sz))
            zm[...] = z_next
            put(sz, z_next)
            return carry

        lax.fori_loop(0, NS_STEPS, newton, 0)
        s_mat = zm[...] / jnp.sqrt(scale)
        zm[...] = s_mat
        put(sz, s_mat)
        pa_mat = dot6(parts(sz), parts(sz))
        c_innov = jnp.sum(cif[...], axis=1, keepdims=True)
        w_mean = jnp.sum(pa_mat * c_innov, axis=0, keepdims=True)
        t_mat = math.sqrt(MEMBERS - 1) * zm[...] + w_mean
        put(st, t_mat)
        rest = 1.0 - jnp.sum(t_mat, axis=1, keepdims=True)

        def by_channel(group, carry):
            spot = pl.ds(pl.multiple_of(group * GROUP, GROUP), GROUP)
            for part in range(2):
                piece = buf[OWNERS * chunk + group // SUBS, pl.ds((group % SUBS) * GROUP, GROUP), part * 16:part * 16 + 16]
                moved = dot(perm_ref[...], piece.reshape(256, PATCH)).astype(BF16)
                work[part * 16:part * 16 + 16, spot] = moved.reshape(16, 16, PATCH)
            return carry

        lax.fori_loop(0, MEMBERS // GROUP, by_channel, 0)

        def transform(c, carry):
            states = work[c]
            moved = dot(st[2], states) + dot(st[1], states) + dot(st[0], states)
            work[c] = (moved + rest * xbar[pl.ds(c, 1)]).astype(BF16)
            return carry

        lax.fori_loop(0, CHANS, transform, 0)

        for target in range(OWNERS):
            def by_member(index, carry):
                spot = pl.ds(pl.multiple_of(target * MINE + index * GROUP, GROUP), GROUP)
                for part in range(2):
                    piece = work[part * 16:part * 16 + 16, spot]
                    moved = dot(perm_ref[...], piece.reshape(256, PATCH)).astype(BF16)
                    xbuf[2 * chunk + target // 2, pl.ds(index * GROUP, GROUP), part * 16:part * 16 + 16,
                         (target % 2) * PATCH:(target % 2 + 1) * PATCH] = moved.reshape(16, 16, PATCH)
                return carry

            lax.fori_loop(0, SUBS, by_member, 0)

            @pl.when(me != target)
            def _():
                r_copy(chunk, target).start()

            @pl.when(me == target)
            def _():
                own_copy(chunk, target).start()
        return carry

    lax.fori_loop(0, CHUNKS, analyse, 0)

    def finish(chunk, carry):
        for t in range(1, OWNERS):
            f_copy(chunk, t, 0, MINE).wait_send()
            source = (me + t) % OWNERS
            pltpu.make_async_remote_copy(
                r_stage(chunk, 0), r_place(chunk, source), r_send.at[chunk, 0], r_recv.at[chunk, source],
                device_id={'ens': source}, device_id_type=MESH).wait_recv()
        for target in range(OWNERS):
            @pl.when(me != target)
            def _():
                r_copy(chunk, target).wait_send()

            @pl.when(me == target)
            def _():
                own_copy(chunk, target).wait()
        edge_copy(chunk).wait_send()
        return carry

    lax.fori_loop(0, CHUNKS, finish, 0)

    @pl.when(lat > 0)
    def _():
        send_up.wait_send()

    @pl.when(lat < lat_count - 1)
    def _():
        send_down.wait_send()


def solution(mesh):
    lat_count = mesh.shape['lat']
    dom_count = mesh.shape['dom']
    spots = np.arange(256)
    perm = np.zeros((256, 256), np.float32)
    perm[spots, (spots % 16) * 16 + spots // 16] = 1.0

    def local_cycle(ens_block, w_in, w_out, obs_op, obs_val, obs_wt):
        state = jnp.transpose(ens_block, (0, 1, 3, 2))
        op_t = jnp.transpose(obs_op)
        eye8 = jnp.eye(8, dtype=BF16)
        spread = (op_t[:, None, None, :] * eye8[None, :, :, None]).reshape(8 * OBS, 8 * CHANS)
        vmem = pl.BlockSpec(memory_space=pltpu.VMEM)
        hbm = pl.BlockSpec(memory_space=pl.ANY)
        result = pl.pallas_call(
            functools.partial(kernel, lat_count, dom_count),
            out_shape=jax.ShapeDtypeStruct(state.shape, BF16),
            in_specs=[vmem] * 6 + [hbm],
            out_specs=hbm,
            scratch_shapes=[
                pltpu.VMEM((STAGE + 3 * CHUNKS, MINE, CHANS, PATCH), BF16),
                pltpu.VMEM((ROWS + 2, MINE, CHANS, COLS), BF16),
                pltpu.VMEM((CHUNKS, 2, CHANS, 128), BF16),
                pltpu.VMEM((CHUNKS, 2, CHANS, 128), BF16),
                pltpu.VMEM((3 * OBS, MEMBERS, PATCH), BF16),
                pltpu.VMEM((MEMBERS, MEMBERS), F32),
                pltpu.VMEM((MEMBERS, MEMBERS), F32),
                pltpu.VMEM((MEMBERS, MEMBERS), F32),
                pltpu.VMEM((MEMBERS, MEMBERS), F32),
                pltpu.VMEM((3, MEMBERS, MEMBERS), BF16),
                pltpu.VMEM((3, MEMBERS, MEMBERS), BF16),
                pltpu.VMEM((3, MEMBERS, MEMBERS), BF16),
                pltpu.VMEM((CHANS, PATCH), F32),
                pltpu.VMEM((OBS, PATCH), F32),
                pltpu.VMEM((OBS, PATCH), F32),
                pltpu.VMEM((OBS, PATCH), F32),
                pltpu.SemaphoreType.DMA((ROWS,)),
                pltpu.SemaphoreType.DMA((2,)),
                pltpu.SemaphoreType.DMA((2,)),
                pltpu.SemaphoreType.DMA((2,)),
                pltpu.SemaphoreType.DMA((CHUNKS,)),
                pltpu.SemaphoreType.DMA((CHUNKS,)),
                pltpu.SemaphoreType.DMA((CHUNKS, 3)),
                pltpu.SemaphoreType.DMA((CHUNKS, OWNERS)),
                pltpu.SemaphoreType.DMA((CHUNKS, OWNERS)),
                pltpu.SemaphoreType.DMA((CHUNKS, OWNERS)),
                pltpu.SemaphoreType.DMA((CHUNKS,)),
            ],
            compiler_params=pltpu.CompilerParams(collective_id=0, has_side_effects=True, vmem_limit_bytes=67043328),
        )(jnp.transpose(w_in), jnp.transpose(w_out), spread, jnp.asarray(perm, BF16),
          jnp.transpose(obs_val, (0, 1, 3, 2)), jnp.transpose(obs_wt, (0, 1, 3, 2)), state)
        return jnp.transpose(result, (0, 1, 3, 2))

    state_spec = P('ens', 'lat', 'dom', None)
    obs_spec = P('lat', 'dom', None, None)
    return jax.shard_map(local_cycle, mesh=mesh, in_specs=(state_spec, P(), P(), P(), obs_spec, obs_spec), out_specs=state_spec, check_vma=False)
```

```python
import functools
import math

import jax
import jax.numpy as jnp
import numpy as np
from jax import lax
from jax.experimental import pallas as pl
from jax.experimental.pallas import tpu as pltpu
from jax.sharding import PartitionSpec as P

NS_STEPS = 12
MESH = pl.DeviceIdType.MESH
F32 = jnp.float32
BF16 = jnp.bfloat16
MEMBERS = 256
MINE = 64
ROWS = 8
COLS = 512
CHANS = 32
PATCH = 256
OBS = 16
CHUNKS = 4
OWNERS = 4
GROUP = 16
BATCH = 4
PACK = 8
SUBS = MINE // GROUP
STAGE = CHUNKS * OWNERS


def split3(value):
    high = value.astype(BF16)
    rest = value - high.astype(F32)
    mid = rest.astype(BF16)
    low = (rest - mid.astype(F32)).astype(BF16)
    return high, mid, low


def dot(a, b):
    return jnp.dot(a, b, preferred_element_type=F32)


def dot_t(a, b):
    return lax.dot_general(a, b, (((1,), (1,)), ((), ())), preferred_element_type=F32)


def dot6(a, b):
    small = dot(a[2][...], b[0][...]) + dot(a[0][...], b[2][...]) + dot(a[1][...], b[1][...])
    return small + dot(a[1][...], b[0][...]) + dot(a[0][...], b[1][...]) + dot(a[0][...], b[0][...])


def chunk_row(chunk, which):
    last = chunk // (CHUNKS - 1)
    return (1 - last) * (1 + 2 * chunk + which) + last * (ROWS - 1) * which


def kernel(lat_count, dom_count, w1_ref, w2_ref, bd_ref, perm_ref, yo_ref, wt_ref, x_ref, out_ref,
           buf, xbuf, edge_out, edge_in, work, am, pm, zm, cif, sy, sz, st, xbar, ybar, sw_ref, sd_ref,
           x_sem, halo_send, halo_recv, halo_local, edge_send, edge_recv, f_send, f_recv, r_send, r_recv, own_sem):
    me = lax.axis_index('ens')
    lat = lax.axis_index('lat')
    dom = lax.axis_index('dom')
    my_row = me // 2
    my_half = me % 2
    lat_up = (lat + lat_count - 1) % lat_count
    lat_down = (lat + 1) % lat_count
    dom_other = (dom + 1) % dom_count

    row_copies = [pltpu.make_async_copy(x_ref.at[:, r], xbuf.at[r + 1], x_sem.at[r]) for r in range(ROWS)]
    for r in range(ROWS):
        row_copies[r].start()

    barrier = pltpu.get_barrier_semaphore()
    for t in range(1, OWNERS):
        pl.semaphore_signal(barrier, inc=1, device_id={'ens': (me + t) % OWNERS}, device_id_type=MESH)
    pl.semaphore_signal(barrier, inc=1, device_id={'lat': lat_up}, device_id_type=MESH)
    pl.semaphore_signal(barrier, inc=1, device_id={'lat': lat_down}, device_id_type=MESH)
    pl.semaphore_signal(barrier, inc=1, device_id={'dom': dom_other}, device_id_type=MESH)
    pl.semaphore_wait(barrier, OWNERS + 2)

    send_up = pltpu.make_async_remote_copy(x_ref.at[:, 0], xbuf.at[ROWS + 1], halo_send.at[0], halo_recv.at[1],
                                           device_id={'lat': lat_up}, device_id_type=MESH)
    send_down = pltpu.make_async_remote_copy(x_ref.at[:, ROWS - 1], xbuf.at[0], halo_send.at[1], halo_recv.at[0],
                                             device_id={'lat': lat_down}, device_id_type=MESH)
    top_copy = pltpu.make_async_copy(x_ref.at[:, 0], xbuf.at[0], halo_local.at[0])
    bottom_copy = pltpu.make_async_copy(x_ref.at[:, ROWS - 1], xbuf.at[ROWS + 1], halo_local.at[1])

    @pl.when(lat > 0)
    def _():
        send_up.start()

    @pl.when(lat < lat_count - 1)
    def _():
        send_down.start()

    @pl.when(lat == 0)
    def _():
        top_copy.start()

    @pl.when(lat == lat_count - 1)
    def _():
        bottom_copy.start()

    lane = lax.broadcasted_iota(jnp.int32, (CHANS, 128), 1)

    def edge_copy(chunk):
        return pltpu.make_async_remote_copy(edge_out.at[chunk], edge_in.at[chunk], edge_send.at[chunk], edge_recv.at[chunk],
                                            device_id={'dom': dom_other}, device_id_type=MESH)

    def pack(chunk, carry):
        def members(index, acc):
            first, last = acc
            for offset in range(PACK):
                m = index * PACK + offset
                for which in range(2):
                    row = chunk_row(chunk, which) + 1
                    spot = lane == which * MINE + m
                    west = xbuf[row, m, :, 0:128].astype(F32)
                    east = xbuf[row, m, :, COLS - 128:COLS].astype(F32)
                    first = jnp.where(spot, west[:, 0:1], first)
                    last = jnp.where(spot, east[:, 127:128], last)
            return first, last

        zero = jnp.zeros((CHANS, 128), F32)
        first, last = lax.fori_loop(0, MINE // PACK, members, (zero, zero))
        edge_out[chunk, 0] = first.astype(BF16)
        edge_out[chunk, 1] = last.astype(BF16)
        edge_copy(chunk).start()
        return carry

    for r in range(4):
        row_copies[r].wait()
    pack(0, 0)
    for r in range(4, ROWS):
        row_copies[r].wait()
    lax.fori_loop(1, CHUNKS, pack, 0)

    def f_copy(chunk, t, start, size):
        owner = (me + t) % OWNERS
        return pltpu.make_async_remote_copy(
            buf.at[STAGE + 3 * chunk + t - 1, pl.ds(start, size)], buf.at[OWNERS * chunk + me, pl.ds(start, size)],
            f_send.at[chunk, t - 1], f_recv.at[chunk, me], device_id={'ens': owner}, device_id_type=MESH)

    def forecast_chunk(chunk, carry):
        edge_copy(chunk).wait_recv()

        @pl.when((chunk == CHUNKS - 1) & (lat > 0))
        def _():
            send_down.wait_recv()

        @pl.when((chunk == CHUNKS - 1) & (lat == 0))
        def _():
            top_copy.wait()

        @pl.when((chunk == CHUNKS - 1) & (lat < lat_count - 1))
        def _():
            send_up.wait_recv()

        @pl.when((chunk == CHUNKS - 1) & (lat == lat_count - 1))
        def _():
            bottom_copy.wait()

        slots = []
        for owner in range(OWNERS):
            ahead = (owner - me + OWNERS) % OWNERS
            own = 1 - (ahead + OWNERS - 1) // OWNERS
            slots.append(own * (OWNERS * chunk + me) + (1 - own) * (STAGE + 3 * chunk + ahead - 1))

        def members(index, carry):
            from_east = edge_in[chunk, 0].astype(F32)
            from_west = edge_in[chunk, 1].astype(F32)
            places, kept, features = [], [], []
            for m in [index * BATCH + offset for offset in range(BATCH)]:
                for which in range(2):
                    row = chunk_row(chunk, which) + 1
                    spot = which * MINE + m
                    halo_west = pltpu.roll(from_west, (128 - spot) % 128, 1)
                    halo_east = pltpu.roll(from_east, 127 - spot, 1)
                    here = xbuf[row, m]
                    mid = here.astype(F32)
                    above = xbuf[row - 1, m].astype(F32)
                    below = xbuf[row + 1, m].astype(F32)
                    west = pltpu.roll(mid, 1, 1)
                    east = pltpu.roll(mid, COLS - 1, 1)
                    west = jnp.concatenate([jnp.where(lane == 0, halo_west, west[:, :128]), west[:, 128:]], axis=1)
                    east = jnp.concatenate([east[:, :COLS - 128], jnp.where(lane == 127, halo_east, east[:, COLS - 128:])], axis=1)
                    laplace = (above + below + west + east - 4.0 * mid).astype(BF16)
                    features.append(jnp.concatenate([here, laplace], axis=0))
                    places.append((row, m, which))
            pre_act = dot(w1_ref[...], jnp.concatenate(features, axis=1))
            hidden = (0.5 * pre_act * (1.0 + lax.erf(pre_act * math.sqrt(0.5)))).astype(BF16)
            update = dot(w2_ref[...], hidden)
            for unit, (row, m, which) in enumerate(places):
                for half in range(2):
                    part = update[:, unit * COLS + half * PATCH:unit * COLS + (half + 1) * PATCH]
                    mid = xbuf[row, m, :, half * PATCH:(half + 1) * PATCH].astype(F32)
                    buf[slots[2 * which + half], m] = (mid + part).astype(BF16)
            return carry

        def sub(index, carry):
            start = index * GROUP
            lax.fori_loop(index * (GROUP // BATCH), (index + 1) * (GROUP // BATCH), members, 0)
            for t in (2, 1, 3):
                f_copy(chunk, t, start, GROUP).start()
            return carry

        lax.fori_loop(0, SUBS, sub, 0)
        return carry

    lax.fori_loop(0, CHUNKS, forecast_chunk, 0)

    def r_place(chunk, owner):
        return out_ref.at[:, chunk_row(chunk, owner // 2), :, pl.ds(pl.multiple_of((owner % 2) * PATCH, PATCH), PATCH)]

    def r_stage(chunk, target):
        return xbuf.at[2 * chunk + target // 2, :, :, (target % 2) * PATCH:(target % 2 + 1) * PATCH]

    def r_copy(chunk, target):
        return pltpu.make_async_remote_copy(
            r_stage(chunk, target), r_place(chunk, me), r_send.at[chunk, target], r_recv.at[chunk, me],
            device_id={'ens': target}, device_id_type=MESH)

    def own_copy(chunk, target):
        return pltpu.make_async_copy(r_stage(chunk, target), r_place(chunk, me), own_sem.at[chunk])

    row_id = lax.broadcasted_iota(jnp.int32, (MEMBERS, MEMBERS), 0)
    col_id = lax.broadcasted_iota(jnp.int32, (MEMBERS, MEMBERS), 1)

    def analyse(chunk, carry):
        for t in range(1, OWNERS):
            source = (me + t) % OWNERS
            pltpu.make_async_remote_copy(
                buf.at[STAGE], buf.at[OWNERS * chunk + source], f_send.at[chunk, 0], f_recv.at[chunk, source],
                device_id={'ens': source}, device_id_type=MESH).wait_recv()
        row = chunk_row(chunk, my_row)

        def block(group):
            return buf[OWNERS * chunk + group // SUBS, pl.ds((group % SUBS) * GROUP, GROUP)]

        def sums(group, acc):
            x_sum, y_sum = acc
            states = block(group)
            x_sum = x_sum + jnp.sum(states.astype(F32), axis=0)
            for part in range(2):
                y_sum = y_sum + dot(bd_ref[...], states[part * 8:part * 8 + 8].reshape(8 * CHANS, PATCH))
            return x_sum, y_sum

        x_sum, y_sum = lax.fori_loop(0, MEMBERS // GROUP, sums,
                                     (jnp.zeros((CHANS, PATCH), F32), jnp.zeros((8 * OBS, PATCH), F32)))
        xbar[...] = x_sum * (1.0 / MEMBERS)
        y_mean = jnp.sum(y_sum.reshape(OBS, 8, PATCH), axis=1) * (1.0 / MEMBERS)
        ybar[...] = y_mean
        root_wt = jnp.sqrt(wt_ref[row, my_half])
        sw_ref[...] = root_wt
        sd_ref[...] = root_wt * (yo_ref[row, my_half] - y_mean)

        def anomalies(group, carry):
            states = block(group)
            y_parts = [dot(bd_ref[...], states[part * 8:part * 8 + 8].reshape(8 * CHANS, PATCH)) for part in range(2)]
            spot = pl.ds(pl.multiple_of(group * GROUP, GROUP), GROUP)
            c_innov = jnp.zeros((GROUP, PATCH), F32)
            for o in range(OBS):
                y = jnp.concatenate([y_parts[0][o * 8:o * 8 + 8], y_parts[1][o * 8:o * 8 + 8]], axis=0)
                scaled = (y - ybar[o:o + 1]) * sw_ref[o:o + 1]
                c_innov = c_innov + scaled * sd_ref[o:o + 1]
                high, mid, low = split3(scaled)
                work[o, spot] = high
                work[OBS + o, spot] = mid
                work[2 * OBS + o, spot] = low
            cif[spot] = c_innov
            return carry

        lax.fori_loop(0, MEMBERS // GROUP, anomalies, 0)

        am[...] = jnp.zeros((MEMBERS, MEMBERS), F32)
        pm[...] = jnp.zeros((MEMBERS, MEMBERS), F32)

        def gram(o, carry):
            high = work[o]
            mid = work[OBS + o]
            pm[...] += dot_t(high, mid) + dot_t(high, work[2 * OBS + o])
            am[...] += dot_t(mid, mid) + dot_t(high, high)
            return carry

        lax.fori_loop(0, OBS, gram, 0)
        eye = jnp.where(row_id == col_id, 1.0, 0.0).astype(F32)
        cross = pm[...]
        a_mat = (MEMBERS - 1) * eye + (am[...] + (cross + cross.T))
        scale = jnp.sqrt(jnp.sum(jnp.sum(a_mat * a_mat, axis=0, keepdims=True), axis=1, keepdims=True))

        def put(refs, value):
            for index, part in enumerate(split3(value)):
                refs[index] = part

        def parts(refs):
            return [refs.at[index] for index in range(3)]

        put(sy, a_mat / scale)
        put(sz, eye)

        def newton(step, carry):
            unit = jnp.where(row_id == col_id, 1.5, 0.0).astype(F32)
            put(st, unit - 0.5 * dot6(parts(sz), parts(sy)))
            put(sy, dot6(parts(sy), parts(st)))
            z_next = dot6(parts(st), parts(sz))
            zm[...] = z_next
            put(sz, z_next)
            return carry

        lax.fori_loop(0, NS_STEPS, newton, 0)
        s_mat = zm[...] / jnp.sqrt(scale)
        zm[...] = s_mat
        put(sz, s_mat)
        pa_mat = dot6(parts(sz), parts(sz))
        c_innov = jnp.sum(cif[...], axis=1, keepdims=True)
        w_mean = jnp.sum(pa_mat * c_innov, axis=0, keepdims=True)
        t_mat = math.sqrt(MEMBERS - 1) * zm[...] + w_mean
        put(st, t_mat)
        rest = 1.0 - jnp.sum(t_mat, axis=1, keepdims=True)

        def by_channel(group, carry):
            spot = pl.ds(pl.multiple_of(group * GROUP, GROUP), GROUP)
            for part in range(2):
                piece = buf[OWNERS * chunk + group // SUBS, pl.ds((group % SUBS) * GROUP, GROUP), part * 16:part * 16 + 16]
                moved = dot(perm_ref[...], piece.reshape(256, PATCH)).astype(BF16)
                work[part * 16:part * 16 + 16, spot] = moved.reshape(16, 16, PATCH)
            return carry

        lax.fori_loop(0, MEMBERS // GROUP, by_channel, 0)

        def transform(c, carry):
            states = work[c]
            moved = dot(st[2], states) + dot(st[1], states) + dot(st[0], states)
            work[c] = (moved + rest * xbar[pl.ds(c, 1)]).astype(BF16)
            return carry

        lax.fori_loop(0, CHANS, transform, 0)

        for target in range(OWNERS):
            def by_member(index, carry):
                spot = pl.ds(pl.multiple_of(target * MINE + index * GROUP, GROUP), GROUP)
                for part in range(2):
                    piece = work[part * 16:part * 16 + 16, spot]
                    moved = dot(perm_ref[...], piece.reshape(256, PATCH)).astype(BF16)
                    xbuf[2 * chunk + target // 2, pl.ds(index * GROUP, GROUP), part * 16:part * 16 + 16,
                         (target % 2) * PATCH:(target % 2 + 1) * PATCH] = moved.reshape(16, 16, PATCH)
                return carry

            lax.fori_loop(0, SUBS, by_member, 0)

            @pl.when(me != target)
            def _():
                r_copy(chunk, target).start()

            @pl.when(me == target)
            def _():
                own_copy(chunk, target).start()
        return carry

    lax.fori_loop(0, CHUNKS, analyse, 0)

    def finish(chunk, carry):
        for t in range(1, OWNERS):
            f_copy(chunk, t, 0, MINE).wait_send()
            source = (me + t) % OWNERS
            pltpu.make_async_remote_copy(
                r_stage(chunk, 0), r_place(chunk, source), r_send.at[chunk, 0], r_recv.at[chunk, source],
                device_id={'ens': source}, device_id_type=MESH).wait_recv()
        for target in range(OWNERS):
            @pl.when(me != target)
            def _():
                r_copy(chunk, target).wait_send()

            @pl.when(me == target)
            def _():
                own_copy(chunk, target).wait()
        edge_copy(chunk).wait_send()
        return carry

    lax.fori_loop(0, CHUNKS, finish, 0)

    @pl.when(lat > 0)
    def _():
        send_up.wait_send()

    @pl.when(lat < lat_count - 1)
    def _():
        send_down.wait_send()


def solution(mesh):
    lat_count = mesh.shape['lat']
    dom_count = mesh.shape['dom']
    spots = np.arange(256)
    perm = np.zeros((256, 256), np.float32)
    perm[spots, (spots % 16) * 16 + spots // 16] = 1.0

    def local_cycle(ens_block, w_in, w_out, obs_op, obs_val, obs_wt):
        state = jnp.transpose(ens_block, (0, 1, 3, 2))
        op_t = jnp.transpose(obs_op)
        eye8 = jnp.eye(8, dtype=BF16)
        spread = (op_t[:, None, None, :] * eye8[None, :, :, None]).reshape(8 * OBS, 8 * CHANS)
        vmem = pl.BlockSpec(memory_space=pltpu.VMEM)
        hbm = pl.BlockSpec(memory_space=pl.ANY)
        result = pl.pallas_call(
            functools.partial(kernel, lat_count, dom_count),
            out_shape=jax.ShapeDtypeStruct(state.shape, BF16),
            in_specs=[vmem] * 6 + [hbm],
            out_specs=hbm,
            scratch_shapes=[
                pltpu.VMEM((STAGE + 3 * CHUNKS, MINE, CHANS, PATCH), BF16),
                pltpu.VMEM((ROWS + 2, MINE, CHANS, COLS), BF16),
                pltpu.VMEM((CHUNKS, 2, CHANS, 128), BF16),
                pltpu.VMEM((CHUNKS, 2, CHANS, 128), BF16),
                pltpu.VMEM((3 * OBS, MEMBERS, PATCH), BF16),
                pltpu.VMEM((MEMBERS, MEMBERS), F32),
                pltpu.VMEM((MEMBERS, MEMBERS), F32),
                pltpu.VMEM((MEMBERS, MEMBERS), F32),
                pltpu.VMEM((MEMBERS, MEMBERS), F32),
                pltpu.VMEM((3, MEMBERS, MEMBERS), BF16),
                pltpu.VMEM((3, MEMBERS, MEMBERS), BF16),
                pltpu.VMEM((3, MEMBERS, MEMBERS), BF16),
                pltpu.VMEM((CHANS, PATCH), F32),
                pltpu.VMEM((OBS, PATCH), F32),
                pltpu.VMEM((OBS, PATCH), F32),
                pltpu.VMEM((OBS, PATCH), F32),
                pltpu.SemaphoreType.DMA((ROWS,)),
                pltpu.SemaphoreType.DMA((2,)),
                pltpu.SemaphoreType.DMA((2,)),
                pltpu.SemaphoreType.DMA((2,)),
                pltpu.SemaphoreType.DMA((CHUNKS,)),
                pltpu.SemaphoreType.DMA((CHUNKS,)),
                pltpu.SemaphoreType.DMA((CHUNKS, 3)),
                pltpu.SemaphoreType.DMA((CHUNKS, OWNERS)),
                pltpu.SemaphoreType.DMA((CHUNKS, OWNERS)),
                pltpu.SemaphoreType.DMA((CHUNKS, OWNERS)),
                pltpu.SemaphoreType.DMA((CHUNKS,)),
            ],
            compiler_params=pltpu.CompilerParams(collective_id=0, has_side_effects=True, vmem_limit_bytes=67043328),
        )(jnp.transpose(w_in), jnp.transpose(w_out), spread, jnp.asarray(perm, BF16),
          jnp.transpose(obs_val, (0, 1, 3, 2)), jnp.transpose(obs_wt, (0, 1, 3, 2)), state)
        return jnp.transpose(result, (0, 1, 3, 2))

    state_spec = P('ens', 'lat', 'dom', None)
    obs_spec = P('lat', 'dom', None, None)
    return jax.shard_map(local_cycle, mesh=mesh, in_specs=(state_spec, P(), P(), P(), obs_spec, obs_spec), out_specs=state_spec, check_vma=False)
```

```python
import functools
import math

import jax
import jax.numpy as jnp
from jax import lax
from jax.experimental import pallas as pl
from jax.experimental.pallas import tpu as pltpu
from jax.sharding import PartitionSpec as P

NS_STEPS = 12
MESH = pl.DeviceIdType.MESH
F32 = jnp.float32
BF16 = jnp.bfloat16
MEMBERS = 256
MINE = 64
ROWS = 8
COLS = 512
CHANS = 32
PATCH = 256
OBS = 16
CHUNKS = 4
OWNERS = 4
GROUP = 16
BATCH = 4
PACK = 8
SUBS = MINE // GROUP
FIRST_ROWS = (1, 2, 0, 3)
STAGE = CHUNKS * OWNERS


def split3(value):
    high = value.astype(BF16)
    rest = value - high.astype(F32)
    mid = rest.astype(BF16)
    low = (rest - mid.astype(F32)).astype(BF16)
    return high, mid, low


def dot(a, b):
    return jnp.dot(a, b, preferred_element_type=F32)


def dot_t(a, b):
    return lax.dot_general(a, b, (((1,), (1,)), ((), ())), preferred_element_type=F32)


def dot6(a, b):
    small = dot(a[2][...], b[0][...]) + dot(a[0][...], b[2][...]) + dot(a[1][...], b[1][...])
    return small + dot(a[1][...], b[0][...]) + dot(a[0][...], b[1][...]) + dot(a[0][...], b[0][...])


def chunk_row(chunk, which):
    last = chunk // (CHUNKS - 1)
    return (1 - last) * (1 + 2 * chunk + which) + last * (ROWS - 1) * which


def kernel(lat_count, dom_count, w_in_ref, w2_ref, op_ref, yo_hbm, wt_hbm, x_ref, xbuf,
           buf, w1_ref, bd_ref, perm_ref, yo_ref, wt_ref, edge_out, edge_in, work, am, pm, zm, cif, sy, sz, st, xbar, ybar, sw_ref, sd_ref,
           x_sem, halo_send, halo_recv, halo_local, edge_send, edge_recv, f_send, f_recv, r_send, r_recv, obs_sem, ready):
    me = lax.axis_index('ens')
    lat = lax.axis_index('lat')
    dom = lax.axis_index('dom')
    my_row = me // 2
    my_half = me % 2
    lat_up = (lat + lat_count - 1) % lat_count
    lat_down = (lat + 1) % lat_count
    dom_other = (dom + 1) % dom_count

    row_copies = [pltpu.make_async_copy(x_ref.at[:, r], xbuf.at[r + 1], x_sem.at[r]) for r in range(ROWS)]
    obs_copies = [pltpu.make_async_copy(yo_hbm, yo_ref, obs_sem.at[0]), pltpu.make_async_copy(wt_hbm, wt_ref, obs_sem.at[1])]
    for r in FIRST_ROWS:
        row_copies[r].start()

    barrier = pltpu.get_barrier_semaphore()
    for t in range(1, OWNERS):
        pl.semaphore_signal(barrier, inc=1, device_id={'ens': (me + t) % OWNERS}, device_id_type=MESH)
    pl.semaphore_signal(barrier, inc=1, device_id={'lat': lat_up}, device_id_type=MESH)
    pl.semaphore_signal(barrier, inc=1, device_id={'lat': lat_down}, device_id_type=MESH)
    pl.semaphore_signal(barrier, inc=1, device_id={'dom': dom_other}, device_id_type=MESH)

    w1_ref[...] = w_in_ref[...].astype(F32).T.astype(BF16)
    chan_id = lax.broadcasted_iota(jnp.int32, (CHANS, 8 * CHANS), 0)
    slot_id = lax.broadcasted_iota(jnp.int32, (CHANS, 8 * CHANS), 1)
    repeat = jnp.where(chan_id == slot_id % CHANS, 1.0, 0.0).astype(BF16)
    wide = jnp.broadcast_to(dot(op_ref[...], repeat)[:, None, :], (OBS, 8, 8 * CHANS))
    copy_id = lax.broadcasted_iota(jnp.int32, (OBS, 8, 8 * CHANS), 1)
    place_id = lax.broadcasted_iota(jnp.int32, (OBS, 8, 8 * CHANS), 2)
    bd_ref[...] = jnp.where(copy_id == place_id // CHANS, wide, 0.0).reshape(8 * OBS, 8 * CHANS).astype(BF16)
    row_id = lax.broadcasted_iota(jnp.int32, (MEMBERS, MEMBERS), 0)
    col_id = lax.broadcasted_iota(jnp.int32, (MEMBERS, MEMBERS), 1)
    perm_ref[...] = jnp.where((row_id // 16 == col_id % 16) & (row_id % 16 == col_id // 16), 1.0, 0.0).astype(BF16)
    pl.semaphore_wait(barrier, OWNERS + 2)

    send_up = pltpu.make_async_remote_copy(x_ref.at[:, 0], xbuf.at[ROWS + 1], halo_send.at[0], halo_recv.at[1],
                                           device_id={'lat': lat_up}, device_id_type=MESH)
    send_down = pltpu.make_async_remote_copy(x_ref.at[:, ROWS - 1], xbuf.at[0], halo_send.at[1], halo_recv.at[0],
                                             device_id={'lat': lat_down}, device_id_type=MESH)
    top_copy = pltpu.make_async_copy(x_ref.at[:, 0], xbuf.at[0], halo_local.at[0])
    bottom_copy = pltpu.make_async_copy(x_ref.at[:, ROWS - 1], xbuf.at[ROWS + 1], halo_local.at[1])

    @pl.when(lat > 0)
    def _():
        send_up.start()

    @pl.when(lat < lat_count - 1)
    def _():
        send_down.start()

    @pl.when(lat == 0)
    def _():
        top_copy.start()

    @pl.when(lat == lat_count - 1)
    def _():
        bottom_copy.start()

    lane = lax.broadcasted_iota(jnp.int32, (CHANS, 128), 1)

    def edge_copy(chunk):
        return pltpu.make_async_remote_copy(edge_out.at[chunk], edge_in.at[chunk], edge_send.at[chunk], edge_recv.at[chunk],
                                            device_id={'dom': dom_other}, device_id_type=MESH)

    def pack(chunk):
        def members(index, acc):
            first, last = acc
            for offset in range(PACK):
                m = index * PACK + offset
                for which in range(2):
                    row = chunk_row(chunk, which) + 1
                    spot = lane == which * MINE + m
                    west = xbuf[row, m, :, 0:128].astype(F32)
                    east = xbuf[row, m, :, COLS - 128:COLS].astype(F32)
                    first = jnp.where(spot, west[:, 0:1], first)
                    last = jnp.where(spot, east[:, 127:128], last)
            return first, last

        zero = jnp.zeros((CHANS, 128), F32)
        first, last = lax.fori_loop(0, MINE // PACK, members, (zero, zero))
        edge_out[chunk, 0] = first.astype(BF16)
        edge_out[chunk, 1] = last.astype(BF16)
        edge_copy(chunk).start()

    for r in (1, 2):
        row_copies[r].wait()
    pack(0)
    for r in (0, 3):
        row_copies[r].wait()
    for r in range(4, ROWS):
        row_copies[r].start()
    for copy in obs_copies:
        copy.start()
    row_copies[4].wait()
    pack(1)

    def f_copy(chunk, t, start, size):
        owner = (me + t) % OWNERS
        return pltpu.make_async_remote_copy(
            buf.at[STAGE + 3 * chunk + t - 1, pl.ds(start, size)], buf.at[OWNERS * chunk + me, pl.ds(start, size)],
            f_send.at[chunk, t - 1], f_recv.at[chunk, me], device_id={'ens': owner}, device_id_type=MESH)

    def forecast_chunk(chunk, carry):
        edge_copy(chunk).wait_recv()

        @pl.when((chunk == CHUNKS - 1) & (lat > 0))
        def _():
            send_down.wait_recv()

        @pl.when((chunk == CHUNKS - 1) & (lat == 0))
        def _():
            top_copy.wait()

        @pl.when((chunk == CHUNKS - 1) & (lat < lat_count - 1))
        def _():
            send_up.wait_recv()

        @pl.when((chunk == CHUNKS - 1) & (lat == lat_count - 1))
        def _():
            bottom_copy.wait()

        slots = []
        for owner in range(OWNERS):
            ahead = (owner - me + OWNERS) % OWNERS
            own = 1 - (ahead + OWNERS - 1) // OWNERS
            slots.append(own * (OWNERS * chunk + me) + (1 - own) * (STAGE + 3 * chunk + ahead - 1))

        def members(index):
            from_east = edge_in[chunk, 0].astype(F32)
            from_west = edge_in[chunk, 1].astype(F32)
            places, kept, features = [], [], []
            for m in [index * BATCH + offset for offset in range(BATCH)]:
                for which in range(2):
                    row = chunk_row(chunk, which) + 1
                    spot = which * MINE + m
                    halo_west = pltpu.roll(from_west, (128 - spot) % 128, 1)
                    halo_east = pltpu.roll(from_east, 127 - spot, 1)
                    here = xbuf[row, m]
                    mid = here.astype(F32)
                    above = xbuf[row - 1, m].astype(F32)
                    below = xbuf[row + 1, m].astype(F32)
                    west = pltpu.roll(mid, 1, 1)
                    east = pltpu.roll(mid, COLS - 1, 1)
                    west = jnp.concatenate([jnp.where(lane == 0, halo_west, west[:, :128]), west[:, 128:]], axis=1)
                    east = jnp.concatenate([east[:, :COLS - 128], jnp.where(lane == 127, halo_east, east[:, COLS - 128:])], axis=1)
                    laplace = (above + below + west + east - 4.0 * mid).astype(BF16)
                    features.append(jnp.concatenate([here, laplace], axis=0))
                    places.append((row, m, which))
            pre_act = dot(w1_ref[...], jnp.concatenate(features, axis=1))
            hidden = (0.5 * pre_act * (1.0 + lax.erf(pre_act * math.sqrt(0.5)))).astype(BF16)
            update = dot(w2_ref[...], hidden)
            for unit, (row, m, which) in enumerate(places):
                for half in range(2):
                    part = update[:, unit * COLS + half * PATCH:unit * COLS + (half + 1) * PATCH]
                    mid = xbuf[row, m, :, half * PATCH:(half + 1) * PATCH].astype(F32)
                    buf[slots[2 * which + half], m] = (mid + part).astype(BF16)

        def send(index, carry):
            members(index)
            for t in (2, 1, 3):
                f_copy(chunk, t, index * BATCH, BATCH).start()
            return carry

        lax.fori_loop(0, MINE // BATCH, send, 0)

        @pl.when(chunk == 0)
        def _():
            for r in range(5, ROWS):
                row_copies[r].wait()

        @pl.when(chunk < CHUNKS - 2)
        def _():
            pack(chunk + 2)
        return carry

    lax.fori_loop(0, CHUNKS, forecast_chunk, 0)
    for t in range(1, OWNERS):
        pl.semaphore_signal(ready, inc=1, device_id={'ens': (me + t) % OWNERS}, device_id_type=MESH)
    for copy in obs_copies:
        copy.wait()

    def place(chunk, owner):
        return chunk_row(chunk, owner // 2) + 1, pl.ds(pl.multiple_of((owner % 2) * PATCH, PATCH), PATCH)

    def r_copy(chunk, t, source):
        row, span = place(chunk, source)
        return pltpu.make_async_remote_copy(
            buf.at[STAGE + 3 * chunk + t - 1], xbuf.at[row, :, :, span], r_send.at[chunk, t - 1], r_recv.at[chunk, source],
            device_id={'ens': (me + t) % OWNERS}, device_id_type=MESH)

    def analyse(chunk, carry):
        for t in range(1, OWNERS):
            source = (me + t) % OWNERS
            pltpu.make_async_remote_copy(
                buf.at[STAGE], buf.at[OWNERS * chunk + source], f_send.at[chunk, 0], f_recv.at[chunk, source],
                device_id={'ens': source}, device_id_type=MESH).wait_recv()
        row = chunk_row(chunk, my_row)

        def block(group):
            return buf[OWNERS * chunk + group // SUBS, pl.ds((group % SUBS) * GROUP, GROUP)]

        def sums(group, acc):
            x_sum, y_sum = acc
            states = block(group)
            x_sum = x_sum + jnp.sum(states.astype(F32), axis=0)
            for part in range(2):
                y_sum = y_sum + dot(bd_ref[...], states[part * 8:part * 8 + 8].reshape(8 * CHANS, PATCH))
            return x_sum, y_sum

        x_sum, y_sum = lax.fori_loop(0, MEMBERS // GROUP, sums,
                                     (jnp.zeros((CHANS, PATCH), F32), jnp.zeros((8 * OBS, PATCH), F32)))
        xbar[...] = x_sum * (1.0 / MEMBERS)
        y_mean = jnp.sum(y_sum.reshape(OBS, 8, PATCH), axis=1) * (1.0 / MEMBERS)
        ybar[...] = y_mean
        root_wt = jnp.sqrt(wt_ref[row, my_half])
        sw_ref[...] = root_wt
        sd_ref[...] = root_wt * (yo_ref[row, my_half] - y_mean)

        def anomalies(group, carry):
            states = block(group)
            y_parts = [dot(bd_ref[...], states[part * 8:part * 8 + 8].reshape(8 * CHANS, PATCH)) for part in range(2)]
            spot = pl.ds(pl.multiple_of(group * GROUP, GROUP), GROUP)
            c_innov = jnp.zeros((GROUP, PATCH), F32)
            for o in range(OBS):
                y = jnp.concatenate([y_parts[0][o * 8:o * 8 + 8], y_parts[1][o * 8:o * 8 + 8]], axis=0)
                scaled = (y - ybar[o:o + 1]) * sw_ref[o:o + 1]
                c_innov = c_innov + scaled * sd_ref[o:o + 1]
                high, mid, low = split3(scaled)
                work[o, spot] = high
                work[OBS + o, spot] = mid
                work[2 * OBS + o, spot] = low
            cif[spot] = c_innov
            return carry

        lax.fori_loop(0, MEMBERS // GROUP, anomalies, 0)

        am[...] = jnp.zeros((MEMBERS, MEMBERS), F32)
        pm[...] = jnp.zeros((MEMBERS, MEMBERS), F32)

        def gram(o, carry):
            high = work[o]
            mid = work[OBS + o]
            pm[...] += dot_t(high, mid) + dot_t(high, work[2 * OBS + o])
            am[...] += dot_t(mid, mid) + dot_t(high, high)
            return carry

        lax.fori_loop(0, OBS, gram, 0)
        eye = jnp.where(row_id == col_id, 1.0, 0.0).astype(F32)
        cross = pm[...]
        a_mat = (MEMBERS - 1) * eye + (am[...] + (cross + cross.T))
        scale = jnp.sqrt(jnp.sum(jnp.sum(a_mat * a_mat, axis=0, keepdims=True), axis=1, keepdims=True))

        def put(refs, value):
            for index, part in enumerate(split3(value)):
                refs[index] = part

        def parts(refs):
            return [refs.at[index] for index in range(3)]

        put(sy, a_mat / scale)
        put(sz, eye)

        def newton(step, carry):
            unit = jnp.where(row_id == col_id, 1.5, 0.0).astype(F32)
            put(st, unit - 0.5 * dot6(parts(sz), parts(sy)))
            put(sy, dot6(parts(sy), parts(st)))
            z_next = dot6(parts(st), parts(sz))
            zm[...] = z_next
            put(sz, z_next)
            return carry

        lax.fori_loop(0, NS_STEPS, newton, 0)
        s_mat = zm[...] / jnp.sqrt(scale)
        zm[...] = s_mat
        put(sz, s_mat)
        pa_mat = dot6(parts(sz), parts(sz))
        c_innov = jnp.sum(cif[...], axis=1, keepdims=True)
        w_mean = jnp.sum(pa_mat * c_innov, axis=0, keepdims=True)
        t_mat = math.sqrt(MEMBERS - 1) * zm[...] + w_mean
        put(st, t_mat)
        rest = 1.0 - jnp.sum(t_mat, axis=1, keepdims=True)

        def by_channel(group, carry):
            spot = pl.ds(pl.multiple_of(group * GROUP, GROUP), GROUP)
            for part in range(2):
                piece = buf[OWNERS * chunk + group // SUBS, pl.ds((group % SUBS) * GROUP, GROUP), part * 16:part * 16 + 16]
                moved = dot(perm_ref[...], piece.reshape(256, PATCH)).astype(BF16)
                work[part * 16:part * 16 + 16, spot] = moved.reshape(16, 16, PATCH)
            return carry

        lax.fori_loop(0, MEMBERS // GROUP, by_channel, 0)

        def transform(c, carry):
            states = work[c]
            moved = dot(st[2], states) + dot(st[1], states) + dot(st[0], states)
            work[c] = (moved + rest * xbar[pl.ds(c, 1)]).astype(BF16)
            return carry

        lax.fori_loop(0, CHANS, transform, 0)

        for t in range(1, OWNERS):
            f_copy(chunk, t, 0, MINE).wait_send()

        @pl.when(chunk == 0)
        def _():
            pl.semaphore_wait(ready, OWNERS - 1)

        for t in (2, 1, 3, 0):
            def by_member(index, carry):
                spot = pl.ds(pl.multiple_of(((me + t) % OWNERS) * MINE + index * GROUP, GROUP), GROUP)
                for part in range(2):
                    piece = work[part * 16:part * 16 + 16, spot]
                    moved = dot(perm_ref[...], piece.reshape(256, PATCH)).astype(BF16).reshape(16, 16, PATCH)
                    if t == 0:
                        own_row, own_span = place(chunk, me)
                        xbuf[own_row, pl.ds(index * GROUP, GROUP), part * 16:part * 16 + 16, own_span] = moved
                    else:
                        buf[STAGE + 3 * chunk + t - 1, pl.ds(index * GROUP, GROUP), part * 16:part * 16 + 16] = moved
                return carry

            lax.fori_loop(0, SUBS, by_member, 0)
            if t:
                r_copy(chunk, t, me).start()
        return carry

    lax.fori_loop(0, CHUNKS, analyse, 0)

    def finish(chunk, carry):
        for t in range(1, OWNERS):
            r_copy(chunk, t, (me + t) % OWNERS).wait_recv()
            r_copy(chunk, t, me).wait_send()
        edge_copy(chunk).wait_send()
        return carry

    lax.fori_loop(0, CHUNKS, finish, 0)

    @pl.when(lat > 0)
    def _():
        send_up.wait_send()

    @pl.when(lat < lat_count - 1)
    def _():
        send_down.wait_send()


def store_kernel(held, out_ref, sems):
    copies = [pltpu.make_async_copy(held.at[r + 1], out_ref.at[:, r], sems.at[r]) for r in range(ROWS)]
    for copy in copies:
        copy.start()
    for copy in copies:
        copy.wait()


def solution(mesh):
    lat_count = mesh.shape['lat']
    dom_count = mesh.shape['dom']

    def local_cycle(ens_block, w_in, w_out, obs_op, obs_val, obs_wt):
        state = jnp.transpose(ens_block, (0, 1, 3, 2))
        vmem = pl.BlockSpec(memory_space=pltpu.VMEM)
        hbm = pl.BlockSpec(memory_space=pl.ANY)
        held = pl.pallas_call(
            functools.partial(kernel, lat_count, dom_count),
            out_shape=pltpu.VMEM((ROWS + 2, MINE, CHANS, COLS), BF16),
            in_specs=[vmem] * 3 + [hbm] * 3,
            out_specs=vmem,
            scratch_shapes=[
                pltpu.VMEM((STAGE + 3 * CHUNKS, MINE, CHANS, PATCH), BF16),
                pltpu.VMEM((128, 2 * CHANS), BF16),
                pltpu.VMEM((8 * OBS, 8 * CHANS), BF16),
                pltpu.VMEM((256, 256), BF16),
                pltpu.VMEM((ROWS, 2, OBS, PATCH), F32),
                pltpu.VMEM((ROWS, 2, OBS, PATCH), F32),
                pltpu.VMEM((CHUNKS, 2, CHANS, 128), BF16),
                pltpu.VMEM((CHUNKS, 2, CHANS, 128), BF16),
                pltpu.VMEM((3 * OBS, MEMBERS, PATCH), BF16),
                pltpu.VMEM((MEMBERS, MEMBERS), F32),
                pltpu.VMEM((MEMBERS, MEMBERS), F32),
                pltpu.VMEM((MEMBERS, MEMBERS), F32),
                pltpu.VMEM((MEMBERS, MEMBERS), F32),
                pltpu.VMEM((3, MEMBERS, MEMBERS), BF16),
                pltpu.VMEM((3, MEMBERS, MEMBERS), BF16),
                pltpu.VMEM((3, MEMBERS, MEMBERS), BF16),
                pltpu.VMEM((CHANS, PATCH), F32),
                pltpu.VMEM((OBS, PATCH), F32),
                pltpu.VMEM((OBS, PATCH), F32),
                pltpu.VMEM((OBS, PATCH), F32),
                pltpu.SemaphoreType.DMA((ROWS,)),
                pltpu.SemaphoreType.DMA((2,)),
                pltpu.SemaphoreType.DMA((2,)),
                pltpu.SemaphoreType.DMA((2,)),
                pltpu.SemaphoreType.DMA((CHUNKS,)),
                pltpu.SemaphoreType.DMA((CHUNKS,)),
                pltpu.SemaphoreType.DMA((CHUNKS, 3)),
                pltpu.SemaphoreType.DMA((CHUNKS, OWNERS)),
                pltpu.SemaphoreType.DMA((CHUNKS, 3)),
                pltpu.SemaphoreType.DMA((CHUNKS, OWNERS)),
                pltpu.SemaphoreType.DMA((2,)),
                pltpu.SemaphoreType.REGULAR,
            ],
            compiler_params=pltpu.CompilerParams(collective_id=0, has_side_effects=True, vmem_limit_bytes=43 * 2 ** 20),
        )(w_in, jnp.transpose(w_out), jnp.transpose(obs_op),
          jnp.transpose(obs_val, (0, 1, 3, 2)), jnp.transpose(obs_wt, (0, 1, 3, 2)), state)
        result = pl.pallas_call(
            store_kernel,
            out_shape=jax.ShapeDtypeStruct(state.shape, BF16),
            in_specs=[vmem],
            out_specs=hbm,
            scratch_shapes=[pltpu.SemaphoreType.DMA((ROWS,))],
            compiler_params=pltpu.CompilerParams(vmem_limit_bytes=2 ** 20),
        )(pltpu.with_memory_space_constraint(held, pltpu.VMEM))
        return jnp.transpose(result, (0, 1, 3, 2))

    state_spec = P('ens', 'lat', 'dom', None)
    obs_spec = P('lat', 'dom', None, None)
    return jax.shard_map(local_cycle, mesh=mesh, in_specs=(state_spec, P(), P(), P(), obs_spec, obs_spec), out_specs=state_spec, check_vma=False)
```

```python
import functools
import math

import jax
import jax.numpy as jnp
from jax import lax
from jax.experimental import pallas as pl
from jax.experimental.pallas import tpu as pltpu
from jax.sharding import PartitionSpec as P

NS_STEPS = 12
MESH = pl.DeviceIdType.MESH
F32 = jnp.float32
BF16 = jnp.bfloat16
MEMBERS = 256
MINE = 64
ROWS = 8
COLS = 512
CHANS = 32
PATCH = 256
OBS = 16
CHUNKS = 4
OWNERS = 4
GROUP = 16
BATCH = 4
PACK = 8
SUBS = MINE // GROUP
FIRST = 16
INNER = 32
STAGE = CHUNKS * OWNERS


def split3(value):
    high = value.astype(BF16)
    rest = value - high.astype(F32)
    mid = rest.astype(BF16)
    low = (rest - mid.astype(F32)).astype(BF16)
    return high, mid, low


def dot(a, b):
    return jnp.dot(a, b, preferred_element_type=F32)


def dot_t(a, b):
    return lax.dot_general(a, b, (((1,), (1,)), ((), ())), preferred_element_type=F32)


def dot6(a, b):
    small = dot(a[2][...], b[0][...]) + dot(a[0][...], b[2][...]) + dot(a[1][...], b[1][...])
    return small + dot(a[1][...], b[0][...]) + dot(a[0][...], b[1][...]) + dot(a[0][...], b[0][...])


def chunk_row(chunk, which):
    last = chunk // (CHUNKS - 1)
    return (1 - last) * (1 + 2 * chunk + which) + last * (ROWS - 1) * which


def kernel(lat_count, dom_count, w_in_hbm, w_out_hbm, op_hbm, yo_hbm, wt_hbm, x_ref, xbuf,
           buf, w_in_ref, w2_ref, op_ref, w1_ref, bd_ref, perm_ref, yo_ref, wt_ref, edge_out, edge_in, work, am, pm, zm, cif, sy, sz, st, xbar, ybar, sw_ref, sd_ref,
           first_sem, x_sem, small_sem, halo_send, halo_recv, halo_local, edge_send, edge_recv, f_send, f_recv, r_send, r_recv, obs_sem, ready):
    me = lax.axis_index('ens')
    lat = lax.axis_index('lat')
    dom = lax.axis_index('dom')
    my_row = me // 2
    my_half = me % 2
    lat_up = (lat + lat_count - 1) % lat_count
    lat_down = (lat + 1) % lat_count
    dom_other = (dom + 1) % dom_count

    first_copies = [pltpu.make_async_copy(x_ref.at[0:FIRST, r], xbuf.at[r + 1, 0:FIRST], first_sem.at[r]) for r in range(4)]
    row_copies = [pltpu.make_async_copy(x_ref.at[FIRST:, r], xbuf.at[r + 1, FIRST:], x_sem.at[r]) for r in range(4)]
    row_copies += [pltpu.make_async_copy(x_ref.at[:, r], xbuf.at[r + 1], x_sem.at[r]) for r in range(4, ROWS)]
    small_copies = [pltpu.make_async_copy(source, target, small_sem.at[index]) for index, (source, target) in enumerate(
        ((w_in_hbm, w_in_ref), (w_out_hbm, w2_ref), (op_hbm, op_ref)))]
    obs_copies = [pltpu.make_async_copy(yo_hbm, yo_ref, obs_sem.at[0]), pltpu.make_async_copy(wt_hbm, wt_ref, obs_sem.at[1])]
    for copy in small_copies + first_copies:
        copy.start()

    barrier = pltpu.get_barrier_semaphore()
    for t in range(1, OWNERS):
        pl.semaphore_signal(barrier, inc=1, device_id={'ens': (me + t) % OWNERS}, device_id_type=MESH)
    pl.semaphore_signal(barrier, inc=1, device_id={'lat': lat_up}, device_id_type=MESH)
    pl.semaphore_signal(barrier, inc=1, device_id={'lat': lat_down}, device_id_type=MESH)
    pl.semaphore_signal(barrier, inc=1, device_id={'dom': dom_other}, device_id_type=MESH)

    for copy in small_copies:
        copy.wait()
    w1_ref[...] = w_in_ref[...].astype(F32).T.astype(BF16)
    pl.semaphore_wait(barrier, OWNERS + 2)

    send_up = pltpu.make_async_remote_copy(x_ref.at[:, 0], xbuf.at[ROWS + 1], halo_send.at[0], halo_recv.at[1],
                                           device_id={'lat': lat_up}, device_id_type=MESH)
    send_down = pltpu.make_async_remote_copy(x_ref.at[:, ROWS - 1], xbuf.at[0], halo_send.at[1], halo_recv.at[0],
                                             device_id={'lat': lat_down}, device_id_type=MESH)
    top_copy = pltpu.make_async_copy(x_ref.at[:, 0], xbuf.at[0], halo_local.at[0])
    bottom_copy = pltpu.make_async_copy(x_ref.at[:, ROWS - 1], xbuf.at[ROWS + 1], halo_local.at[1])

    lane = lax.broadcasted_iota(jnp.int32, (CHANS, 128), 1)

    def edge_copy(chunk):
        return pltpu.make_async_remote_copy(edge_out.at[chunk], edge_in.at[chunk], edge_send.at[chunk], edge_recv.at[chunk],
                                            device_id={'dom': dom_other}, device_id_type=MESH)

    def pack(chunk):
        def members(index, acc):
            first, last = acc
            for offset in range(PACK):
                m = index * PACK + offset
                for which in range(2):
                    row = chunk_row(chunk, which) + 1
                    spot = lane == which * MINE + m
                    west = xbuf[row, m, :, 0:128].astype(F32)
                    east = xbuf[row, m, :, COLS - 128:COLS].astype(F32)
                    first = jnp.where(spot, west[:, 0:1], first)
                    last = jnp.where(spot, east[:, 127:128], last)
            return first, last

        zero = jnp.zeros((CHANS, 128), F32)
        first, last = lax.fori_loop(0, MINE // PACK, members, (zero, zero))
        edge_out[chunk, 0] = first.astype(BF16)
        edge_out[chunk, 1] = last.astype(BF16)
        edge_copy(chunk).start()

    for copy in first_copies:
        copy.wait()
    for r in range(4):
        row_copies[r].start()

    def f_copy(chunk, t, start, size, kind='all'):
        owner = (me + t) % OWNERS
        source = buf.at[STAGE + 3 * chunk + t - 1, pl.ds(start, size)]
        target = buf.at[OWNERS * chunk + me, pl.ds(start, size)]
        if kind != 'all':
            half = owner % 2 if kind == 'outer' else 1 - owner % 2
            span = pl.ds(pl.multiple_of(half * 128, 128), 128)
            source = source.at[:, :, span]
            target = target.at[:, :, span]
        return pltpu.make_async_remote_copy(source, target, f_send.at[chunk, t - 1], f_recv.at[chunk, me],
                                            device_id={'ens': owner}, device_id_type=MESH)

    def slots_of(chunk):
        slots = []
        for owner in range(OWNERS):
            ahead = (owner - me + OWNERS) % OWNERS
            own = 1 - (ahead + OWNERS - 1) // OWNERS
            slots.append(own * (OWNERS * chunk + me) + (1 - own) * (STAGE + 3 * chunk + ahead - 1))
        return slots

    pieces_of = {'all': (PATCH, ((0, 0, 0), (PATCH, 0, 1))),
                 'inner': (128, ((128, 128, 0), (PATCH, 0, 1))),
                 'outer': (128, ((0, 0, 0), (PATCH + 128, 128, 1)))}

    def members(chunk, index, kind):
        width, pieces = pieces_of[kind]
        slots = slots_of(chunk)
        if kind != 'inner':
            from_east = edge_in[chunk, 0].astype(F32)
            from_west = edge_in[chunk, 1].astype(F32)
        places, features = [], []
        for m in [index * BATCH + offset for offset in range(BATCH)]:
            for which in range(2):
                row = chunk_row(chunk, which) + 1
                spot = which * MINE + m
                here = xbuf[row, m]
                mid = here.astype(F32)
                above = xbuf[row - 1, m].astype(F32)
                below = xbuf[row + 1, m].astype(F32)
                west = pltpu.roll(mid, 1, 1)
                east = pltpu.roll(mid, COLS - 1, 1)
                if kind != 'inner':
                    halo_west = pltpu.roll(from_west, (128 - spot) % 128, 1)
                    halo_east = pltpu.roll(from_east, 127 - spot, 1)
                    west = jnp.concatenate([jnp.where(lane == 0, halo_west, west[:, :128]), west[:, 128:]], axis=1)
                    east = jnp.concatenate([east[:, :COLS - 128], jnp.where(lane == 127, halo_east, east[:, COLS - 128:])], axis=1)
                laplace = (above + below + west + east - 4.0 * mid).astype(BF16)
                for column, first_lane, half in pieces:
                    span = slice(column, column + width)
                    features.append(jnp.concatenate([here[:, span], laplace[:, span]], axis=0))
                    places.append((row, m, span, slice(first_lane, first_lane + width), slots[2 * which + half]))
        pre_act = dot(w1_ref[...], jnp.concatenate(features, axis=1))
        hidden = (0.5 * pre_act * (1.0 + lax.erf(pre_act * math.sqrt(0.5)))).astype(BF16)
        update = dot(w2_ref[...], hidden)
        for unit, (row, m, span, lanes, slot) in enumerate(places):
            part = update[:, unit * width:(unit + 1) * width]
            buf[slot, m, :, lanes] = (xbuf[row, m, :, span].astype(F32) + part).astype(BF16)

    def forecast(chunk, start, stop, kind):
        def step(index, carry):
            members(chunk, index, kind)
            for t in (2, 1, 3):
                f_copy(chunk, t, index * BATCH, BATCH, kind).start()
            return carry

        lax.fori_loop(start // BATCH, stop // BATCH, step, 0)

    forecast(0, 0, FIRST, 'inner')
    for r in range(4):
        row_copies[r].wait()
    for r in range(4, ROWS):
        row_copies[r].start()
    for copy in obs_copies:
        copy.start()
    pack(0)

    @pl.when(lat > 0)
    def _():
        send_up.start()

    @pl.when(lat < lat_count - 1)
    def _():
        send_down.start()

    @pl.when(lat == 0)
    def _():
        top_copy.start()

    @pl.when(lat == lat_count - 1)
    def _():
        bottom_copy.start()

    forecast(0, FIRST, INNER, 'inner')
    edge_copy(0).wait_recv()
    forecast(0, 0, INNER, 'outer')
    forecast(0, INNER, MINE, 'all')
    for r in range(4, ROWS):
        row_copies[r].wait()
    pack(1)

    def forecast_chunk(chunk, carry):
        edge_copy(chunk).wait_recv()

        @pl.when((chunk == CHUNKS - 1) & (lat > 0))
        def _():
            send_down.wait_recv()

        @pl.when((chunk == CHUNKS - 1) & (lat == 0))
        def _():
            top_copy.wait()

        @pl.when((chunk == CHUNKS - 1) & (lat < lat_count - 1))
        def _():
            send_up.wait_recv()

        @pl.when((chunk == CHUNKS - 1) & (lat == lat_count - 1))
        def _():
            bottom_copy.wait()

        @pl.when(chunk < CHUNKS - 1)
        def _():
            pack(chunk + 1)

        forecast(chunk, 0, MINE, 'all')
        return carry

    lax.fori_loop(1, CHUNKS, forecast_chunk, 0)

    chan_id = lax.broadcasted_iota(jnp.int32, (CHANS, 8 * CHANS), 0)
    slot_id = lax.broadcasted_iota(jnp.int32, (CHANS, 8 * CHANS), 1)
    repeat = jnp.where(chan_id == slot_id % CHANS, 1.0, 0.0).astype(BF16)
    wide = jnp.broadcast_to(dot(op_ref[...], repeat)[:, None, :], (OBS, 8, 8 * CHANS))
    copy_id = lax.broadcasted_iota(jnp.int32, (OBS, 8, 8 * CHANS), 1)
    place_id = lax.broadcasted_iota(jnp.int32, (OBS, 8, 8 * CHANS), 2)
    bd_ref[...] = jnp.where(copy_id == place_id // CHANS, wide, 0.0).reshape(8 * OBS, 8 * CHANS).astype(BF16)
    row_id = lax.broadcasted_iota(jnp.int32, (MEMBERS, MEMBERS), 0)
    col_id = lax.broadcasted_iota(jnp.int32, (MEMBERS, MEMBERS), 1)
    perm_ref[...] = jnp.where((row_id // 16 == col_id % 16) & (row_id % 16 == col_id // 16), 1.0, 0.0).astype(BF16)
    for t in range(1, OWNERS):
        pl.semaphore_signal(ready, inc=1, device_id={'ens': (me + t) % OWNERS}, device_id_type=MESH)
    for copy in obs_copies:
        copy.wait()

    def place(chunk, owner):
        return chunk_row(chunk, owner // 2) + 1, pl.ds(pl.multiple_of((owner % 2) * PATCH, PATCH), PATCH)

    def r_copy(chunk, t, source):
        row, span = place(chunk, source)
        return pltpu.make_async_remote_copy(
            buf.at[STAGE + 3 * chunk + t - 1], xbuf.at[row, :, :, span], r_send.at[chunk, t - 1], r_recv.at[chunk, source],
            device_id={'ens': (me + t) % OWNERS}, device_id_type=MESH)

    def analyse(chunk, carry):
        for t in range(1, OWNERS):
            source = (me + t) % OWNERS
            pltpu.make_async_remote_copy(
                buf.at[STAGE], buf.at[OWNERS * chunk + source], f_send.at[chunk, 0], f_recv.at[chunk, source],
                device_id={'ens': source}, device_id_type=MESH).wait_recv()
        row = chunk_row(chunk, my_row)

        def block(group):
            return buf[OWNERS * chunk + group // SUBS, pl.ds((group % SUBS) * GROUP, GROUP)]

        def sums(group, acc):
            x_sum, y_sum = acc
            states = block(group)
            x_sum = x_sum + jnp.sum(states.astype(F32), axis=0)
            for part in range(2):
                y_sum = y_sum + dot(bd_ref[...], states[part * 8:part * 8 + 8].reshape(8 * CHANS, PATCH))
            return x_sum, y_sum

        x_sum, y_sum = lax.fori_loop(0, MEMBERS // GROUP, sums,
                                     (jnp.zeros((CHANS, PATCH), F32), jnp.zeros((8 * OBS, PATCH), F32)))
        xbar[...] = x_sum * (1.0 / MEMBERS)
        y_mean = jnp.sum(y_sum.reshape(OBS, 8, PATCH), axis=1) * (1.0 / MEMBERS)
        ybar[...] = y_mean
        root_wt = jnp.sqrt(wt_ref[row, my_half])
        sw_ref[...] = root_wt
        sd_ref[...] = root_wt * (yo_ref[row, my_half] - y_mean)

        def anomalies(group, carry):
            states = block(group)
            y_parts = [dot(bd_ref[...], states[part * 8:part * 8 + 8].reshape(8 * CHANS, PATCH)) for part in range(2)]
            spot = pl.ds(pl.multiple_of(group * GROUP, GROUP), GROUP)
            c_innov = jnp.zeros((GROUP, PATCH), F32)
            for o in range(OBS):
                y = jnp.concatenate([y_parts[0][o * 8:o * 8 + 8], y_parts[1][o * 8:o * 8 + 8]], axis=0)
                scaled = (y - ybar[o:o + 1]) * sw_ref[o:o + 1]
                c_innov = c_innov + scaled * sd_ref[o:o + 1]
                high, mid, low = split3(scaled)
                work[o, spot] = high
                work[OBS + o, spot] = mid
                work[2 * OBS + o, spot] = low
            cif[spot] = c_innov
            return carry

        lax.fori_loop(0, MEMBERS // GROUP, anomalies, 0)

        am[...] = jnp.zeros((MEMBERS, MEMBERS), F32)
        pm[...] = jnp.zeros((MEMBERS, MEMBERS), F32)

        def gram(o, carry):
            high = work[o]
            mid = work[OBS + o]
            pm[...] += dot_t(high, mid) + dot_t(high, work[2 * OBS + o])
            am[...] += dot_t(mid, mid) + dot_t(high, high)
            return carry

        lax.fori_loop(0, OBS, gram, 0)
        eye = jnp.where(row_id == col_id, 1.0, 0.0).astype(F32)
        cross = pm[...]
        a_mat = (MEMBERS - 1) * eye + (am[...] + (cross + cross.T))
        scale = jnp.sqrt(jnp.sum(jnp.sum(a_mat * a_mat, axis=0, keepdims=True), axis=1, keepdims=True))

        def put(refs, value):
            for index, part in enumerate(split3(value)):
                refs[index] = part

        def parts(refs):
            return [refs.at[index] for index in range(3)]

        put(sy, a_mat / scale)
        put(sz, eye)

        def newton(step, carry):
            unit = jnp.where(row_id == col_id, 1.5, 0.0).astype(F32)
            put(st, unit - 0.5 * dot6(parts(sz), parts(sy)))
            put(sy, dot6(parts(sy), parts(st)))
            z_next = dot6(parts(st), parts(sz))
            zm[...] = z_next
            put(sz, z_next)
            return carry

        lax.fori_loop(0, NS_STEPS, newton, 0)
        s_mat = zm[...] / jnp.sqrt(scale)
        zm[...] = s_mat
        put(sz, s_mat)
        pa_mat = dot6(parts(sz), parts(sz))
        c_innov = jnp.sum(cif[...], axis=1, keepdims=True)
        w_mean = jnp.sum(pa_mat * c_innov, axis=0, keepdims=True)
        t_mat = math.sqrt(MEMBERS - 1) * zm[...] + w_mean
        put(st, t_mat)
        rest = 1.0 - jnp.sum(t_mat, axis=1, keepdims=True)

        def by_channel(group, carry):
            spot = pl.ds(pl.multiple_of(group * GROUP, GROUP), GROUP)
            for part in range(2):
                piece = buf[OWNERS * chunk + group // SUBS, pl.ds((group % SUBS) * GROUP, GROUP), part * 16:part * 16 + 16]
                moved = dot(perm_ref[...], piece.reshape(256, PATCH)).astype(BF16)
                work[part * 16:part * 16 + 16, spot] = moved.reshape(16, 16, PATCH)
            return carry

        lax.fori_loop(0, MEMBERS // GROUP, by_channel, 0)

        def transform(c, carry):
            states = work[c]
            moved = dot(st[2], states) + dot(st[1], states) + dot(st[0], states)
            work[c] = (moved + rest * xbar[pl.ds(c, 1)]).astype(BF16)
            return carry

        lax.fori_loop(0, CHANS, transform, 0)

        for t in range(1, OWNERS):
            f_copy(chunk, t, 0, MINE).wait_send()

        @pl.when(chunk == 0)
        def _():
            pl.semaphore_wait(ready, OWNERS - 1)

        for t in (2, 1, 3, 0):
            def by_member(index, carry):
                spot = pl.ds(pl.multiple_of(((me + t) % OWNERS) * MINE + index * GROUP, GROUP), GROUP)
                for part in range(2):
                    piece = work[part * 16:part * 16 + 16, spot]
                    moved = dot(perm_ref[...], piece.reshape(256, PATCH)).astype(BF16).reshape(16, 16, PATCH)
                    if t == 0:
                        own_row, own_span = place(chunk, me)
                        xbuf[own_row, pl.ds(index * GROUP, GROUP), part * 16:part * 16 + 16, own_span] = moved
                    else:
                        buf[STAGE + 3 * chunk + t - 1, pl.ds(index * GROUP, GROUP), part * 16:part * 16 + 16] = moved
                return carry

            lax.fori_loop(0, SUBS, by_member, 0)
            if t:
                r_copy(chunk, t, me).start()
        return carry

    lax.fori_loop(0, CHUNKS, analyse, 0)

    def finish(chunk, carry):
        for t in range(1, OWNERS):
            r_copy(chunk, t, (me + t) % OWNERS).wait_recv()
            r_copy(chunk, t, me).wait_send()
        edge_copy(chunk).wait_send()
        return carry

    lax.fori_loop(0, CHUNKS, finish, 0)

    @pl.when(lat > 0)
    def _():
        send_up.wait_send()

    @pl.when(lat < lat_count - 1)
    def _():
        send_down.wait_send()


def store_kernel(held, out_ref, sems):
    copies = [pltpu.make_async_copy(held.at[r + 1], out_ref.at[:, r], sems.at[r]) for r in range(ROWS)]
    for copy in copies:
        copy.start()
    for copy in copies:
        copy.wait()


def solution(mesh):
    lat_count = mesh.shape['lat']
    dom_count = mesh.shape['dom']

    def local_cycle(ens_block, w_in, w_out, obs_op, obs_val, obs_wt):
        state = jnp.transpose(ens_block, (0, 1, 3, 2))
        vmem = pl.BlockSpec(memory_space=pltpu.VMEM)
        hbm = pl.BlockSpec(memory_space=pl.ANY)
        held = pl.pallas_call(
            functools.partial(kernel, lat_count, dom_count),
            out_shape=pltpu.VMEM((ROWS + 2, MINE, CHANS, COLS), BF16),
            in_specs=[hbm] * 6,
            out_specs=vmem,
            scratch_shapes=[
                pltpu.VMEM((STAGE + 3 * CHUNKS, MINE, CHANS, PATCH), BF16),
                pltpu.VMEM((2 * CHANS, 128), BF16),
                pltpu.VMEM((CHANS, 128), BF16),
                pltpu.VMEM((OBS, CHANS), BF16),
                pltpu.VMEM((128, 2 * CHANS), BF16),
                pltpu.VMEM((8 * OBS, 8 * CHANS), BF16),
                pltpu.VMEM((256, 256), BF16),
                pltpu.VMEM((ROWS, 2, OBS, PATCH), F32),
                pltpu.VMEM((ROWS, 2, OBS, PATCH), F32),
                pltpu.VMEM((CHUNKS, 2, CHANS, 128), BF16),
                pltpu.VMEM((CHUNKS, 2, CHANS, 128), BF16),
                pltpu.VMEM((3 * OBS, MEMBERS, PATCH), BF16),
                pltpu.VMEM((MEMBERS, MEMBERS), F32),
                pltpu.VMEM((MEMBERS, MEMBERS), F32),
                pltpu.VMEM((MEMBERS, MEMBERS), F32),
                pltpu.VMEM((MEMBERS, MEMBERS), F32),
                pltpu.VMEM((3, MEMBERS, MEMBERS), BF16),
                pltpu.VMEM((3, MEMBERS, MEMBERS), BF16),
                pltpu.VMEM((3, MEMBERS, MEMBERS), BF16),
                pltpu.VMEM((CHANS, PATCH), F32),
                pltpu.VMEM((OBS, PATCH), F32),
                pltpu.VMEM((OBS, PATCH), F32),
                pltpu.VMEM((OBS, PATCH), F32),
                pltpu.SemaphoreType.DMA((4,)),
                pltpu.SemaphoreType.DMA((ROWS,)),
                pltpu.SemaphoreType.DMA((3,)),
                pltpu.SemaphoreType.DMA((2,)),
                pltpu.SemaphoreType.DMA((2,)),
                pltpu.SemaphoreType.DMA((2,)),
                pltpu.SemaphoreType.DMA((CHUNKS,)),
                pltpu.SemaphoreType.DMA((CHUNKS,)),
                pltpu.SemaphoreType.DMA((CHUNKS, 3)),
                pltpu.SemaphoreType.DMA((CHUNKS, OWNERS)),
                pltpu.SemaphoreType.DMA((CHUNKS, 3)),
                pltpu.SemaphoreType.DMA((CHUNKS, OWNERS)),
                pltpu.SemaphoreType.DMA((2,)),
                pltpu.SemaphoreType.REGULAR,
            ],
            compiler_params=pltpu.CompilerParams(collective_id=0, has_side_effects=True, vmem_limit_bytes=43 * 2 ** 20),
        )(w_in, jnp.transpose(w_out), jnp.transpose(obs_op),
          jnp.transpose(obs_val, (0, 1, 3, 2)), jnp.transpose(obs_wt, (0, 1, 3, 2)), state)
        result = pl.pallas_call(
            store_kernel,
            out_shape=jax.ShapeDtypeStruct(state.shape, BF16),
            in_specs=[vmem],
            out_specs=hbm,
            scratch_shapes=[pltpu.SemaphoreType.DMA((ROWS,))],
            compiler_params=pltpu.CompilerParams(vmem_limit_bytes=2 ** 20),
        )(pltpu.with_memory_space_constraint(held, pltpu.VMEM))
        return jnp.transpose(result, (0, 1, 3, 2))

    state_spec = P('ens', 'lat', 'dom', None)
    obs_spec = P('lat', 'dom', None, None)
    return jax.shard_map(local_cycle, mesh=mesh, in_specs=(state_spec, P(), P(), P(), obs_spec, obs_spec), out_specs=state_spec, check_vma=False)
```

```python
import functools
import math

import jax
import jax.numpy as jnp
from jax import lax
from jax.experimental import pallas as pl
from jax.experimental.pallas import tpu as pltpu
from jax.sharding import PartitionSpec as P

NS_STEPS = 12
MESH = pl.DeviceIdType.MESH
F32 = jnp.float32
BF16 = jnp.bfloat16
MEMBERS = 256
MINE = 64
ROWS = 8
COLS = 512
CHANS = 32
PATCH = 256
OBS = 16
CHUNKS = 4
OWNERS = 4
GROUP = 16
BATCH = 4
PACK = 8
SUBS = MINE // GROUP
FIRST = 16
INNER = 32
STAGE = CHUNKS * OWNERS


def split3(value):
    high = value.astype(BF16)
    rest = value - high.astype(F32)
    mid = rest.astype(BF16)
    low = (rest - mid.astype(F32)).astype(BF16)
    return high, mid, low


def dot(a, b):
    return jnp.dot(a, b, preferred_element_type=F32)


def dot_t(a, b):
    return lax.dot_general(a, b, (((1,), (1,)), ((), ())), preferred_element_type=F32)


def dot6(a, b):
    small = dot(a[2][...], b[0][...]) + dot(a[0][...], b[2][...]) + dot(a[1][...], b[1][...])
    return small + dot(a[1][...], b[0][...]) + dot(a[0][...], b[1][...]) + dot(a[0][...], b[0][...])


def chunk_row(chunk, which):
    last = chunk // (CHUNKS - 1)
    return (1 - last) * (1 + 2 * chunk + which) + last * (ROWS - 1) * which


def kernel(lat_count, dom_count, w_in_hbm, w_out_hbm, op_hbm, yo_hbm, wt_hbm, x_ref, xbuf,
           buf, w_in_ref, w2_ref, op_ref, w1_ref, bd_ref, perm_ref, yo_ref, wt_ref, edge_out, edge_in, work, am, pm, zm, cif, sy, sz, st, xbar, ybar, sw_ref, sd_ref,
           first_sem, upper_sem, lower_sem, small_sem, halo_send, halo_recv, halo_local, edge_send, edge_recv, f_send, f_recv, r_send, r_recv, obs_sem, ready):
    me = lax.axis_index('ens')
    lat = lax.axis_index('lat')
    dom = lax.axis_index('dom')
    my_row = me // 2
    my_half = me % 2
    lat_up = (lat + lat_count - 1) % lat_count
    lat_down = (lat + 1) % lat_count
    dom_other = (dom + 1) % dom_count

    def first_copy(index):
        some = pl.ds(index * BATCH, BATCH)
        return pltpu.make_async_copy(x_ref.at[some, 0:4], xbuf.at[some, 1:5], first_sem.at[index])

    def block_copies(start, first_row, sems):
        size = (MINE - start) // 4
        return [pltpu.make_async_copy(x_ref.at[start + size * part:start + size * part + size, first_row:first_row + 4],
                                      xbuf.at[start + size * part:start + size * part + size, first_row + 1:first_row + 5],
                                      sems.at[part]) for part in range(4)]

    upper_copies = block_copies(FIRST, 0, upper_sem)
    lower_copies = block_copies(0, 4, lower_sem)
    small_copies = [pltpu.make_async_copy(source, target, small_sem.at[index]) for index, (source, target) in enumerate(
        ((w_in_hbm, w_in_ref), (w_out_hbm, w2_ref), (op_hbm, op_ref)))]
    obs_copies = [pltpu.make_async_copy(yo_hbm, yo_ref, obs_sem.at[0]), pltpu.make_async_copy(wt_hbm, wt_ref, obs_sem.at[1])]
    first_copy(0).start()
    for copy in small_copies:
        copy.start()
    for index in range(1, FIRST // BATCH):
        first_copy(index).start()

    barrier = pltpu.get_barrier_semaphore()
    for t in range(1, OWNERS):
        pl.semaphore_signal(barrier, inc=1, device_id={'ens': (me + t) % OWNERS}, device_id_type=MESH)
    pl.semaphore_signal(barrier, inc=1, device_id={'lat': lat_up}, device_id_type=MESH)
    pl.semaphore_signal(barrier, inc=1, device_id={'lat': lat_down}, device_id_type=MESH)
    pl.semaphore_signal(barrier, inc=1, device_id={'dom': dom_other}, device_id_type=MESH)

    for copy in small_copies:
        copy.wait()
    w1_ref[...] = w_in_ref[...].astype(F32).T.astype(BF16)
    pl.semaphore_wait(barrier, OWNERS + 2)

    send_up = pltpu.make_async_remote_copy(x_ref.at[:, 0], xbuf.at[:, ROWS + 1], halo_send.at[0], halo_recv.at[1],
                                           device_id={'lat': lat_up}, device_id_type=MESH)
    send_down = pltpu.make_async_remote_copy(x_ref.at[:, ROWS - 1], xbuf.at[:, 0], halo_send.at[1], halo_recv.at[0],
                                             device_id={'lat': lat_down}, device_id_type=MESH)
    top_copy = pltpu.make_async_copy(x_ref.at[:, 0], xbuf.at[:, 0], halo_local.at[0])
    bottom_copy = pltpu.make_async_copy(x_ref.at[:, ROWS - 1], xbuf.at[:, ROWS + 1], halo_local.at[1])

    lane = lax.broadcasted_iota(jnp.int32, (CHANS, 128), 1)

    def edge_copy(chunk):
        return pltpu.make_async_remote_copy(edge_out.at[chunk], edge_in.at[chunk], edge_send.at[chunk], edge_recv.at[chunk],
                                            device_id={'dom': dom_other}, device_id_type=MESH)

    def pack(chunk):
        def members(index, acc):
            first, last = acc
            for offset in range(PACK):
                m = index * PACK + offset
                for which in range(2):
                    row = chunk_row(chunk, which) + 1
                    spot = lane == which * MINE + m
                    west = xbuf[m, row, :, 0:128].astype(F32)
                    east = xbuf[m, row, :, COLS - 128:COLS].astype(F32)
                    first = jnp.where(spot, west[:, 0:1], first)
                    last = jnp.where(spot, east[:, 127:128], last)
            return first, last

        zero = jnp.zeros((CHANS, 128), F32)
        first, last = lax.fori_loop(0, MINE // PACK, members, (zero, zero))
        edge_out[chunk, 0] = first.astype(BF16)
        edge_out[chunk, 1] = last.astype(BF16)
        edge_copy(chunk).start()

    for copy in upper_copies:
        copy.start()

    def f_copy(chunk, t, start, size, kind='all'):
        owner = (me + t) % OWNERS
        source = buf.at[STAGE + 3 * chunk + t - 1, pl.ds(start, size)]
        target = buf.at[OWNERS * chunk + me, pl.ds(start, size)]
        if kind != 'all':
            half = owner % 2 if kind == 'outer' else 1 - owner % 2
            span = pl.ds(pl.multiple_of(half * 128, 128), 128)
            source = source.at[:, :, span]
            target = target.at[:, :, span]
        return pltpu.make_async_remote_copy(source, target, f_send.at[chunk, t - 1], f_recv.at[chunk, me],
                                            device_id={'ens': owner}, device_id_type=MESH)

    def slots_of(chunk):
        slots = []
        for owner in range(OWNERS):
            ahead = (owner - me + OWNERS) % OWNERS
            own = 1 - (ahead + OWNERS - 1) // OWNERS
            slots.append(own * (OWNERS * chunk + me) + (1 - own) * (STAGE + 3 * chunk + ahead - 1))
        return slots

    pieces_of = {'all': (PATCH, ((0, 0, 0), (PATCH, 0, 1))),
                 'inner': (128, ((128, 128, 0), (PATCH, 0, 1))),
                 'outer': (128, ((0, 0, 0), (PATCH + 128, 128, 1)))}

    def members(chunk, index, kind):
        width, pieces = pieces_of[kind]
        slots = slots_of(chunk)
        if kind != 'inner':
            from_east = edge_in[chunk, 0].astype(F32)
            from_west = edge_in[chunk, 1].astype(F32)
        places, features = [], []
        for m in [index * BATCH + offset for offset in range(BATCH)]:
            for which in range(2):
                row = chunk_row(chunk, which) + 1
                spot = which * MINE + m
                here = xbuf[m, row]
                mid = here.astype(F32)
                above = xbuf[m, row - 1].astype(F32)
                below = xbuf[m, row + 1].astype(F32)
                west = pltpu.roll(mid, 1, 1)
                east = pltpu.roll(mid, COLS - 1, 1)
                if kind != 'inner':
                    halo_west = pltpu.roll(from_west, (128 - spot) % 128, 1)
                    halo_east = pltpu.roll(from_east, 127 - spot, 1)
                    west = jnp.concatenate([jnp.where(lane == 0, halo_west, west[:, :128]), west[:, 128:]], axis=1)
                    east = jnp.concatenate([east[:, :COLS - 128], jnp.where(lane == 127, halo_east, east[:, COLS - 128:])], axis=1)
                laplace = (above + below + west + east - 4.0 * mid).astype(BF16)
                for column, first_lane, half in pieces:
                    span = slice(column, column + width)
                    features.append(jnp.concatenate([here[:, span], laplace[:, span]], axis=0))
                    places.append((row, m, span, slice(first_lane, first_lane + width), slots[2 * which + half]))
        pre_act = dot(w1_ref[...], jnp.concatenate(features, axis=1))
        hidden = (0.5 * pre_act * (1.0 + lax.erf(pre_act * math.sqrt(0.5)))).astype(BF16)
        update = dot(w2_ref[...], hidden)
        for unit, (row, m, span, lanes, slot) in enumerate(places):
            part = update[:, unit * width:(unit + 1) * width]
            buf[slot, m, :, lanes] = (xbuf[m, row, :, span].astype(F32) + part).astype(BF16)

    def forecast(chunk, start, stop, kind):
        def step(index, carry):
            if kind == 'inner' and start == 0:
                first_copy(index).wait()
            members(chunk, index, kind)
            for t in (2, 1, 3):
                f_copy(chunk, t, index * BATCH, BATCH, kind).start()
            return carry

        lax.fori_loop(start // BATCH, stop // BATCH, step, 0)

    forecast(0, 0, FIRST, 'inner')
    for copy in upper_copies:
        copy.wait()
    for copy in lower_copies:
        copy.start()
    for copy in obs_copies:
        copy.start()
    pack(0)

    @pl.when(lat > 0)
    def _():
        send_up.start()

    @pl.when(lat < lat_count - 1)
    def _():
        send_down.start()

    @pl.when(lat == 0)
    def _():
        top_copy.start()

    @pl.when(lat == lat_count - 1)
    def _():
        bottom_copy.start()

    forecast(0, FIRST, INNER, 'inner')
    edge_copy(0).wait_recv()
    forecast(0, 0, INNER, 'outer')
    forecast(0, INNER, MINE, 'all')
    for copy in lower_copies:
        copy.wait()
    pack(1)

    def forecast_chunk(chunk, carry):
        edge_copy(chunk).wait_recv()

        @pl.when((chunk == CHUNKS - 1) & (lat > 0))
        def _():
            send_down.wait_recv()

        @pl.when((chunk == CHUNKS - 1) & (lat == 0))
        def _():
            top_copy.wait()

        @pl.when((chunk == CHUNKS - 1) & (lat < lat_count - 1))
        def _():
            send_up.wait_recv()

        @pl.when((chunk == CHUNKS - 1) & (lat == lat_count - 1))
        def _():
            bottom_copy.wait()

        @pl.when(chunk < CHUNKS - 1)
        def _():
            pack(chunk + 1)

        forecast(chunk, 0, MINE, 'all')
        return carry

    lax.fori_loop(1, CHUNKS, forecast_chunk, 0)

    chan_id = lax.broadcasted_iota(jnp.int32, (CHANS, 8 * CHANS), 0)
    slot_id = lax.broadcasted_iota(jnp.int32, (CHANS, 8 * CHANS), 1)
    repeat = jnp.where(chan_id == slot_id % CHANS, 1.0, 0.0).astype(BF16)
    wide = jnp.broadcast_to(dot(op_ref[...], repeat)[:, None, :], (OBS, 8, 8 * CHANS))
    copy_id = lax.broadcasted_iota(jnp.int32, (OBS, 8, 8 * CHANS), 1)
    place_id = lax.broadcasted_iota(jnp.int32, (OBS, 8, 8 * CHANS), 2)
    bd_ref[...] = jnp.where(copy_id == place_id // CHANS, wide, 0.0).reshape(8 * OBS, 8 * CHANS).astype(BF16)
    row_id = lax.broadcasted_iota(jnp.int32, (MEMBERS, MEMBERS), 0)
    col_id = lax.broadcasted_iota(jnp.int32, (MEMBERS, MEMBERS), 1)
    perm_ref[...] = jnp.where((row_id // 16 == col_id % 16) & (row_id % 16 == col_id // 16), 1.0, 0.0).astype(BF16)
    for t in range(1, OWNERS):
        pl.semaphore_signal(ready, inc=1, device_id={'ens': (me + t) % OWNERS}, device_id_type=MESH)
    for copy in obs_copies:
        copy.wait()

    def place(chunk, owner):
        return chunk_row(chunk, owner // 2) + 1, pl.ds(pl.multiple_of((owner % 2) * PATCH, PATCH), PATCH)

    def r_copy(chunk, t, source):
        row, span = place(chunk, source)
        return pltpu.make_async_remote_copy(
            buf.at[STAGE + 3 * chunk + t - 1], xbuf.at[:, row, :, span], r_send.at[chunk, t - 1], r_recv.at[chunk, source],
            device_id={'ens': (me + t) % OWNERS}, device_id_type=MESH)

    def analyse(chunk, carry):
        for t in range(1, OWNERS):
            source = (me + t) % OWNERS
            pltpu.make_async_remote_copy(
                buf.at[STAGE], buf.at[OWNERS * chunk + source], f_send.at[chunk, 0], f_recv.at[chunk, source],
                device_id={'ens': source}, device_id_type=MESH).wait_recv()
        row = chunk_row(chunk, my_row)

        def block(group):
            return buf[OWNERS * chunk + group // SUBS, pl.ds((group % SUBS) * GROUP, GROUP)]

        def sums(group, acc):
            x_sum, y_sum = acc
            states = block(group)
            x_sum = x_sum + jnp.sum(states.astype(F32), axis=0)
            for part in range(2):
                y_sum = y_sum + dot(bd_ref[...], states[part * 8:part * 8 + 8].reshape(8 * CHANS, PATCH))
            return x_sum, y_sum

        x_sum, y_sum = lax.fori_loop(0, MEMBERS // GROUP, sums,
                                     (jnp.zeros((CHANS, PATCH), F32), jnp.zeros((8 * OBS, PATCH), F32)))
        xbar[...] = x_sum * (1.0 / MEMBERS)
        y_mean = jnp.sum(y_sum.reshape(OBS, 8, PATCH), axis=1) * (1.0 / MEMBERS)
        ybar[...] = y_mean
        root_wt = jnp.sqrt(wt_ref[row, my_half])
        sw_ref[...] = root_wt
        sd_ref[...] = root_wt * (yo_ref[row, my_half] - y_mean)

        def anomalies(group, carry):
            states = block(group)
            y_parts = [dot(bd_ref[...], states[part * 8:part * 8 + 8].reshape(8 * CHANS, PATCH)) for part in range(2)]
            spot = pl.ds(pl.multiple_of(group * GROUP, GROUP), GROUP)
            c_innov = jnp.zeros((GROUP, PATCH), F32)
            for o in range(OBS):
                y = jnp.concatenate([y_parts[0][o * 8:o * 8 + 8], y_parts[1][o * 8:o * 8 + 8]], axis=0)
                scaled = (y - ybar[o:o + 1]) * sw_ref[o:o + 1]
                c_innov = c_innov + scaled * sd_ref[o:o + 1]
                high, mid, low = split3(scaled)
                work[o, spot] = high
                work[OBS + o, spot] = mid
                work[2 * OBS + o, spot] = low
            cif[spot] = c_innov
            return carry

        lax.fori_loop(0, MEMBERS // GROUP, anomalies, 0)

        am[...] = jnp.zeros((MEMBERS, MEMBERS), F32)
        pm[...] = jnp.zeros((MEMBERS, MEMBERS), F32)

        def gram(o, carry):
            high = work[o]
            mid = work[OBS + o]
            pm[...] += dot_t(high, mid) + dot_t(high, work[2 * OBS + o])
            am[...] += dot_t(mid, mid) + dot_t(high, high)
            return carry

        lax.fori_loop(0, OBS, gram, 0)
        eye = jnp.where(row_id == col_id, 1.0, 0.0).astype(F32)
        cross = pm[...]
        a_mat = (MEMBERS - 1) * eye + (am[...] + (cross + cross.T))
        scale = jnp.sqrt(jnp.sum(jnp.sum(a_mat * a_mat, axis=0, keepdims=True), axis=1, keepdims=True))

        def put(refs, value):
            for index, part in enumerate(split3(value)):
                refs[index] = part

        def parts(refs):
            return [refs.at[index] for index in range(3)]

        put(sy, a_mat / scale)
        put(sz, eye)

        def newton(step, carry):
            unit = jnp.where(row_id == col_id, 1.5, 0.0).astype(F32)
            put(st, unit - 0.5 * dot6(parts(sz), parts(sy)))
            put(sy, dot6(parts(sy), parts(st)))
            z_next = dot6(parts(st), parts(sz))
            zm[...] = z_next
            put(sz, z_next)
            return carry

        lax.fori_loop(0, NS_STEPS, newton, 0)
        s_mat = zm[...] / jnp.sqrt(scale)
        zm[...] = s_mat
        put(sz, s_mat)
        pa_mat = dot6(parts(sz), parts(sz))
        c_innov = jnp.sum(cif[...], axis=1, keepdims=True)
        w_mean = jnp.sum(pa_mat * c_innov, axis=0, keepdims=True)
        t_mat = math.sqrt(MEMBERS - 1) * zm[...] + w_mean
        put(st, t_mat)
        rest = 1.0 - jnp.sum(t_mat, axis=1, keepdims=True)

        def by_channel(group, carry):
            spot = pl.ds(pl.multiple_of(group * GROUP, GROUP), GROUP)
            for part in range(2):
                piece = buf[OWNERS * chunk + group // SUBS, pl.ds((group % SUBS) * GROUP, GROUP), part * 16:part * 16 + 16]
                moved = dot(perm_ref[...], piece.reshape(256, PATCH)).astype(BF16)
                work[part * 16:part * 16 + 16, spot] = moved.reshape(16, 16, PATCH)
            return carry

        lax.fori_loop(0, MEMBERS // GROUP, by_channel, 0)

        def transform(c, carry):
            states = work[c]
            moved = dot(st[2], states) + dot(st[1], states) + dot(st[0], states)
            work[c] = (moved + rest * xbar[pl.ds(c, 1)]).astype(BF16)
            return carry

        lax.fori_loop(0, CHANS, transform, 0)

        for t in range(1, OWNERS):
            f_copy(chunk, t, 0, MINE).wait_send()

        @pl.when(chunk == 0)
        def _():
            pl.semaphore_wait(ready, OWNERS - 1)

        for t in (2, 1, 3, 0):
            def by_member(index, carry):
                spot = pl.ds(pl.multiple_of(((me + t) % OWNERS) * MINE + index * GROUP, GROUP), GROUP)
                for part in range(2):
                    piece = work[part * 16:part * 16 + 16, spot]
                    moved = dot(perm_ref[...], piece.reshape(256, PATCH)).astype(BF16).reshape(16, 16, PATCH)
                    if t == 0:
                        own_row, own_span = place(chunk, me)
                        xbuf[pl.ds(index * GROUP, GROUP), own_row, part * 16:part * 16 + 16, own_span] = moved
                    else:
                        buf[STAGE + 3 * chunk + t - 1, pl.ds(index * GROUP, GROUP), part * 16:part * 16 + 16] = moved
                return carry

            lax.fori_loop(0, SUBS, by_member, 0)
            if t:
                r_copy(chunk, t, me).start()
        return carry

    lax.fori_loop(0, CHUNKS, analyse, 0)

    def finish(chunk, carry):
        for t in range(1, OWNERS):
            r_copy(chunk, t, (me + t) % OWNERS).wait_recv()
            r_copy(chunk, t, me).wait_send()
        edge_copy(chunk).wait_send()
        return carry

    lax.fori_loop(0, CHUNKS, finish, 0)

    @pl.when(lat > 0)
    def _():
        send_up.wait_send()

    @pl.when(lat < lat_count - 1)
    def _():
        send_down.wait_send()


def store_kernel(held, out_ref, sems):
    size = MINE // ROWS
    copies = [pltpu.make_async_copy(held.at[part * size:part * size + size, 1:ROWS + 1], out_ref.at[part * size:part * size + size], sems.at[part])
              for part in range(ROWS)]
    for copy in copies:
        copy.start()
    for copy in copies:
        copy.wait()


def solution(mesh):
    lat_count = mesh.shape['lat']
    dom_count = mesh.shape['dom']

    def local_cycle(ens_block, w_in, w_out, obs_op, obs_val, obs_wt):
        state = jnp.transpose(ens_block, (0, 1, 3, 2))
        vmem = pl.BlockSpec(memory_space=pltpu.VMEM)
        hbm = pl.BlockSpec(memory_space=pl.ANY)
        held = pl.pallas_call(
            functools.partial(kernel, lat_count, dom_count),
            out_shape=pltpu.VMEM((MINE, ROWS + 2, CHANS, COLS), BF16),
            in_specs=[hbm] * 6,
            out_specs=vmem,
            scratch_shapes=[
                pltpu.VMEM((STAGE + 3 * CHUNKS, MINE, CHANS, PATCH), BF16),
                pltpu.VMEM((2 * CHANS, 128), BF16),
                pltpu.VMEM((CHANS, 128), BF16),
                pltpu.VMEM((OBS, CHANS), BF16),
                pltpu.VMEM((128, 2 * CHANS), BF16),
                pltpu.VMEM((8 * OBS, 8 * CHANS), BF16),
                pltpu.VMEM((256, 256), BF16),
                pltpu.VMEM((ROWS, 2, OBS, PATCH), F32),
                pltpu.VMEM((ROWS, 2, OBS, PATCH), F32),
                pltpu.VMEM((CHUNKS, 2, CHANS, 128), BF16),
                pltpu.VMEM((CHUNKS, 2, CHANS, 128), BF16),
                pltpu.VMEM((3 * OBS, MEMBERS, PATCH), BF16),
                pltpu.VMEM((MEMBERS, MEMBERS), F32),
                pltpu.VMEM((MEMBERS, MEMBERS), F32),
                pltpu.VMEM((MEMBERS, MEMBERS), F32),
                pltpu.VMEM((MEMBERS, MEMBERS), F32),
                pltpu.VMEM((3, MEMBERS, MEMBERS), BF16),
                pltpu.VMEM((3, MEMBERS, MEMBERS), BF16),
                pltpu.VMEM((3, MEMBERS, MEMBERS), BF16),
                pltpu.VMEM((CHANS, PATCH), F32),
                pltpu.VMEM((OBS, PATCH), F32),
                pltpu.VMEM((OBS, PATCH), F32),
                pltpu.VMEM((OBS, PATCH), F32),
                pltpu.SemaphoreType.DMA((FIRST // BATCH,)),
                pltpu.SemaphoreType.DMA((4,)),
                pltpu.SemaphoreType.DMA((4,)),
                pltpu.SemaphoreType.DMA((3,)),
                pltpu.SemaphoreType.DMA((2,)),
                pltpu.SemaphoreType.DMA((2,)),
                pltpu.SemaphoreType.DMA((2,)),
                pltpu.SemaphoreType.DMA((CHUNKS,)),
                pltpu.SemaphoreType.DMA((CHUNKS,)),
                pltpu.SemaphoreType.DMA((CHUNKS, 3)),
                pltpu.SemaphoreType.DMA((CHUNKS, OWNERS)),
                pltpu.SemaphoreType.DMA((CHUNKS, 3)),
                pltpu.SemaphoreType.DMA((CHUNKS, OWNERS)),
                pltpu.SemaphoreType.DMA((2,)),
                pltpu.SemaphoreType.REGULAR,
            ],
            compiler_params=pltpu.CompilerParams(collective_id=0, has_side_effects=True, vmem_limit_bytes=43 * 2 ** 20),
        )(w_in, jnp.transpose(w_out), jnp.transpose(obs_op),
          jnp.transpose(obs_val, (0, 1, 3, 2)), jnp.transpose(obs_wt, (0, 1, 3, 2)), state)
        result = pl.pallas_call(
            store_kernel,
            out_shape=jax.ShapeDtypeStruct(state.shape, BF16),
            in_specs=[vmem],
            out_specs=hbm,
            scratch_shapes=[pltpu.SemaphoreType.DMA((ROWS,))],
            compiler_params=pltpu.CompilerParams(vmem_limit_bytes=2 ** 20),
        )(pltpu.with_memory_space_constraint(held, pltpu.VMEM))
        return jnp.transpose(result, (0, 1, 3, 2))

    state_spec = P('ens', 'lat', 'dom', None)
    obs_spec = P('lat', 'dom', None, None)
    return jax.shard_map(local_cycle, mesh=mesh, in_specs=(state_spec, P(), P(), P(), obs_spec, obs_spec), out_specs=state_spec, check_vma=False)
```

```python
import functools
import math

import jax
import jax.numpy as jnp
from jax import lax
from jax.experimental import pallas as pl
from jax.experimental.pallas import tpu as pltpu
from jax.sharding import PartitionSpec as P

NS_STEPS = 12
MESH = pl.DeviceIdType.MESH
F32 = jnp.float32
BF16 = jnp.bfloat16
MEMBERS = 256
MINE = 64
ROWS = 8
COLS = 512
CHANS = 32
PATCH = 256
OBS = 16
CHUNKS = 4
OWNERS = 4
GROUP = 16
BATCH = 4
PACK = 8
STORES = 32
SUBS = MINE // GROUP
FIRST = 16
INNER = 32
STAGE = CHUNKS * OWNERS


def split3(value):
    high = value.astype(BF16)
    rest = value - high.astype(F32)
    mid = rest.astype(BF16)
    low = (rest - mid.astype(F32)).astype(BF16)
    return high, mid, low


def dot(a, b):
    return jnp.dot(a, b, preferred_element_type=F32)


def dot_t(a, b):
    return lax.dot_general(a, b, (((1,), (1,)), ((), ())), preferred_element_type=F32)


def dot6(a, b):
    small = dot(a[2][...], b[0][...]) + dot(a[0][...], b[2][...]) + dot(a[1][...], b[1][...])
    return small + dot(a[1][...], b[0][...]) + dot(a[0][...], b[1][...]) + dot(a[0][...], b[0][...])


def chunk_row(chunk, which):
    last = chunk // (CHUNKS - 1)
    return (1 - last) * (1 + 2 * chunk + which) + last * (ROWS - 1) * which


def kernel(lat_count, dom_count, w_in_hbm, w_out_hbm, op_hbm, yo_hbm, wt_hbm, x_ref, xbuf,
           buf, w_in_ref, w2_ref, op_ref, w1_ref, bd_ref, perm_ref, yo_ref, wt_ref, edge_out, edge_in, work, am, pm, zm, cif, sy, sz, st, xbar, ybar, sw_ref, sd_ref,
           first_sem, upper_sem, lower_sem, small_sem, halo_send, halo_recv, halo_local, edge_send, edge_recv, f_send, f_recv, r_send, r_recv, obs_sem, ready):
    me = lax.axis_index('ens')
    lat = lax.axis_index('lat')
    dom = lax.axis_index('dom')
    my_row = me // 2
    my_half = me % 2
    lat_up = (lat + lat_count - 1) % lat_count
    lat_down = (lat + 1) % lat_count
    dom_other = (dom + 1) % dom_count

    def first_copy(index):
        some = pl.ds(index * BATCH, BATCH)
        return pltpu.make_async_copy(x_ref.at[some, 0:4], xbuf.at[some, 1:5], first_sem.at[index])

    def block_copies(start, first_row, sems):
        size = (MINE - start) // 4
        return [pltpu.make_async_copy(x_ref.at[start + size * part:start + size * part + size, first_row:first_row + 4],
                                      xbuf.at[start + size * part:start + size * part + size, first_row + 1:first_row + 5],
                                      sems.at[part]) for part in range(4)]

    upper_copies = block_copies(FIRST, 0, upper_sem)
    lower_copies = block_copies(0, 4, lower_sem)
    small_copies = [pltpu.make_async_copy(source, target, small_sem.at[index]) for index, (source, target) in enumerate(
        ((w_in_hbm, w_in_ref), (w_out_hbm, w2_ref), (op_hbm, op_ref)))]
    obs_copies = [pltpu.make_async_copy(yo_hbm, yo_ref, obs_sem.at[0]), pltpu.make_async_copy(wt_hbm, wt_ref, obs_sem.at[1])]
    first_copy(0).start()
    for copy in small_copies:
        copy.start()
    for index in range(1, FIRST // BATCH):
        first_copy(index).start()

    barrier = pltpu.get_barrier_semaphore()
    for t in range(1, OWNERS):
        pl.semaphore_signal(barrier, inc=1, device_id={'ens': (me + t) % OWNERS}, device_id_type=MESH)
    pl.semaphore_signal(barrier, inc=1, device_id={'lat': lat_up}, device_id_type=MESH)
    pl.semaphore_signal(barrier, inc=1, device_id={'lat': lat_down}, device_id_type=MESH)
    pl.semaphore_signal(barrier, inc=1, device_id={'dom': dom_other}, device_id_type=MESH)

    for copy in small_copies:
        copy.wait()
    w1_ref[...] = w_in_ref[...].astype(F32).T.astype(BF16)

    send_up = pltpu.make_async_remote_copy(x_ref.at[:, 0], xbuf.at[:, ROWS + 1], halo_send.at[0], halo_recv.at[1],
                                           device_id={'lat': lat_up}, device_id_type=MESH)
    send_down = pltpu.make_async_remote_copy(x_ref.at[:, ROWS - 1], xbuf.at[:, 0], halo_send.at[1], halo_recv.at[0],
                                             device_id={'lat': lat_down}, device_id_type=MESH)
    top_copy = pltpu.make_async_copy(x_ref.at[:, 0], xbuf.at[:, 0], halo_local.at[0])
    bottom_copy = pltpu.make_async_copy(x_ref.at[:, ROWS - 1], xbuf.at[:, ROWS + 1], halo_local.at[1])

    lane = lax.broadcasted_iota(jnp.int32, (CHANS, 128), 1)

    def edge_copy(chunk):
        return pltpu.make_async_remote_copy(edge_out.at[chunk], edge_in.at[chunk], edge_send.at[chunk], edge_recv.at[chunk],
                                            device_id={'dom': dom_other}, device_id_type=MESH)

    def pack(chunk):
        def members(index, acc):
            first, last = acc
            for offset in range(PACK):
                m = index * PACK + offset
                for which in range(2):
                    row = chunk_row(chunk, which) + 1
                    spot = lane == which * MINE + m
                    west = xbuf[m, row, :, 0:128].astype(F32)
                    east = xbuf[m, row, :, COLS - 128:COLS].astype(F32)
                    first = jnp.where(spot, west[:, 0:1], first)
                    last = jnp.where(spot, east[:, 127:128], last)
            return first, last

        zero = jnp.zeros((CHANS, 128), F32)
        first, last = lax.fori_loop(0, MINE // PACK, members, (zero, zero))
        edge_out[chunk, 0] = first.astype(BF16)
        edge_out[chunk, 1] = last.astype(BF16)
        edge_copy(chunk).start()

    def f_copy(chunk, t, start, size, kind='all'):
        owner = (me + t) % OWNERS
        source = buf.at[STAGE + 3 * chunk + t - 1, pl.ds(start, size)]
        target = buf.at[OWNERS * chunk + me, pl.ds(start, size)]
        if kind != 'all':
            half = owner % 2 if kind == 'outer' else 1 - owner % 2
            span = pl.ds(pl.multiple_of(half * 128, 128), 128)
            source = source.at[:, :, span]
            target = target.at[:, :, span]
        return pltpu.make_async_remote_copy(source, target, f_send.at[chunk, t - 1], f_recv.at[chunk, me],
                                            device_id={'ens': owner}, device_id_type=MESH)

    def slots_of(chunk):
        slots = []
        for owner in range(OWNERS):
            ahead = (owner - me + OWNERS) % OWNERS
            own = 1 - (ahead + OWNERS - 1) // OWNERS
            slots.append(own * (OWNERS * chunk + me) + (1 - own) * (STAGE + 3 * chunk + ahead - 1))
        return slots

    pieces_of = {'all': (PATCH, ((0, 0, 0), (PATCH, 0, 1))),
                 'inner': (128, ((128, 128, 0), (PATCH, 0, 1))),
                 'outer': (128, ((0, 0, 0), (PATCH + 128, 128, 1)))}

    def members(chunk, start, size, kind):
        width, pieces = pieces_of[kind]
        slots = slots_of(chunk)
        if kind != 'inner':
            from_east = edge_in[chunk, 0].astype(F32)
            from_west = edge_in[chunk, 1].astype(F32)
        places, features = [], []
        for m in [start + offset for offset in range(size)]:
            for which in range(2):
                row = chunk_row(chunk, which) + 1
                spot = which * MINE + m
                here = xbuf[m, row]
                mid = here.astype(F32)
                above = xbuf[m, row - 1].astype(F32)
                below = xbuf[m, row + 1].astype(F32)
                west = pltpu.roll(mid, 1, 1)
                east = pltpu.roll(mid, COLS - 1, 1)
                if kind != 'inner':
                    halo_west = pltpu.roll(from_west, (128 - spot) % 128, 1)
                    halo_east = pltpu.roll(from_east, 127 - spot, 1)
                    west = jnp.concatenate([jnp.where(lane == 0, halo_west, west[:, :128]), west[:, 128:]], axis=1)
                    east = jnp.concatenate([east[:, :COLS - 128], jnp.where(lane == 127, halo_east, east[:, COLS - 128:])], axis=1)
                laplace = (above + below + west + east - 4.0 * mid).astype(BF16)
                for column, first_lane, half in pieces:
                    span = slice(column, column + width)
                    features.append(jnp.concatenate([here[:, span], laplace[:, span]], axis=0))
                    places.append((row, m, span, slice(first_lane, first_lane + width), slots[2 * which + half]))
        pre_act = dot(w1_ref[...], jnp.concatenate(features, axis=1))
        hidden = (0.5 * pre_act * (1.0 + lax.erf(pre_act * math.sqrt(0.5)))).astype(BF16)
        update = dot(w2_ref[...], hidden)
        for unit, (row, m, span, lanes, slot) in enumerate(places):
            part = update[:, unit * width:(unit + 1) * width]
            buf[slot, m, :, lanes] = (xbuf[m, row, :, span].astype(F32) + part).astype(BF16)

    def send(chunk, start, size, kind):
        for t in (2, 1, 3):
            f_copy(chunk, t, start, size, kind).start()

    def forecast(chunk, start, stop, kind):
        def step(index, carry):
            if kind == 'inner' and start == BATCH:
                first_copy(index).wait()
            members(chunk, index * BATCH, BATCH, kind)
            send(chunk, index * BATCH, BATCH, kind)
            return carry

        lax.fori_loop(start // BATCH, stop // BATCH, step, 0)

    first_copy(0).wait()
    members(0, 0, BATCH // 2, 'inner')
    pl.semaphore_wait(barrier, OWNERS + 2)
    send(0, 0, BATCH // 2, 'inner')
    for copy in upper_copies:
        copy.start()
    members(0, BATCH // 2, BATCH // 2, 'inner')
    send(0, BATCH // 2, BATCH // 2, 'inner')
    forecast(0, BATCH, FIRST, 'inner')
    for copy in upper_copies:
        copy.wait()
    for copy in lower_copies:
        copy.start()
    for copy in obs_copies:
        copy.start()
    pack(0)

    @pl.when(lat > 0)
    def _():
        send_up.start()

    @pl.when(lat < lat_count - 1)
    def _():
        send_down.start()

    @pl.when(lat == 0)
    def _():
        top_copy.start()

    @pl.when(lat == lat_count - 1)
    def _():
        bottom_copy.start()

    forecast(0, FIRST, INNER, 'inner')
    edge_copy(0).wait_recv()
    forecast(0, 0, INNER, 'outer')
    forecast(0, INNER, MINE, 'all')
    for copy in lower_copies:
        copy.wait()
    pack(1)

    def forecast_chunk(chunk, carry):
        edge_copy(chunk).wait_recv()

        @pl.when((chunk == CHUNKS - 1) & (lat > 0))
        def _():
            send_down.wait_recv()

        @pl.when((chunk == CHUNKS - 1) & (lat == 0))
        def _():
            top_copy.wait()

        @pl.when((chunk == CHUNKS - 1) & (lat < lat_count - 1))
        def _():
            send_up.wait_recv()

        @pl.when((chunk == CHUNKS - 1) & (lat == lat_count - 1))
        def _():
            bottom_copy.wait()

        @pl.when(chunk < CHUNKS - 1)
        def _():
            pack(chunk + 1)

        forecast(chunk, 0, MINE, 'all')
        return carry

    lax.fori_loop(1, CHUNKS, forecast_chunk, 0)

    chan_id = lax.broadcasted_iota(jnp.int32, (CHANS, 8 * CHANS), 0)
    slot_id = lax.broadcasted_iota(jnp.int32, (CHANS, 8 * CHANS), 1)
    repeat = jnp.where(chan_id == slot_id % CHANS, 1.0, 0.0).astype(BF16)
    wide = jnp.broadcast_to(dot(op_ref[...], repeat)[:, None, :], (OBS, 8, 8 * CHANS))
    copy_id = lax.broadcasted_iota(jnp.int32, (OBS, 8, 8 * CHANS), 1)
    place_id = lax.broadcasted_iota(jnp.int32, (OBS, 8, 8 * CHANS), 2)
    bd_ref[...] = jnp.where(copy_id == place_id // CHANS, wide, 0.0).reshape(8 * OBS, 8 * CHANS).astype(BF16)
    row_id = lax.broadcasted_iota(jnp.int32, (MEMBERS, MEMBERS), 0)
    col_id = lax.broadcasted_iota(jnp.int32, (MEMBERS, MEMBERS), 1)
    perm_ref[...] = jnp.where((row_id // 16 == col_id % 16) & (row_id % 16 == col_id // 16), 1.0, 0.0).astype(BF16)
    for t in range(1, OWNERS):
        pl.semaphore_signal(ready, inc=1, device_id={'ens': (me + t) % OWNERS}, device_id_type=MESH)
    for copy in obs_copies:
        copy.wait()

    def place(chunk, owner):
        return chunk_row(chunk, owner // 2) + 1, pl.ds(pl.multiple_of((owner % 2) * PATCH, PATCH), PATCH)

    def r_copy(chunk, t, source):
        row, span = place(chunk, source)
        return pltpu.make_async_remote_copy(
            buf.at[STAGE + 3 * chunk + t - 1], xbuf.at[:, row, :, span], r_send.at[chunk, t - 1], r_recv.at[chunk, source],
            device_id={'ens': (me + t) % OWNERS}, device_id_type=MESH)

    def analyse(chunk, carry):
        for t in range(1, OWNERS):
            source = (me + t) % OWNERS
            pltpu.make_async_remote_copy(
                buf.at[STAGE], buf.at[OWNERS * chunk + source], f_send.at[chunk, 0], f_recv.at[chunk, source],
                device_id={'ens': source}, device_id_type=MESH).wait_recv()
        row = chunk_row(chunk, my_row)

        def block(group):
            return buf[OWNERS * chunk + group // SUBS, pl.ds((group % SUBS) * GROUP, GROUP)]

        def sums(group, acc):
            x_sum, y_sum = acc
            states = block(group)
            x_sum = x_sum + jnp.sum(states.astype(F32), axis=0)
            for part in range(2):
                y_sum = y_sum + dot(bd_ref[...], states[part * 8:part * 8 + 8].reshape(8 * CHANS, PATCH))
            return x_sum, y_sum

        x_sum, y_sum = lax.fori_loop(0, MEMBERS // GROUP, sums,
                                     (jnp.zeros((CHANS, PATCH), F32), jnp.zeros((8 * OBS, PATCH), F32)))
        xbar[...] = x_sum * (1.0 / MEMBERS)
        y_mean = jnp.sum(y_sum.reshape(OBS, 8, PATCH), axis=1) * (1.0 / MEMBERS)
        ybar[...] = y_mean
        root_wt = jnp.sqrt(wt_ref[row, my_half])
        sw_ref[...] = root_wt
        sd_ref[...] = root_wt * (yo_ref[row, my_half] - y_mean)

        def anomalies(group, carry):
            states = block(group)
            y_parts = [dot(bd_ref[...], states[part * 8:part * 8 + 8].reshape(8 * CHANS, PATCH)) for part in range(2)]
            spot = pl.ds(pl.multiple_of(group * GROUP, GROUP), GROUP)
            c_innov = jnp.zeros((GROUP, PATCH), F32)
            for o in range(OBS):
                y = jnp.concatenate([y_parts[0][o * 8:o * 8 + 8], y_parts[1][o * 8:o * 8 + 8]], axis=0)
                scaled = (y - ybar[o:o + 1]) * sw_ref[o:o + 1]
                c_innov = c_innov + scaled * sd_ref[o:o + 1]
                high, mid, low = split3(scaled)
                work[o, spot] = high
                work[OBS + o, spot] = mid
                work[2 * OBS + o, spot] = low
            cif[spot] = c_innov
            return carry

        lax.fori_loop(0, MEMBERS // GROUP, anomalies, 0)

        am[...] = jnp.zeros((MEMBERS, MEMBERS), F32)
        pm[...] = jnp.zeros((MEMBERS, MEMBERS), F32)

        def gram(o, carry):
            high = work[o]
            mid = work[OBS + o]
            pm[...] += dot_t(high, mid) + dot_t(high, work[2 * OBS + o])
            am[...] += dot_t(mid, mid) + dot_t(high, high)
            return carry

        lax.fori_loop(0, OBS, gram, 0)
        eye = jnp.where(row_id == col_id, 1.0, 0.0).astype(F32)
        cross = pm[...]
        a_mat = (MEMBERS - 1) * eye + (am[...] + (cross + cross.T))
        scale = jnp.sqrt(jnp.sum(jnp.sum(a_mat * a_mat, axis=0, keepdims=True), axis=1, keepdims=True))

        def put(refs, value):
            for index, part in enumerate(split3(value)):
                refs[index] = part

        def parts(refs):
            return [refs.at[index] for index in range(3)]

        put(sy, a_mat / scale)
        put(sz, eye)

        def newton(step, carry):
            unit = jnp.where(row_id == col_id, 1.5, 0.0).astype(F32)
            put(st, unit - 0.5 * dot6(parts(sz), parts(sy)))
            put(sy, dot6(parts(sy), parts(st)))
            z_next = dot6(parts(st), parts(sz))
            zm[...] = z_next
            put(sz, z_next)
            return carry

        lax.fori_loop(0, NS_STEPS, newton, 0)
        s_mat = zm[...] / jnp.sqrt(scale)
        zm[...] = s_mat
        put(sz, s_mat)
        pa_mat = dot6(parts(sz), parts(sz))
        c_innov = jnp.sum(cif[...], axis=1, keepdims=True)
        w_mean = jnp.sum(pa_mat * c_innov, axis=0, keepdims=True)
        t_mat = math.sqrt(MEMBERS - 1) * zm[...] + w_mean
        put(st, t_mat)
        rest = 1.0 - jnp.sum(t_mat, axis=1, keepdims=True)

        def by_channel(group, carry):
            spot = pl.ds(pl.multiple_of(group * GROUP, GROUP), GROUP)
            for part in range(2):
                piece = buf[OWNERS * chunk + group // SUBS, pl.ds((group % SUBS) * GROUP, GROUP), part * 16:part * 16 + 16]
                moved = dot(perm_ref[...], piece.reshape(256, PATCH)).astype(BF16)
                work[part * 16:part * 16 + 16, spot] = moved.reshape(16, 16, PATCH)
            return carry

        lax.fori_loop(0, MEMBERS // GROUP, by_channel, 0)

        def transform(c, carry):
            states = work[c]
            moved = dot(st[2], states) + dot(st[1], states) + dot(st[0], states)
            work[c] = (moved + rest * xbar[pl.ds(c, 1)]).astype(BF16)
            return carry

        lax.fori_loop(0, CHANS, transform, 0)

        for t in range(1, OWNERS):
            f_copy(chunk, t, 0, MINE).wait_send()

        @pl.when(chunk == 0)
        def _():
            pl.semaphore_wait(ready, OWNERS - 1)

        for t in (2, 1, 3, 0):
            def by_member(index, carry):
                spot = pl.ds(pl.multiple_of(((me + t) % OWNERS) * MINE + index * GROUP, GROUP), GROUP)
                for part in range(2):
                    piece = work[part * 16:part * 16 + 16, spot]
                    moved = dot(perm_ref[...], piece.reshape(256, PATCH)).astype(BF16).reshape(16, 16, PATCH)
                    if t == 0:
                        own_row, own_span = place(chunk, me)
                        xbuf[pl.ds(index * GROUP, GROUP), own_row, part * 16:part * 16 + 16, own_span] = moved
                    else:
                        buf[STAGE + 3 * chunk + t - 1, pl.ds(index * GROUP, GROUP), part * 16:part * 16 + 16] = moved
                return carry

            lax.fori_loop(0, SUBS, by_member, 0)
            if t:
                r_copy(chunk, t, me).start()
        return carry

    lax.fori_loop(0, CHUNKS, analyse, 0)

    def finish(chunk, carry):
        for t in range(1, OWNERS):
            r_copy(chunk, t, (me + t) % OWNERS).wait_recv()
            r_copy(chunk, t, me).wait_send()
        edge_copy(chunk).wait_send()
        return carry

    lax.fori_loop(0, CHUNKS, finish, 0)

    @pl.when(lat > 0)
    def _():
        send_up.wait_send()

    @pl.when(lat < lat_count - 1)
    def _():
        send_down.wait_send()


def store_kernel(held, out_ref, sems):
    size = MINE // STORES
    copies = [pltpu.make_async_copy(held.at[part * size:part * size + size, 1:ROWS + 1], out_ref.at[part * size:part * size + size], sems.at[part])
              for part in range(STORES)]
    for copy in copies:
        copy.start()
    for copy in copies:
        copy.wait()


def solution(mesh):
    lat_count = mesh.shape['lat']
    dom_count = mesh.shape['dom']

    def local_cycle(ens_block, w_in, w_out, obs_op, obs_val, obs_wt):
        state = jnp.transpose(ens_block, (0, 1, 3, 2))
        vmem = pl.BlockSpec(memory_space=pltpu.VMEM)
        hbm = pl.BlockSpec(memory_space=pl.ANY)
        held = pl.pallas_call(
            functools.partial(kernel, lat_count, dom_count),
            out_shape=pltpu.VMEM((MINE, ROWS + 2, CHANS, COLS), BF16),
            in_specs=[hbm] * 6,
            out_specs=vmem,
            scratch_shapes=[
                pltpu.VMEM((STAGE + 3 * CHUNKS, MINE, CHANS, PATCH), BF16),
                pltpu.VMEM((2 * CHANS, 128), BF16),
                pltpu.VMEM((CHANS, 128), BF16),
                pltpu.VMEM((OBS, CHANS), BF16),
                pltpu.VMEM((128, 2 * CHANS), BF16),
                pltpu.VMEM((8 * OBS, 8 * CHANS), BF16),
                pltpu.VMEM((256, 256), BF16),
                pltpu.VMEM((ROWS, 2, OBS, PATCH), F32),
                pltpu.VMEM((ROWS, 2, OBS, PATCH), F32),
                pltpu.VMEM((CHUNKS, 2, CHANS, 128), BF16),
                pltpu.VMEM((CHUNKS, 2, CHANS, 128), BF16),
                pltpu.VMEM((3 * OBS, MEMBERS, PATCH), BF16),
                pltpu.VMEM((MEMBERS, MEMBERS), F32),
                pltpu.VMEM((MEMBERS, MEMBERS), F32),
                pltpu.VMEM((MEMBERS, MEMBERS), F32),
                pltpu.VMEM((MEMBERS, MEMBERS), F32),
                pltpu.VMEM((3, MEMBERS, MEMBERS), BF16),
                pltpu.VMEM((3, MEMBERS, MEMBERS), BF16),
                pltpu.VMEM((3, MEMBERS, MEMBERS), BF16),
                pltpu.VMEM((CHANS, PATCH), F32),
                pltpu.VMEM((OBS, PATCH), F32),
                pltpu.VMEM((OBS, PATCH), F32),
                pltpu.VMEM((OBS, PATCH), F32),
                pltpu.SemaphoreType.DMA((FIRST // BATCH,)),
                pltpu.SemaphoreType.DMA((4,)),
                pltpu.SemaphoreType.DMA((4,)),
                pltpu.SemaphoreType.DMA((3,)),
                pltpu.SemaphoreType.DMA((2,)),
                pltpu.SemaphoreType.DMA((2,)),
                pltpu.SemaphoreType.DMA((2,)),
                pltpu.SemaphoreType.DMA((CHUNKS,)),
                pltpu.SemaphoreType.DMA((CHUNKS,)),
                pltpu.SemaphoreType.DMA((CHUNKS, 3)),
                pltpu.SemaphoreType.DMA((CHUNKS, OWNERS)),
                pltpu.SemaphoreType.DMA((CHUNKS, 3)),
                pltpu.SemaphoreType.DMA((CHUNKS, OWNERS)),
                pltpu.SemaphoreType.DMA((2,)),
                pltpu.SemaphoreType.REGULAR,
            ],
            compiler_params=pltpu.CompilerParams(collective_id=0, has_side_effects=True, vmem_limit_bytes=43 * 2 ** 20),
        )(w_in, jnp.transpose(w_out), jnp.transpose(obs_op),
          jnp.transpose(obs_val, (0, 1, 3, 2)), jnp.transpose(obs_wt, (0, 1, 3, 2)), state)
        result = pl.pallas_call(
            store_kernel,
            out_shape=jax.ShapeDtypeStruct(state.shape, BF16),
            in_specs=[vmem],
            out_specs=hbm,
            scratch_shapes=[pltpu.SemaphoreType.DMA((STORES,))],
            compiler_params=pltpu.CompilerParams(vmem_limit_bytes=2 ** 20),
        )(pltpu.with_memory_space_constraint(held, pltpu.VMEM))
        return jnp.transpose(result, (0, 1, 3, 2))

    state_spec = P('ens', 'lat', 'dom', None)
    obs_spec = P('lat', 'dom', None, None)
    return jax.shard_map(local_cycle, mesh=mesh, in_specs=(state_spec, P(), P(), P(), obs_spec, obs_spec), out_specs=state_spec, check_vma=False)
```

```python
import functools
import math

import jax
import jax.numpy as jnp
from jax import lax
from jax.experimental import pallas as pl
from jax.experimental.pallas import tpu as pltpu
from jax.sharding import PartitionSpec as P

NS_STEPS = 12
MESH = pl.DeviceIdType.MESH
F32 = jnp.float32
BF16 = jnp.bfloat16
MEMBERS = 256
MINE = 64
ROWS = 8
COLS = 512
CHANS = 32
PATCH = 256
OBS = 16
CHUNKS = 4
OWNERS = 4
GROUP = 16
BATCH = 4
PACK = 8
STORES = 8
TAIL = 8
MAIN = MINE - TAIL
SUBS = MINE // GROUP
FIRST = 16
INNER = 32
STAGE = CHUNKS * OWNERS


def split3(value):
    high = value.astype(BF16)
    rest = value - high.astype(F32)
    mid = rest.astype(BF16)
    low = (rest - mid.astype(F32)).astype(BF16)
    return high, mid, low


def dot(a, b):
    return jnp.dot(a, b, preferred_element_type=F32)


def dot_t(a, b):
    return lax.dot_general(a, b, (((1,), (1,)), ((), ())), preferred_element_type=F32)


def dot6(a, b):
    small = dot(a[2][...], b[0][...]) + dot(a[0][...], b[2][...]) + dot(a[1][...], b[1][...])
    return small + dot(a[1][...], b[0][...]) + dot(a[0][...], b[1][...]) + dot(a[0][...], b[0][...])


def chunk_row(chunk, which):
    last = chunk // (CHUNKS - 1)
    return (1 - last) * (1 + 2 * chunk + which) + last * (ROWS - 1) * which


def kernel(lat_count, dom_count, w_in_hbm, w_out_hbm, op_hbm, yo_hbm, wt_hbm, x_ref, xbuf, tail_a, tail_b,
           buf, w_in_ref, w2_ref, op_ref, w1_ref, bd_ref, perm_ref, yo_ref, wt_ref, edge_out, edge_in, work, am, pm, zm, cif, sy, sz, st, xbar, ybar, sw_ref, sd_ref,
           first_sem, upper_sem, lower_sem, small_sem, halo_send, halo_recv, halo_local, edge_send, edge_recv, f_send, f_recv, r_send, r_recv, last_send, last_recv, tail_sem, obs_sem, ready):
    me = lax.axis_index('ens')
    lat = lax.axis_index('lat')
    dom = lax.axis_index('dom')
    my_row = me // 2
    my_half = me % 2
    lat_up = (lat + lat_count - 1) % lat_count
    lat_down = (lat + 1) % lat_count
    dom_other = (dom + 1) % dom_count

    def first_copy(index):
        some = pl.ds(index * BATCH, BATCH)
        return pltpu.make_async_copy(x_ref.at[some, 0:4], xbuf.at[some, 1:5], first_sem.at[index])

    def block_copies(start, first_row, sems):
        size = (MINE - start) // 4
        return [pltpu.make_async_copy(x_ref.at[start + size * part:start + size * part + size, first_row:first_row + 4],
                                      xbuf.at[start + size * part:start + size * part + size, first_row + 1:first_row + 5],
                                      sems.at[part]) for part in range(4)]

    upper_copies = block_copies(FIRST, 0, upper_sem)
    lower_copies = block_copies(0, 4, lower_sem)
    small_copies = [pltpu.make_async_copy(source, target, small_sem.at[index]) for index, (source, target) in enumerate(
        ((w_in_hbm, w_in_ref), (w_out_hbm, w2_ref), (op_hbm, op_ref)))]
    obs_copies = [pltpu.make_async_copy(yo_hbm, yo_ref, obs_sem.at[0]), pltpu.make_async_copy(wt_hbm, wt_ref, obs_sem.at[1])]
    first_copy(0).start()
    for copy in small_copies:
        copy.start()
    for index in range(1, FIRST // BATCH):
        first_copy(index).start()

    barrier = pltpu.get_barrier_semaphore()
    for t in range(1, OWNERS):
        pl.semaphore_signal(barrier, inc=1, device_id={'ens': (me + t) % OWNERS}, device_id_type=MESH)
    pl.semaphore_signal(barrier, inc=1, device_id={'lat': lat_up}, device_id_type=MESH)
    pl.semaphore_signal(barrier, inc=1, device_id={'lat': lat_down}, device_id_type=MESH)
    pl.semaphore_signal(barrier, inc=1, device_id={'dom': dom_other}, device_id_type=MESH)

    for copy in small_copies:
        copy.wait()
    w1_ref[...] = w_in_ref[...].astype(F32).T.astype(BF16)

    send_up = pltpu.make_async_remote_copy(x_ref.at[:, 0], xbuf.at[:, ROWS + 1], halo_send.at[0], halo_recv.at[1],
                                           device_id={'lat': lat_up}, device_id_type=MESH)
    send_down = pltpu.make_async_remote_copy(x_ref.at[:, ROWS - 1], xbuf.at[:, 0], halo_send.at[1], halo_recv.at[0],
                                             device_id={'lat': lat_down}, device_id_type=MESH)
    top_copy = pltpu.make_async_copy(x_ref.at[:, 0], xbuf.at[:, 0], halo_local.at[0])
    bottom_copy = pltpu.make_async_copy(x_ref.at[:, ROWS - 1], xbuf.at[:, ROWS + 1], halo_local.at[1])

    lane = lax.broadcasted_iota(jnp.int32, (CHANS, 128), 1)

    def edge_copy(chunk):
        return pltpu.make_async_remote_copy(edge_out.at[chunk], edge_in.at[chunk], edge_send.at[chunk], edge_recv.at[chunk],
                                            device_id={'dom': dom_other}, device_id_type=MESH)

    def pack(chunk):
        def members(index, acc):
            first, last = acc
            for offset in range(PACK):
                m = index * PACK + offset
                for which in range(2):
                    row = chunk_row(chunk, which) + 1
                    spot = lane == which * MINE + m
                    west = xbuf[m, row, :, 0:128].astype(F32)
                    east = xbuf[m, row, :, COLS - 128:COLS].astype(F32)
                    first = jnp.where(spot, west[:, 0:1], first)
                    last = jnp.where(spot, east[:, 127:128], last)
            return first, last

        zero = jnp.zeros((CHANS, 128), F32)
        first, last = lax.fori_loop(0, MINE // PACK, members, (zero, zero))
        edge_out[chunk, 0] = first.astype(BF16)
        edge_out[chunk, 1] = last.astype(BF16)
        edge_copy(chunk).start()

    def f_copy(chunk, t, start, size, kind='all'):
        owner = (me + t) % OWNERS
        source = buf.at[STAGE + 3 * chunk + t - 1, pl.ds(start, size)]
        target = buf.at[OWNERS * chunk + me, pl.ds(start, size)]
        if kind != 'all':
            half = owner % 2 if kind == 'outer' else 1 - owner % 2
            span = pl.ds(pl.multiple_of(half * 128, 128), 128)
            source = source.at[:, :, span]
            target = target.at[:, :, span]
        return pltpu.make_async_remote_copy(source, target, f_send.at[chunk, t - 1], f_recv.at[chunk, me],
                                            device_id={'ens': owner}, device_id_type=MESH)

    def slots_of(chunk):
        slots = []
        for owner in range(OWNERS):
            ahead = (owner - me + OWNERS) % OWNERS
            own = 1 - (ahead + OWNERS - 1) // OWNERS
            slots.append(own * (OWNERS * chunk + me) + (1 - own) * (STAGE + 3 * chunk + ahead - 1))
        return slots

    pieces_of = {'all': (PATCH, ((0, 0, 0), (PATCH, 0, 1))),
                 'inner': (128, ((128, 128, 0), (PATCH, 0, 1))),
                 'outer': (128, ((0, 0, 0), (PATCH + 128, 128, 1)))}

    def members(chunk, start, size, kind):
        width, pieces = pieces_of[kind]
        slots = slots_of(chunk)
        if kind != 'inner':
            from_east = edge_in[chunk, 0].astype(F32)
            from_west = edge_in[chunk, 1].astype(F32)
        places, features = [], []
        for m in [start + offset for offset in range(size)]:
            for which in range(2):
                row = chunk_row(chunk, which) + 1
                spot = which * MINE + m
                here = xbuf[m, row]
                mid = here.astype(F32)
                above = xbuf[m, row - 1].astype(F32)
                below = xbuf[m, row + 1].astype(F32)
                west = pltpu.roll(mid, 1, 1)
                east = pltpu.roll(mid, COLS - 1, 1)
                if kind != 'inner':
                    halo_west = pltpu.roll(from_west, (128 - spot) % 128, 1)
                    halo_east = pltpu.roll(from_east, 127 - spot, 1)
                    west = jnp.concatenate([jnp.where(lane == 0, halo_west, west[:, :128]), west[:, 128:]], axis=1)
                    east = jnp.concatenate([east[:, :COLS - 128], jnp.where(lane == 127, halo_east, east[:, COLS - 128:])], axis=1)
                laplace = (above + below + west + east - 4.0 * mid).astype(BF16)
                for column, first_lane, half in pieces:
                    span = slice(column, column + width)
                    features.append(jnp.concatenate([here[:, span], laplace[:, span]], axis=0))
                    places.append((row, m, span, slice(first_lane, first_lane + width), slots[2 * which + half]))
        pre_act = dot(w1_ref[...], jnp.concatenate(features, axis=1))
        hidden = (0.5 * pre_act * (1.0 + lax.erf(pre_act * math.sqrt(0.5)))).astype(BF16)
        update = dot(w2_ref[...], hidden)
        for unit, (row, m, span, lanes, slot) in enumerate(places):
            part = update[:, unit * width:(unit + 1) * width]
            buf[slot, m, :, lanes] = (xbuf[m, row, :, span].astype(F32) + part).astype(BF16)

    def send(chunk, start, size, kind):
        for t in (2, 1, 3):
            f_copy(chunk, t, start, size, kind).start()

    def forecast(chunk, start, stop, kind):
        def step(index, carry):
            if kind == 'inner' and start == BATCH:
                first_copy(index).wait()
            members(chunk, index * BATCH, BATCH, kind)
            send(chunk, index * BATCH, BATCH, kind)
            return carry

        lax.fori_loop(start // BATCH, stop // BATCH, step, 0)

    first_copy(0).wait()
    members(0, 0, BATCH // 2, 'inner')
    pl.semaphore_wait(barrier, OWNERS + 2)
    send(0, 0, BATCH // 2, 'inner')
    for copy in upper_copies:
        copy.start()
    members(0, BATCH // 2, BATCH // 2, 'inner')
    send(0, BATCH // 2, BATCH // 2, 'inner')
    forecast(0, BATCH, FIRST, 'inner')
    for copy in upper_copies:
        copy.wait()
    for copy in lower_copies:
        copy.start()
    for copy in obs_copies:
        copy.start()
    pack(0)

    @pl.when(lat > 0)
    def _():
        send_up.start()

    @pl.when(lat < lat_count - 1)
    def _():
        send_down.start()

    @pl.when(lat == 0)
    def _():
        top_copy.start()

    @pl.when(lat == lat_count - 1)
    def _():
        bottom_copy.start()

    forecast(0, FIRST, INNER, 'inner')
    edge_copy(0).wait_recv()
    forecast(0, 0, INNER, 'outer')
    forecast(0, INNER, MINE, 'all')
    for copy in lower_copies:
        copy.wait()
    pack(1)

    def forecast_chunk(chunk, carry):
        edge_copy(chunk).wait_recv()

        @pl.when((chunk == CHUNKS - 1) & (lat > 0))
        def _():
            send_down.wait_recv()

        @pl.when((chunk == CHUNKS - 1) & (lat == 0))
        def _():
            top_copy.wait()

        @pl.when((chunk == CHUNKS - 1) & (lat < lat_count - 1))
        def _():
            send_up.wait_recv()

        @pl.when((chunk == CHUNKS - 1) & (lat == lat_count - 1))
        def _():
            bottom_copy.wait()

        @pl.when(chunk < CHUNKS - 1)
        def _():
            pack(chunk + 1)

        forecast(chunk, 0, MINE, 'all')
        return carry

    lax.fori_loop(1, CHUNKS, forecast_chunk, 0)

    chan_id = lax.broadcasted_iota(jnp.int32, (CHANS, 8 * CHANS), 0)
    slot_id = lax.broadcasted_iota(jnp.int32, (CHANS, 8 * CHANS), 1)
    repeat = jnp.where(chan_id == slot_id % CHANS, 1.0, 0.0).astype(BF16)
    wide = jnp.broadcast_to(dot(op_ref[...], repeat)[:, None, :], (OBS, 8, 8 * CHANS))
    copy_id = lax.broadcasted_iota(jnp.int32, (OBS, 8, 8 * CHANS), 1)
    place_id = lax.broadcasted_iota(jnp.int32, (OBS, 8, 8 * CHANS), 2)
    bd_ref[...] = jnp.where(copy_id == place_id // CHANS, wide, 0.0).reshape(8 * OBS, 8 * CHANS).astype(BF16)
    row_id = lax.broadcasted_iota(jnp.int32, (MEMBERS, MEMBERS), 0)
    col_id = lax.broadcasted_iota(jnp.int32, (MEMBERS, MEMBERS), 1)
    perm_ref[...] = jnp.where((row_id // 16 == col_id % 16) & (row_id % 16 == col_id // 16), 1.0, 0.0).astype(BF16)
    for t in range(1, OWNERS):
        pl.semaphore_signal(ready, inc=1, device_id={'ens': (me + t) % OWNERS}, device_id_type=MESH)
    for copy in obs_copies:
        copy.wait()

    def place(chunk, owner):
        return chunk_row(chunk, owner // 2) + 1, pl.ds(pl.multiple_of((owner % 2) * PATCH, PATCH), PATCH)

    def r_copy(chunk, t, source):
        row, span = place(chunk, source)
        return pltpu.make_async_remote_copy(
            buf.at[STAGE + 3 * chunk + t - 1, 0:MAIN], xbuf.at[0:MAIN, row, :, span],
            r_send.at[chunk, t - 1], r_recv.at[chunk, source],
            device_id={'ens': (me + t) % OWNERS}, device_id_type=MESH)

    def last_copy(chunk, t, source):
        row, span = place(chunk, source)
        return pltpu.make_async_remote_copy(
            buf.at[STAGE + 3 * chunk + t - 1, MAIN:MINE], xbuf.at[MAIN:MINE, row, :, span],
            last_send.at[chunk, t - 1], last_recv.at[chunk, source],
            device_id={'ens': (me + t) % OWNERS}, device_id_type=MESH)

    def tail_copy(chunk, t):
        source = buf.at[STAGE + 3 * chunk + t - 1, MAIN:MINE]
        return pltpu.make_async_copy(source, tail_a if t == 2 else tail_b, tail_sem.at[0 if t == 2 else 1])

    def leaves(chunk, t):
        crosses = {1: me % 2, 2: 1, 3: 1 - me % 2}[t]
        return (chunk // (CHUNKS - 1)) * crosses == 1

    def analyse(chunk, carry):
        for t in range(1, OWNERS):
            source = (me + t) % OWNERS
            pltpu.make_async_remote_copy(
                buf.at[STAGE], buf.at[OWNERS * chunk + source], f_send.at[chunk, 0], f_recv.at[chunk, source],
                device_id={'ens': source}, device_id_type=MESH).wait_recv()
        row = chunk_row(chunk, my_row)

        def block(group):
            return buf[OWNERS * chunk + group // SUBS, pl.ds((group % SUBS) * GROUP, GROUP)]

        def sums(group, acc):
            x_sum, y_sum = acc
            states = block(group)
            x_sum = x_sum + jnp.sum(states.astype(F32), axis=0)
            for part in range(2):
                y_sum = y_sum + dot(bd_ref[...], states[part * 8:part * 8 + 8].reshape(8 * CHANS, PATCH))
            return x_sum, y_sum

        x_sum, y_sum = lax.fori_loop(0, MEMBERS // GROUP, sums,
                                     (jnp.zeros((CHANS, PATCH), F32), jnp.zeros((8 * OBS, PATCH), F32)))
        xbar[...] = x_sum * (1.0 / MEMBERS)
        y_mean = jnp.sum(y_sum.reshape(OBS, 8, PATCH), axis=1) * (1.0 / MEMBERS)
        ybar[...] = y_mean
        root_wt = jnp.sqrt(wt_ref[row, my_half])
        sw_ref[...] = root_wt
        sd_ref[...] = root_wt * (yo_ref[row, my_half] - y_mean)

        def anomalies(group, carry):
            states = block(group)
            y_parts = [dot(bd_ref[...], states[part * 8:part * 8 + 8].reshape(8 * CHANS, PATCH)) for part in range(2)]
            spot = pl.ds(pl.multiple_of(group * GROUP, GROUP), GROUP)
            c_innov = jnp.zeros((GROUP, PATCH), F32)
            for o in range(OBS):
                y = jnp.concatenate([y_parts[0][o * 8:o * 8 + 8], y_parts[1][o * 8:o * 8 + 8]], axis=0)
                scaled = (y - ybar[o:o + 1]) * sw_ref[o:o + 1]
                c_innov = c_innov + scaled * sd_ref[o:o + 1]
                high, mid, low = split3(scaled)
                work[o, spot] = high
                work[OBS + o, spot] = mid
                work[2 * OBS + o, spot] = low
            cif[spot] = c_innov
            return carry

        lax.fori_loop(0, MEMBERS // GROUP, anomalies, 0)

        am[...] = jnp.zeros((MEMBERS, MEMBERS), F32)
        pm[...] = jnp.zeros((MEMBERS, MEMBERS), F32)

        def gram(o, carry):
            high = work[o]
            mid = work[OBS + o]
            pm[...] += dot_t(high, mid) + dot_t(high, work[2 * OBS + o])
            am[...] += dot_t(mid, mid) + dot_t(high, high)
            return carry

        lax.fori_loop(0, OBS, gram, 0)
        eye = jnp.where(row_id == col_id, 1.0, 0.0).astype(F32)
        cross = pm[...]
        a_mat = (MEMBERS - 1) * eye + (am[...] + (cross + cross.T))
        scale = jnp.sqrt(jnp.sum(jnp.sum(a_mat * a_mat, axis=0, keepdims=True), axis=1, keepdims=True))

        def put(refs, value):
            for index, part in enumerate(split3(value)):
                refs[index] = part

        def parts(refs):
            return [refs.at[index] for index in range(3)]

        put(sy, a_mat / scale)
        put(sz, eye)

        def newton(step, carry):
            unit = jnp.where(row_id == col_id, 1.5, 0.0).astype(F32)
            put(st, unit - 0.5 * dot6(parts(sz), parts(sy)))
            put(sy, dot6(parts(sy), parts(st)))
            z_next = dot6(parts(st), parts(sz))
            zm[...] = z_next
            put(sz, z_next)
            return carry

        lax.fori_loop(0, NS_STEPS, newton, 0)
        s_mat = zm[...] / jnp.sqrt(scale)
        zm[...] = s_mat
        put(sz, s_mat)
        pa_mat = dot6(parts(sz), parts(sz))
        c_innov = jnp.sum(cif[...], axis=1, keepdims=True)
        w_mean = jnp.sum(pa_mat * c_innov, axis=0, keepdims=True)
        t_mat = math.sqrt(MEMBERS - 1) * zm[...] + w_mean
        put(st, t_mat)
        rest = 1.0 - jnp.sum(t_mat, axis=1, keepdims=True)

        def by_channel(group, carry):
            spot = pl.ds(pl.multiple_of(group * GROUP, GROUP), GROUP)
            for part in range(2):
                piece = buf[OWNERS * chunk + group // SUBS, pl.ds((group % SUBS) * GROUP, GROUP), part * 16:part * 16 + 16]
                moved = dot(perm_ref[...], piece.reshape(256, PATCH)).astype(BF16)
                work[part * 16:part * 16 + 16, spot] = moved.reshape(16, 16, PATCH)
            return carry

        lax.fori_loop(0, MEMBERS // GROUP, by_channel, 0)

        def transform(c, carry):
            states = work[c]
            moved = dot(st[2], states) + dot(st[1], states) + dot(st[0], states)
            work[c] = (moved + rest * xbar[pl.ds(c, 1)]).astype(BF16)
            return carry

        lax.fori_loop(0, CHANS, transform, 0)

        for t in range(1, OWNERS):
            f_copy(chunk, t, 0, MINE).wait_send()

        @pl.when(chunk == 0)
        def _():
            pl.semaphore_wait(ready, OWNERS - 1)

        for t in (2, 1, 3, 0):
            def by_member(index, carry):
                spot = pl.ds(pl.multiple_of(((me + t) % OWNERS) * MINE + index * GROUP, GROUP), GROUP)
                for part in range(2):
                    piece = work[part * 16:part * 16 + 16, spot]
                    moved = dot(perm_ref[...], piece.reshape(256, PATCH)).astype(BF16).reshape(16, 16, PATCH)
                    if t == 0:
                        own_row, own_span = place(chunk, me)
                        xbuf[pl.ds(index * GROUP, GROUP), own_row, part * 16:part * 16 + 16, own_span] = moved
                    else:
                        buf[STAGE + 3 * chunk + t - 1, pl.ds(index * GROUP, GROUP), part * 16:part * 16 + 16] = moved
                return carry

            lax.fori_loop(0, SUBS, by_member, 0)
            if t:
                r_copy(chunk, t, me).start()

                @pl.when(leaves(chunk, t))
                def _():
                    tail_copy(chunk, t).start()

                @pl.when(jnp.logical_not(leaves(chunk, t)))
                def _():
                    last_copy(chunk, t, me).start()
        return carry

    lax.fori_loop(0, CHUNKS, analyse, 0)

    def finish(chunk, carry):
        for t in range(1, OWNERS):
            r_copy(chunk, t, (me + t) % OWNERS).wait_recv()
            r_copy(chunk, t, me).wait_send()

            @pl.when(leaves(chunk, t))
            def _():
                tail_copy(chunk, t).wait()

            @pl.when(jnp.logical_not(leaves(chunk, t)))
            def _():
                last_copy(chunk, t, (me + t) % OWNERS).wait_recv()
                last_copy(chunk, t, me).wait_send()
        edge_copy(chunk).wait_send()
        return carry

    lax.fori_loop(0, CHUNKS, finish, 0)

    @pl.when(lat > 0)
    def _():
        send_up.wait_send()

    @pl.when(lat < lat_count - 1)
    def _():
        send_down.wait_send()


def store_kernel(held, out_ref, sems):
    size = MINE // STORES
    copies = [pltpu.make_async_copy(held.at[part * size:part * size + size, 1:ROWS + 1], out_ref.at[part * size:part * size + size], sems.at[part])
              for part in range(STORES)]
    for copy in copies:
        copy.start()
    for copy in copies:
        copy.wait()


def join_kernel(whole, piece_a, piece_b, out_ref, sems):
    me = lax.axis_index('ens')
    copies = []
    for index, (piece, source) in enumerate(((piece_a, (me + 2) % OWNERS), (piece_b, OWNERS - 1 - me))):
        span = pl.ds(pl.multiple_of((source % 2) * PATCH, PATCH), PATCH)
        row = chunk_row(CHUNKS - 1, source // 2)
        copies.append(pltpu.make_async_copy(piece, out_ref.at[MAIN:MINE, row, :, span], sems.at[index]))
    for copy in copies:
        copy.start()
    for copy in copies:
        copy.wait()


def solution(mesh):
    lat_count = mesh.shape['lat']
    dom_count = mesh.shape['dom']

    def local_cycle(ens_block, w_in, w_out, obs_op, obs_val, obs_wt):
        state = jnp.transpose(ens_block, (0, 1, 3, 2))
        vmem = pl.BlockSpec(memory_space=pltpu.VMEM)
        hbm = pl.BlockSpec(memory_space=pl.ANY)
        tail = jax.ShapeDtypeStruct((TAIL, CHANS, PATCH), BF16)
        held, tail_a, tail_b = pl.pallas_call(
            functools.partial(kernel, lat_count, dom_count),
            out_shape=(pltpu.VMEM((MINE, ROWS + 2, CHANS, COLS), BF16), tail, tail),
            in_specs=[hbm] * 6,
            out_specs=(vmem, hbm, hbm),
            scratch_shapes=[
                pltpu.VMEM((STAGE + 3 * CHUNKS, MINE, CHANS, PATCH), BF16),
                pltpu.VMEM((2 * CHANS, 128), BF16),
                pltpu.VMEM((CHANS, 128), BF16),
                pltpu.VMEM((OBS, CHANS), BF16),
                pltpu.VMEM((128, 2 * CHANS), BF16),
                pltpu.VMEM((8 * OBS, 8 * CHANS), BF16),
                pltpu.VMEM((256, 256), BF16),
                pltpu.VMEM((ROWS, 2, OBS, PATCH), F32),
                pltpu.VMEM((ROWS, 2, OBS, PATCH), F32),
                pltpu.VMEM((CHUNKS, 2, CHANS, 128), BF16),
                pltpu.VMEM((CHUNKS, 2, CHANS, 128), BF16),
                pltpu.VMEM((3 * OBS, MEMBERS, PATCH), BF16),
                pltpu.VMEM((MEMBERS, MEMBERS), F32),
                pltpu.VMEM((MEMBERS, MEMBERS), F32),
                pltpu.VMEM((MEMBERS, MEMBERS), F32),
                pltpu.VMEM((MEMBERS, MEMBERS), F32),
                pltpu.VMEM((3, MEMBERS, MEMBERS), BF16),
                pltpu.VMEM((3, MEMBERS, MEMBERS), BF16),
                pltpu.VMEM((3, MEMBERS, MEMBERS), BF16),
                pltpu.VMEM((CHANS, PATCH), F32),
                pltpu.VMEM((OBS, PATCH), F32),
                pltpu.VMEM((OBS, PATCH), F32),
                pltpu.VMEM((OBS, PATCH), F32),
                pltpu.SemaphoreType.DMA((FIRST // BATCH,)),
                pltpu.SemaphoreType.DMA((4,)),
                pltpu.SemaphoreType.DMA((4,)),
                pltpu.SemaphoreType.DMA((3,)),
                pltpu.SemaphoreType.DMA((2,)),
                pltpu.SemaphoreType.DMA((2,)),
                pltpu.SemaphoreType.DMA((2,)),
                pltpu.SemaphoreType.DMA((CHUNKS,)),
                pltpu.SemaphoreType.DMA((CHUNKS,)),
                pltpu.SemaphoreType.DMA((CHUNKS, 3)),
                pltpu.SemaphoreType.DMA((CHUNKS, OWNERS)),
                pltpu.SemaphoreType.DMA((CHUNKS, 3)),
                pltpu.SemaphoreType.DMA((CHUNKS, OWNERS)),
                pltpu.SemaphoreType.DMA((CHUNKS, 3)),
                pltpu.SemaphoreType.DMA((CHUNKS, OWNERS)),
                pltpu.SemaphoreType.DMA((2,)),
                pltpu.SemaphoreType.DMA((2,)),
                pltpu.SemaphoreType.REGULAR,
            ],
            compiler_params=pltpu.CompilerParams(collective_id=0, has_side_effects=True, vmem_limit_bytes=43 * 2 ** 20),
        )(w_in, jnp.transpose(w_out), jnp.transpose(obs_op),
          jnp.transpose(obs_val, (0, 1, 3, 2)), jnp.transpose(obs_wt, (0, 1, 3, 2)), state)
        tail_a = lax.ppermute(tail_a, 'ens', [(i, (i + 2) % OWNERS) for i in range(OWNERS)])
        tail_b = lax.ppermute(tail_b, 'ens', [(i, OWNERS - 1 - i) for i in range(OWNERS)])
        result = pl.pallas_call(
            store_kernel,
            out_shape=jax.ShapeDtypeStruct(state.shape, BF16),
            in_specs=[vmem],
            out_specs=hbm,
            scratch_shapes=[pltpu.SemaphoreType.DMA((STORES,))],
            compiler_params=pltpu.CompilerParams(vmem_limit_bytes=2 ** 20),
            cost_estimate=pl.CostEstimate(flops=0, bytes_accessed=2 * state.size, transcendentals=0),
        )(pltpu.with_memory_space_constraint(held, pltpu.VMEM))
        result = pl.pallas_call(
            join_kernel,
            out_shape=jax.ShapeDtypeStruct(state.shape, BF16),
            in_specs=[hbm, vmem, vmem],
            out_specs=hbm,
            scratch_shapes=[pltpu.SemaphoreType.DMA((2,))],
            input_output_aliases={0: 0},
            compiler_params=pltpu.CompilerParams(vmem_limit_bytes=2 ** 20),
        )(result, tail_a, tail_b)
        return jnp.transpose(result, (0, 1, 3, 2))

    state_spec = P('ens', 'lat', 'dom', None)
    obs_spec = P('lat', 'dom', None, None)
    return jax.shard_map(local_cycle, mesh=mesh, in_specs=(state_spec, P(), P(), P(), obs_spec, obs_spec), out_specs=state_spec, check_vma=False)
```

```python
import functools
import math

import jax
import jax.numpy as jnp
from jax import lax
from jax.experimental import pallas as pl
from jax.experimental.pallas import tpu as pltpu
from jax.sharding import PartitionSpec as P

NS_STEPS = 12
MESH = pl.DeviceIdType.MESH
F32 = jnp.float32
BF16 = jnp.bfloat16
MEMBERS = 256
MINE = 64
ROWS = 8
COLS = 512
CHANS = 32
PATCH = 256
OBS = 16
CHUNKS = 4
OWNERS = 4
GROUP = 16
BATCH = 4
PACK = 8
STORES = 8
TAIL = 10
MAIN = MINE - TAIL
SUBS = MINE // GROUP
FIRST = 16
INNER = 32
STAGE = CHUNKS * OWNERS


def split3(value):
    high = value.astype(BF16)
    rest = value - high.astype(F32)
    mid = rest.astype(BF16)
    low = (rest - mid.astype(F32)).astype(BF16)
    return high, mid, low


def dot(a, b):
    return jnp.dot(a, b, preferred_element_type=F32)


def dot_t(a, b):
    return lax.dot_general(a, b, (((1,), (1,)), ((), ())), preferred_element_type=F32)


def dot6(a, b):
    small = dot(a[2][...], b[0][...]) + dot(a[0][...], b[2][...]) + dot(a[1][...], b[1][...])
    return small + dot(a[1][...], b[0][...]) + dot(a[0][...], b[1][...]) + dot(a[0][...], b[0][...])


def chunk_row(chunk, which):
    last = chunk // (CHUNKS - 1)
    return (1 - last) * (1 + 2 * chunk + which) + last * (ROWS - 1) * which


def kernel(lat_count, dom_count, w_in_hbm, w_out_hbm, op_hbm, yo_hbm, wt_hbm, x_ref, xbuf, tail_a, tail_b,
           buf, w_in_ref, w2_ref, op_ref, w1_ref, bd_ref, perm_ref, yo_ref, wt_ref, edge_out, edge_in, work, am, pm, zm, cif, sy, sz, st, xbar, ybar, sw_ref, sd_ref,
           first_sem, upper_sem, lower_sem, small_sem, halo_send, halo_recv, halo_local, edge_send, edge_recv, f_send, f_recv, r_send, r_recv, last_send, last_recv, obs_sem, ready):
    me = lax.axis_index('ens')
    lat = lax.axis_index('lat')
    dom = lax.axis_index('dom')
    my_row = me // 2
    my_half = me % 2
    lat_up = (lat + lat_count - 1) % lat_count
    lat_down = (lat + 1) % lat_count
    dom_other = (dom + 1) % dom_count

    def first_copy(index):
        some = pl.ds(index * BATCH, BATCH)
        return pltpu.make_async_copy(x_ref.at[some, 0:4], xbuf.at[some, 1:5], first_sem.at[index])

    def block_copies(start, first_row, sems):
        size = (MINE - start) // 4
        return [pltpu.make_async_copy(x_ref.at[start + size * part:start + size * part + size, first_row:first_row + 4],
                                      xbuf.at[start + size * part:start + size * part + size, first_row + 1:first_row + 5],
                                      sems.at[part]) for part in range(4)]

    upper_copies = block_copies(FIRST, 0, upper_sem)
    lower_copies = block_copies(0, 4, lower_sem)
    small_copies = [pltpu.make_async_copy(source, target, small_sem.at[index]) for index, (source, target) in enumerate(
        ((w_in_hbm, w_in_ref), (w_out_hbm, w2_ref), (op_hbm, op_ref)))]
    obs_copies = [pltpu.make_async_copy(yo_hbm, yo_ref, obs_sem.at[0]), pltpu.make_async_copy(wt_hbm, wt_ref, obs_sem.at[1])]
    first_copy(0).start()
    for copy in small_copies:
        copy.start()
    for index in range(1, FIRST // BATCH):
        first_copy(index).start()

    barrier = pltpu.get_barrier_semaphore()
    for t in range(1, OWNERS):
        pl.semaphore_signal(barrier, inc=1, device_id={'ens': (me + t) % OWNERS}, device_id_type=MESH)
    pl.semaphore_signal(barrier, inc=1, device_id={'lat': lat_up}, device_id_type=MESH)
    pl.semaphore_signal(barrier, inc=1, device_id={'lat': lat_down}, device_id_type=MESH)
    pl.semaphore_signal(barrier, inc=1, device_id={'dom': dom_other}, device_id_type=MESH)

    for copy in small_copies:
        copy.wait()
    w1_ref[...] = w_in_ref[...].astype(F32).T.astype(BF16)

    send_up = pltpu.make_async_remote_copy(x_ref.at[:, 0], xbuf.at[:, ROWS + 1], halo_send.at[0], halo_recv.at[1],
                                           device_id={'lat': lat_up}, device_id_type=MESH)
    send_down = pltpu.make_async_remote_copy(x_ref.at[:, ROWS - 1], xbuf.at[:, 0], halo_send.at[1], halo_recv.at[0],
                                             device_id={'lat': lat_down}, device_id_type=MESH)
    top_copy = pltpu.make_async_copy(x_ref.at[:, 0], xbuf.at[:, 0], halo_local.at[0])
    bottom_copy = pltpu.make_async_copy(x_ref.at[:, ROWS - 1], xbuf.at[:, ROWS + 1], halo_local.at[1])

    lane = lax.broadcasted_iota(jnp.int32, (CHANS, 128), 1)

    def edge_copy(chunk):
        return pltpu.make_async_remote_copy(edge_out.at[chunk], edge_in.at[chunk], edge_send.at[chunk], edge_recv.at[chunk],
                                            device_id={'dom': dom_other}, device_id_type=MESH)

    def pack(chunk):
        def members(index, acc):
            first, last = acc
            for offset in range(PACK):
                m = index * PACK + offset
                for which in range(2):
                    row = chunk_row(chunk, which) + 1
                    spot = lane == which * MINE + m
                    west = xbuf[m, row, :, 0:128].astype(F32)
                    east = xbuf[m, row, :, COLS - 128:COLS].astype(F32)
                    first = jnp.where(spot, west[:, 0:1], first)
                    last = jnp.where(spot, east[:, 127:128], last)
            return first, last

        zero = jnp.zeros((CHANS, 128), F32)
        first, last = lax.fori_loop(0, MINE // PACK, members, (zero, zero))
        edge_out[chunk, 0] = first.astype(BF16)
        edge_out[chunk, 1] = last.astype(BF16)
        edge_copy(chunk).start()

    def f_copy(chunk, t, start, size, kind='all'):
        owner = (me + t) % OWNERS
        source = buf.at[STAGE + 3 * chunk + t - 1, pl.ds(start, size)]
        target = buf.at[OWNERS * chunk + me, pl.ds(start, size)]
        if kind != 'all':
            half = owner % 2 if kind == 'outer' else 1 - owner % 2
            span = pl.ds(pl.multiple_of(half * 128, 128), 128)
            source = source.at[:, :, span]
            target = target.at[:, :, span]
        return pltpu.make_async_remote_copy(source, target, f_send.at[chunk, t - 1], f_recv.at[chunk, me],
                                            device_id={'ens': owner}, device_id_type=MESH)

    def slots_of(chunk):
        slots = []
        for owner in range(OWNERS):
            ahead = (owner - me + OWNERS) % OWNERS
            own = 1 - (ahead + OWNERS - 1) // OWNERS
            slots.append(own * (OWNERS * chunk + me) + (1 - own) * (STAGE + 3 * chunk + ahead - 1))
        return slots

    pieces_of = {'all': (PATCH, ((0, 0, 0), (PATCH, 0, 1))),
                 'inner': (128, ((128, 128, 0), (PATCH, 0, 1))),
                 'outer': (128, ((0, 0, 0), (PATCH + 128, 128, 1)))}

    def members(chunk, start, size, kind):
        width, pieces = pieces_of[kind]
        slots = slots_of(chunk)
        if kind != 'inner':
            from_east = edge_in[chunk, 0].astype(F32)
            from_west = edge_in[chunk, 1].astype(F32)
        places, features = [], []
        for m in [start + offset for offset in range(size)]:
            for which in range(2):
                row = chunk_row(chunk, which) + 1
                spot = which * MINE + m
                here = xbuf[m, row]
                mid = here.astype(F32)
                above = xbuf[m, row - 1].astype(F32)
                below = xbuf[m, row + 1].astype(F32)
                west = pltpu.roll(mid, 1, 1)
                east = pltpu.roll(mid, COLS - 1, 1)
                if kind != 'inner':
                    halo_west = pltpu.roll(from_west, (128 - spot) % 128, 1)
                    halo_east = pltpu.roll(from_east, 127 - spot, 1)
                    west = jnp.concatenate([jnp.where(lane == 0, halo_west, west[:, :128]), west[:, 128:]], axis=1)
                    east = jnp.concatenate([east[:, :COLS - 128], jnp.where(lane == 127, halo_east, east[:, COLS - 128:])], axis=1)
                laplace = (above + below + west + east - 4.0 * mid).astype(BF16)
                for column, first_lane, half in pieces:
                    span = slice(column, column + width)
                    features.append(jnp.concatenate([here[:, span], laplace[:, span]], axis=0))
                    places.append((row, m, span, slice(first_lane, first_lane + width), slots[2 * which + half]))
        pre_act = dot(w1_ref[...], jnp.concatenate(features, axis=1))
        hidden = (0.5 * pre_act * (1.0 + lax.erf(pre_act * math.sqrt(0.5)))).astype(BF16)
        update = dot(w2_ref[...], hidden)
        for unit, (row, m, span, lanes, slot) in enumerate(places):
            part = update[:, unit * width:(unit + 1) * width]
            buf[slot, m, :, lanes] = (xbuf[m, row, :, span].astype(F32) + part).astype(BF16)

    def send(chunk, start, size, kind):
        for t in (2, 1, 3):
            f_copy(chunk, t, start, size, kind).start()

    def forecast(chunk, start, stop, kind):
        def step(index, carry):
            if kind == 'inner' and start == BATCH:
                first_copy(index).wait()
            members(chunk, index * BATCH, BATCH, kind)
            send(chunk, index * BATCH, BATCH, kind)
            return carry

        lax.fori_loop(start // BATCH, stop // BATCH, step, 0)

    first_copy(0).wait()
    members(0, 0, BATCH // 2, 'inner')
    pl.semaphore_wait(barrier, OWNERS + 2)
    send(0, 0, BATCH // 2, 'inner')
    for copy in upper_copies:
        copy.start()
    members(0, BATCH // 2, BATCH // 2, 'inner')
    send(0, BATCH // 2, BATCH // 2, 'inner')
    forecast(0, BATCH, FIRST, 'inner')
    for copy in upper_copies:
        copy.wait()
    for copy in lower_copies:
        copy.start()
    for copy in obs_copies:
        copy.start()
    pack(0)

    @pl.when(lat > 0)
    def _():
        send_up.start()

    @pl.when(lat < lat_count - 1)
    def _():
        send_down.start()

    @pl.when(lat == 0)
    def _():
        top_copy.start()

    @pl.when(lat == lat_count - 1)
    def _():
        bottom_copy.start()

    forecast(0, FIRST, INNER, 'inner')
    edge_copy(0).wait_recv()
    forecast(0, 0, INNER, 'outer')
    forecast(0, INNER, MINE, 'all')
    for copy in lower_copies:
        copy.wait()
    pack(1)

    def forecast_chunk(chunk, carry):
        edge_copy(chunk).wait_recv()

        @pl.when((chunk == CHUNKS - 1) & (lat > 0))
        def _():
            send_down.wait_recv()

        @pl.when((chunk == CHUNKS - 1) & (lat == 0))
        def _():
            top_copy.wait()

        @pl.when((chunk == CHUNKS - 1) & (lat < lat_count - 1))
        def _():
            send_up.wait_recv()

        @pl.when((chunk == CHUNKS - 1) & (lat == lat_count - 1))
        def _():
            bottom_copy.wait()

        @pl.when(chunk < CHUNKS - 1)
        def _():
            pack(chunk + 1)

        forecast(chunk, 0, MINE, 'all')
        return carry

    lax.fori_loop(1, CHUNKS, forecast_chunk, 0)

    chan_id = lax.broadcasted_iota(jnp.int32, (CHANS, 8 * CHANS), 0)
    slot_id = lax.broadcasted_iota(jnp.int32, (CHANS, 8 * CHANS), 1)
    repeat = jnp.where(chan_id == slot_id % CHANS, 1.0, 0.0).astype(BF16)
    wide = jnp.broadcast_to(dot(op_ref[...], repeat)[:, None, :], (OBS, 8, 8 * CHANS))
    copy_id = lax.broadcasted_iota(jnp.int32, (OBS, 8, 8 * CHANS), 1)
    place_id = lax.broadcasted_iota(jnp.int32, (OBS, 8, 8 * CHANS), 2)
    bd_ref[...] = jnp.where(copy_id == place_id // CHANS, wide, 0.0).reshape(8 * OBS, 8 * CHANS).astype(BF16)
    row_id = lax.broadcasted_iota(jnp.int32, (MEMBERS, MEMBERS), 0)
    col_id = lax.broadcasted_iota(jnp.int32, (MEMBERS, MEMBERS), 1)
    perm_ref[...] = jnp.where((row_id // 16 == col_id % 16) & (row_id % 16 == col_id // 16), 1.0, 0.0).astype(BF16)
    for t in range(1, OWNERS):
        pl.semaphore_signal(ready, inc=1, device_id={'ens': (me + t) % OWNERS}, device_id_type=MESH)
    for copy in obs_copies:
        copy.wait()

    def place(chunk, owner):
        return chunk_row(chunk, owner // 2) + 1, pl.ds(pl.multiple_of((owner % 2) * PATCH, PATCH), PATCH)

    def r_copy(chunk, t, source):
        row, span = place(chunk, source)
        return pltpu.make_async_remote_copy(
            buf.at[STAGE + 3 * chunk + t - 1, 0:MAIN], xbuf.at[0:MAIN, row, :, span],
            r_send.at[chunk, t - 1], r_recv.at[chunk, source],
            device_id={'ens': (me + t) % OWNERS}, device_id_type=MESH)

    def last_copy(chunk, t, source):
        row, span = place(chunk, source)
        return pltpu.make_async_remote_copy(
            buf.at[STAGE + 3 * chunk + t - 1, MAIN:MINE], xbuf.at[MAIN:MINE, row, :, span],
            last_send.at[chunk, t - 1], last_recv.at[chunk, source],
            device_id={'ens': (me + t) % OWNERS}, device_id_type=MESH)

    def leaves(chunk, t):
        crosses = {1: me % 2, 2: 1, 3: 1 - me % 2}[t]
        return (chunk // (CHUNKS - 1)) * crosses == 1

    def analyse(chunk, carry):
        for t in range(1, OWNERS):
            source = (me + t) % OWNERS
            pltpu.make_async_remote_copy(
                buf.at[STAGE], buf.at[OWNERS * chunk + source], f_send.at[chunk, 0], f_recv.at[chunk, source],
                device_id={'ens': source}, device_id_type=MESH).wait_recv()
        row = chunk_row(chunk, my_row)

        def block(group):
            return buf[OWNERS * chunk + group // SUBS, pl.ds((group % SUBS) * GROUP, GROUP)]

        def sums(group, acc):
            x_sum, y_sum = acc
            states = block(group)
            x_sum = x_sum + jnp.sum(states.astype(F32), axis=0)
            for part in range(2):
                y_sum = y_sum + dot(bd_ref[...], states[part * 8:part * 8 + 8].reshape(8 * CHANS, PATCH))
            return x_sum, y_sum

        x_sum, y_sum = lax.fori_loop(0, MEMBERS // GROUP, sums,
                                     (jnp.zeros((CHANS, PATCH), F32), jnp.zeros((8 * OBS, PATCH), F32)))
        xbar[...] = x_sum * (1.0 / MEMBERS)
        y_mean = jnp.sum(y_sum.reshape(OBS, 8, PATCH), axis=1) * (1.0 / MEMBERS)
        ybar[...] = y_mean
        root_wt = jnp.sqrt(wt_ref[row, my_half])
        sw_ref[...] = root_wt
        sd_ref[...] = root_wt * (yo_ref[row, my_half] - y_mean)

        def anomalies(group, carry):
            states = block(group)
            y_parts = [dot(bd_ref[...], states[part * 8:part * 8 + 8].reshape(8 * CHANS, PATCH)) for part in range(2)]
            spot = pl.ds(pl.multiple_of(group * GROUP, GROUP), GROUP)
            c_innov = jnp.zeros((GROUP, PATCH), F32)
            for o in range(OBS):
                y = jnp.concatenate([y_parts[0][o * 8:o * 8 + 8], y_parts[1][o * 8:o * 8 + 8]], axis=0)
                scaled = (y - ybar[o:o + 1]) * sw_ref[o:o + 1]
                c_innov = c_innov + scaled * sd_ref[o:o + 1]
                high, mid, low = split3(scaled)
                work[o, spot] = high
                work[OBS + o, spot] = mid
                work[2 * OBS + o, spot] = low
            cif[spot] = c_innov
            return carry

        lax.fori_loop(0, MEMBERS // GROUP, anomalies, 0)

        am[...] = jnp.zeros((MEMBERS, MEMBERS), F32)
        pm[...] = jnp.zeros((MEMBERS, MEMBERS), F32)

        def gram(o, carry):
            high = work[o]
            mid = work[OBS + o]
            pm[...] += dot_t(high, mid) + dot_t(high, work[2 * OBS + o])
            am[...] += dot_t(mid, mid) + dot_t(high, high)
            return carry

        lax.fori_loop(0, OBS, gram, 0)
        eye = jnp.where(row_id == col_id, 1.0, 0.0).astype(F32)
        cross = pm[...]
        a_mat = (MEMBERS - 1) * eye + (am[...] + (cross + cross.T))
        scale = jnp.sqrt(jnp.sum(jnp.sum(a_mat * a_mat, axis=0, keepdims=True), axis=1, keepdims=True))

        def put(refs, value):
            for index, part in enumerate(split3(value)):
                refs[index] = part

        def parts(refs):
            return [refs.at[index] for index in range(3)]

        put(sy, a_mat / scale)
        put(sz, eye)

        def newton(step, carry):
            unit = jnp.where(row_id == col_id, 1.5, 0.0).astype(F32)
            put(st, unit - 0.5 * dot6(parts(sz), parts(sy)))
            put(sy, dot6(parts(sy), parts(st)))
            z_next = dot6(parts(st), parts(sz))
            zm[...] = z_next
            put(sz, z_next)
            return carry

        lax.fori_loop(0, NS_STEPS, newton, 0)
        s_mat = zm[...] / jnp.sqrt(scale)
        zm[...] = s_mat
        put(sz, s_mat)
        pa_mat = dot6(parts(sz), parts(sz))
        c_innov = jnp.sum(cif[...], axis=1, keepdims=True)
        w_mean = jnp.sum(pa_mat * c_innov, axis=0, keepdims=True)
        t_mat = math.sqrt(MEMBERS - 1) * zm[...] + w_mean
        put(st, t_mat)
        rest = 1.0 - jnp.sum(t_mat, axis=1, keepdims=True)

        def by_channel(group, carry):
            spot = pl.ds(pl.multiple_of(group * GROUP, GROUP), GROUP)
            for part in range(2):
                piece = buf[OWNERS * chunk + group // SUBS, pl.ds((group % SUBS) * GROUP, GROUP), part * 16:part * 16 + 16]
                moved = dot(perm_ref[...], piece.reshape(256, PATCH)).astype(BF16)
                work[part * 16:part * 16 + 16, spot] = moved.reshape(16, 16, PATCH)
            return carry

        lax.fori_loop(0, MEMBERS // GROUP, by_channel, 0)

        def transform(c, carry):
            states = work[c]
            moved = dot(st[2], states) + dot(st[1], states) + dot(st[0], states)
            work[c] = (moved + rest * xbar[pl.ds(c, 1)]).astype(BF16)
            return carry

        lax.fori_loop(0, CHANS, transform, 0)

        for t in range(1, OWNERS):
            f_copy(chunk, t, 0, MINE).wait_send()

        @pl.when(chunk == 0)
        def _():
            pl.semaphore_wait(ready, OWNERS - 1)

        for t in (2, 1, 3, 0):
            def by_member(index, carry):
                spot = pl.ds(pl.multiple_of(((me + t) % OWNERS) * MINE + index * GROUP, GROUP), GROUP)
                for part in range(2):
                    piece = work[part * 16:part * 16 + 16, spot]
                    moved = dot(perm_ref[...], piece.reshape(256, PATCH)).astype(BF16).reshape(16, 16, PATCH)
                    if t == 0:
                        own_row, own_span = place(chunk, me)
                        xbuf[pl.ds(index * GROUP, GROUP), own_row, part * 16:part * 16 + 16, own_span] = moved
                    else:
                        buf[STAGE + 3 * chunk + t - 1, pl.ds(index * GROUP, GROUP), part * 16:part * 16 + 16] = moved

                        @pl.when((index == SUBS - 1) & leaves(chunk, t))
                        def _():
                            tail_ref = tail_a if t == 2 else tail_b
                            tail_ref[:, part * 16:part * 16 + 16] = moved[GROUP - TAIL:]
                return carry

            lax.fori_loop(0, SUBS, by_member, 0)
            if t:
                r_copy(chunk, t, me).start()

                @pl.when(jnp.logical_not(leaves(chunk, t)))
                def _():
                    last_copy(chunk, t, me).start()
        return carry

    lax.fori_loop(0, CHUNKS, analyse, 0)

    def finish(chunk, carry):
        for t in range(1, OWNERS):
            r_copy(chunk, t, (me + t) % OWNERS).wait_recv()
            r_copy(chunk, t, me).wait_send()

            @pl.when(jnp.logical_not(leaves(chunk, t)))
            def _():
                last_copy(chunk, t, (me + t) % OWNERS).wait_recv()
                last_copy(chunk, t, me).wait_send()
        edge_copy(chunk).wait_send()
        return carry

    lax.fori_loop(0, CHUNKS, finish, 0)

    @pl.when(lat > 0)
    def _():
        send_up.wait_send()

    @pl.when(lat < lat_count - 1)
    def _():
        send_down.wait_send()


def store_kernel(held, out_ref, sems):
    size = MINE // STORES
    copies = [pltpu.make_async_copy(held.at[part * size:part * size + size, 1:ROWS + 1], out_ref.at[part * size:part * size + size], sems.at[part])
              for part in range(STORES)]
    for copy in copies:
        copy.start()
    for copy in copies:
        copy.wait()


def join_kernel(whole, piece_a, piece_b, out_ref, sems):
    me = lax.axis_index('ens')
    copies = []
    for index, (piece, source) in enumerate(((piece_a, (me + 2) % OWNERS), (piece_b, OWNERS - 1 - me))):
        span = pl.ds(pl.multiple_of((source % 2) * PATCH, PATCH), PATCH)
        row = chunk_row(CHUNKS - 1, source // 2)
        copies.append(pltpu.make_async_copy(piece, out_ref.at[MAIN:MINE, row, :, span], sems.at[index]))
    for copy in copies:
        copy.start()
    for copy in copies:
        copy.wait()


def solution(mesh):
    lat_count = mesh.shape['lat']
    dom_count = mesh.shape['dom']

    def local_cycle(ens_block, w_in, w_out, obs_op, obs_val, obs_wt):
        state = jnp.transpose(ens_block, (0, 1, 3, 2))
        vmem = pl.BlockSpec(memory_space=pltpu.VMEM)
        hbm = pl.BlockSpec(memory_space=pl.ANY)
        tail = pltpu.VMEM((TAIL, CHANS, PATCH), BF16)
        held, tail_a, tail_b = pl.pallas_call(
            functools.partial(kernel, lat_count, dom_count),
            out_shape=(pltpu.VMEM((MINE, ROWS + 2, CHANS, COLS), BF16), tail, tail),
            in_specs=[hbm] * 6,
            out_specs=(vmem, vmem, vmem),
            scratch_shapes=[
                pltpu.VMEM((STAGE + 3 * CHUNKS, MINE, CHANS, PATCH), BF16),
                pltpu.VMEM((2 * CHANS, 128), BF16),
                pltpu.VMEM((CHANS, 128), BF16),
                pltpu.VMEM((OBS, CHANS), BF16),
                pltpu.VMEM((128, 2 * CHANS), BF16),
                pltpu.VMEM((8 * OBS, 8 * CHANS), BF16),
                pltpu.VMEM((256, 256), BF16),
                pltpu.VMEM((ROWS, 2, OBS, PATCH), F32),
                pltpu.VMEM((ROWS, 2, OBS, PATCH), F32),
                pltpu.VMEM((CHUNKS, 2, CHANS, 128), BF16),
                pltpu.VMEM((CHUNKS, 2, CHANS, 128), BF16),
                pltpu.VMEM((3 * OBS, MEMBERS, PATCH), BF16),
                pltpu.VMEM((MEMBERS, MEMBERS), F32),
                pltpu.VMEM((MEMBERS, MEMBERS), F32),
                pltpu.VMEM((MEMBERS, MEMBERS), F32),
                pltpu.VMEM((MEMBERS, MEMBERS), F32),
                pltpu.VMEM((3, MEMBERS, MEMBERS), BF16),
                pltpu.VMEM((3, MEMBERS, MEMBERS), BF16),
                pltpu.VMEM((3, MEMBERS, MEMBERS), BF16),
                pltpu.VMEM((CHANS, PATCH), F32),
                pltpu.VMEM((OBS, PATCH), F32),
                pltpu.VMEM((OBS, PATCH), F32),
                pltpu.VMEM((OBS, PATCH), F32),
                pltpu.SemaphoreType.DMA((FIRST // BATCH,)),
                pltpu.SemaphoreType.DMA((4,)),
                pltpu.SemaphoreType.DMA((4,)),
                pltpu.SemaphoreType.DMA((3,)),
                pltpu.SemaphoreType.DMA((2,)),
                pltpu.SemaphoreType.DMA((2,)),
                pltpu.SemaphoreType.DMA((2,)),
                pltpu.SemaphoreType.DMA((CHUNKS,)),
                pltpu.SemaphoreType.DMA((CHUNKS,)),
                pltpu.SemaphoreType.DMA((CHUNKS, 3)),
                pltpu.SemaphoreType.DMA((CHUNKS, OWNERS)),
                pltpu.SemaphoreType.DMA((CHUNKS, 3)),
                pltpu.SemaphoreType.DMA((CHUNKS, OWNERS)),
                pltpu.SemaphoreType.DMA((CHUNKS, 3)),
                pltpu.SemaphoreType.DMA((CHUNKS, OWNERS)),
                pltpu.SemaphoreType.DMA((2,)),
                pltpu.SemaphoreType.REGULAR,
            ],
            compiler_params=pltpu.CompilerParams(collective_id=0, has_side_effects=True, vmem_limit_bytes=43 * 2 ** 20),
        )(w_in, jnp.transpose(w_out), jnp.transpose(obs_op),
          jnp.transpose(obs_val, (0, 1, 3, 2)), jnp.transpose(obs_wt, (0, 1, 3, 2)), state)
        tail_a = lax.ppermute(tail_a, 'ens', [(i, (i + 2) % OWNERS) for i in range(OWNERS)])
        tail_b = lax.ppermute(tail_b, 'ens', [(i, OWNERS - 1 - i) for i in range(OWNERS)])
        result = pl.pallas_call(
            store_kernel,
            out_shape=jax.ShapeDtypeStruct(state.shape, BF16),
            in_specs=[vmem],
            out_specs=hbm,
            scratch_shapes=[pltpu.SemaphoreType.DMA((STORES,))],
            compiler_params=pltpu.CompilerParams(vmem_limit_bytes=2 ** 20),
            cost_estimate=pl.CostEstimate(flops=0, bytes_accessed=2 * state.size, transcendentals=0),
        )(pltpu.with_memory_space_constraint(held, pltpu.VMEM))
        result = pl.pallas_call(
            join_kernel,
            out_shape=jax.ShapeDtypeStruct(state.shape, BF16),
            in_specs=[hbm, vmem, vmem],
            out_specs=hbm,
            scratch_shapes=[pltpu.SemaphoreType.DMA((2,))],
            input_output_aliases={0: 0},
            compiler_params=pltpu.CompilerParams(vmem_limit_bytes=2 ** 20),
        )(result, tail_a, tail_b)
        return jnp.transpose(result, (0, 1, 3, 2))

    state_spec = P('ens', 'lat', 'dom', None)
    obs_spec = P('lat', 'dom', None, None)
    return jax.shard_map(local_cycle, mesh=mesh, in_specs=(state_spec, P(), P(), P(), obs_spec, obs_spec), out_specs=state_spec, check_vma=False)
```

```python
import functools
import math

import jax
import jax.numpy as jnp
from jax import lax
from jax.experimental import pallas as pl
from jax.experimental.pallas import tpu as pltpu
from jax.sharding import PartitionSpec as P

NS_STEPS = 12
MESH = pl.DeviceIdType.MESH
F32 = jnp.float32
BF16 = jnp.bfloat16
MEMBERS = 256
MINE = 64
ROWS = 8
COLS = 512
CHANS = 32
PATCH = 256
OBS = 16
CHUNKS = 4
OWNERS = 4
GROUP = 16
BATCH = 4
PACK = 8
STORES = 8
TAIL = 16
MAIN = MINE - TAIL
LAST_CHUNK = {1: CHUNKS, 2: CHUNKS - 1, 3: CHUNKS}
SUBS = MINE // GROUP
FIRST = 16
INNER = 32
STAGE = CHUNKS * OWNERS


def split3(value):
    high = value.astype(BF16)
    rest = value - high.astype(F32)
    mid = rest.astype(BF16)
    low = (rest - mid.astype(F32)).astype(BF16)
    return high, mid, low


def dot(a, b):
    return jnp.dot(a, b, preferred_element_type=F32)


def dot_t(a, b):
    return lax.dot_general(a, b, (((1,), (1,)), ((), ())), preferred_element_type=F32)


def dot6(a, b):
    small = dot(a[2][...], b[0][...]) + dot(a[0][...], b[2][...]) + dot(a[1][...], b[1][...])
    return small + dot(a[1][...], b[0][...]) + dot(a[0][...], b[1][...]) + dot(a[0][...], b[0][...])


def chunk_row(chunk, which):
    last = chunk // (CHUNKS - 1)
    return (1 - last) * (1 + 2 * chunk + which) + last * (ROWS - 1) * which


def kernel(lat_count, dom_count, w_in_hbm, w_out_hbm, op_hbm, yo_hbm, wt_hbm, x_ref, xbuf, tail_ref,
           buf, w_in_ref, w2_ref, op_ref, w1_ref, bd_ref, perm_ref, yo_ref, wt_ref, edge_out, edge_in, work, am, pm, zm, cif, sy, sz, st, xbar, ybar, sw_ref, sd_ref,
           first_sem, upper_sem, lower_sem, small_sem, halo_send, halo_recv, halo_local, edge_send, edge_recv, f_send, f_recv, r_send, r_recv, last_send, last_recv, obs_sem, ready):
    me = lax.axis_index('ens')
    lat = lax.axis_index('lat')
    dom = lax.axis_index('dom')
    my_row = me // 2
    my_half = me % 2
    lat_up = (lat + lat_count - 1) % lat_count
    lat_down = (lat + 1) % lat_count
    dom_other = (dom + 1) % dom_count

    def first_copy(index):
        some = pl.ds(index * BATCH, BATCH)
        return pltpu.make_async_copy(x_ref.at[some, 0:4], xbuf.at[some, 1:5], first_sem.at[index])

    def block_copies(start, first_row, sems):
        size = (MINE - start) // 4
        return [pltpu.make_async_copy(x_ref.at[start + size * part:start + size * part + size, first_row:first_row + 4],
                                      xbuf.at[start + size * part:start + size * part + size, first_row + 1:first_row + 5],
                                      sems.at[part]) for part in range(4)]

    upper_copies = block_copies(FIRST, 0, upper_sem)
    lower_copies = block_copies(0, 4, lower_sem)
    small_copies = [pltpu.make_async_copy(source, target, small_sem.at[index]) for index, (source, target) in enumerate(
        ((w_in_hbm, w_in_ref), (w_out_hbm, w2_ref), (op_hbm, op_ref)))]
    obs_copies = [pltpu.make_async_copy(yo_hbm, yo_ref, obs_sem.at[0]), pltpu.make_async_copy(wt_hbm, wt_ref, obs_sem.at[1])]
    first_copy(0).start()
    for copy in small_copies:
        copy.start()
    for index in range(1, FIRST // BATCH):
        first_copy(index).start()

    barrier = pltpu.get_barrier_semaphore()
    for t in range(1, OWNERS):
        pl.semaphore_signal(barrier, inc=1, device_id={'ens': (me + t) % OWNERS}, device_id_type=MESH)
    pl.semaphore_signal(barrier, inc=1, device_id={'lat': lat_up}, device_id_type=MESH)
    pl.semaphore_signal(barrier, inc=1, device_id={'lat': lat_down}, device_id_type=MESH)
    pl.semaphore_signal(barrier, inc=1, device_id={'dom': dom_other}, device_id_type=MESH)

    for copy in small_copies:
        copy.wait()
    w1_ref[...] = w_in_ref[...].astype(F32).T.astype(BF16)

    send_up = pltpu.make_async_remote_copy(x_ref.at[:, 0], xbuf.at[:, ROWS + 1], halo_send.at[0], halo_recv.at[1],
                                           device_id={'lat': lat_up}, device_id_type=MESH)
    send_down = pltpu.make_async_remote_copy(x_ref.at[:, ROWS - 1], xbuf.at[:, 0], halo_send.at[1], halo_recv.at[0],
                                             device_id={'lat': lat_down}, device_id_type=MESH)
    top_copy = pltpu.make_async_copy(x_ref.at[:, 0], xbuf.at[:, 0], halo_local.at[0])
    bottom_copy = pltpu.make_async_copy(x_ref.at[:, ROWS - 1], xbuf.at[:, ROWS + 1], halo_local.at[1])

    lane = lax.broadcasted_iota(jnp.int32, (CHANS, 128), 1)

    def edge_copy(chunk):
        return pltpu.make_async_remote_copy(edge_out.at[chunk], edge_in.at[chunk], edge_send.at[chunk], edge_recv.at[chunk],
                                            device_id={'dom': dom_other}, device_id_type=MESH)

    def pack(chunk):
        def members(index, acc):
            first, last = acc
            for offset in range(PACK):
                m = index * PACK + offset
                for which in range(2):
                    row = chunk_row(chunk, which) + 1
                    spot = lane == which * MINE + m
                    west = xbuf[m, row, :, 0:128].astype(F32)
                    east = xbuf[m, row, :, COLS - 128:COLS].astype(F32)
                    first = jnp.where(spot, west[:, 0:1], first)
                    last = jnp.where(spot, east[:, 127:128], last)
            return first, last

        zero = jnp.zeros((CHANS, 128), F32)
        first, last = lax.fori_loop(0, MINE // PACK, members, (zero, zero))
        edge_out[chunk, 0] = first.astype(BF16)
        edge_out[chunk, 1] = last.astype(BF16)
        edge_copy(chunk).start()

    def f_copy(chunk, t, start, size, kind='all'):
        owner = (me + t) % OWNERS
        source = buf.at[STAGE + 3 * chunk + t - 1, pl.ds(start, size)]
        target = buf.at[OWNERS * chunk + me, pl.ds(start, size)]
        if kind != 'all':
            half = owner % 2 if kind == 'outer' else 1 - owner % 2
            span = pl.ds(pl.multiple_of(half * 128, 128), 128)
            source = source.at[:, :, span]
            target = target.at[:, :, span]
        return pltpu.make_async_remote_copy(source, target, f_send.at[chunk, t - 1], f_recv.at[chunk, me],
                                            device_id={'ens': owner}, device_id_type=MESH)

    def slots_of(chunk):
        slots = []
        for owner in range(OWNERS):
            ahead = (owner - me + OWNERS) % OWNERS
            own = 1 - (ahead + OWNERS - 1) // OWNERS
            slots.append(own * (OWNERS * chunk + me) + (1 - own) * (STAGE + 3 * chunk + ahead - 1))
        return slots

    pieces_of = {'all': (PATCH, ((0, 0, 0), (PATCH, 0, 1))),
                 'inner': (128, ((128, 128, 0), (PATCH, 0, 1))),
                 'outer': (128, ((0, 0, 0), (PATCH + 128, 128, 1)))}

    def members(chunk, start, size, kind):
        width, pieces = pieces_of[kind]
        slots = slots_of(chunk)
        if kind != 'inner':
            from_east = edge_in[chunk, 0].astype(F32)
            from_west = edge_in[chunk, 1].astype(F32)
        places, features = [], []
        for m in [start + offset for offset in range(size)]:
            for which in range(2):
                row = chunk_row(chunk, which) + 1
                spot = which * MINE + m
                here = xbuf[m, row]
                mid = here.astype(F32)
                above = xbuf[m, row - 1].astype(F32)
                below = xbuf[m, row + 1].astype(F32)
                west = pltpu.roll(mid, 1, 1)
                east = pltpu.roll(mid, COLS - 1, 1)
                if kind != 'inner':
                    halo_west = pltpu.roll(from_west, (128 - spot) % 128, 1)
                    halo_east = pltpu.roll(from_east, 127 - spot, 1)
                    west = jnp.concatenate([jnp.where(lane == 0, halo_west, west[:, :128]), west[:, 128:]], axis=1)
                    east = jnp.concatenate([east[:, :COLS - 128], jnp.where(lane == 127, halo_east, east[:, COLS - 128:])], axis=1)
                laplace = (above + below + west + east - 4.0 * mid).astype(BF16)
                for column, first_lane, half in pieces:
                    span = slice(column, column + width)
                    features.append(jnp.concatenate([here[:, span], laplace[:, span]], axis=0))
                    places.append((row, m, span, slice(first_lane, first_lane + width), slots[2 * which + half]))
        pre_act = dot(w1_ref[...], jnp.concatenate(features, axis=1))
        hidden = (0.5 * pre_act * (1.0 + lax.erf(pre_act * math.sqrt(0.5)))).astype(BF16)
        update = dot(w2_ref[...], hidden)
        for unit, (row, m, span, lanes, slot) in enumerate(places):
            part = update[:, unit * width:(unit + 1) * width]
            buf[slot, m, :, lanes] = (xbuf[m, row, :, span].astype(F32) + part).astype(BF16)

    def send(chunk, start, size, kind):
        for t in (2, 1, 3):
            f_copy(chunk, t, start, size, kind).start()

    def forecast(chunk, start, stop, kind):
        def step(index, carry):
            if kind == 'inner' and start == BATCH:
                first_copy(index).wait()
            members(chunk, index * BATCH, BATCH, kind)
            send(chunk, index * BATCH, BATCH, kind)
            return carry

        lax.fori_loop(start // BATCH, stop // BATCH, step, 0)

    first_copy(0).wait()
    members(0, 0, BATCH // 2, 'inner')
    pl.semaphore_wait(barrier, OWNERS + 2)
    send(0, 0, BATCH // 2, 'inner')
    for copy in upper_copies:
        copy.start()
    members(0, BATCH // 2, BATCH // 2, 'inner')
    send(0, BATCH // 2, BATCH // 2, 'inner')
    forecast(0, BATCH, FIRST, 'inner')
    for copy in upper_copies:
        copy.wait()
    for copy in lower_copies:
        copy.start()
    for copy in obs_copies:
        copy.start()
    pack(0)

    @pl.when(lat > 0)
    def _():
        send_up.start()

    @pl.when(lat < lat_count - 1)
    def _():
        send_down.start()

    @pl.when(lat == 0)
    def _():
        top_copy.start()

    @pl.when(lat == lat_count - 1)
    def _():
        bottom_copy.start()

    forecast(0, FIRST, INNER, 'inner')
    edge_copy(0).wait_recv()
    forecast(0, 0, INNER, 'outer')
    forecast(0, INNER, MINE, 'all')
    for copy in lower_copies:
        copy.wait()
    pack(1)

    def forecast_chunk(chunk, carry):
        edge_copy(chunk).wait_recv()

        @pl.when((chunk == CHUNKS - 1) & (lat > 0))
        def _():
            send_down.wait_recv()

        @pl.when((chunk == CHUNKS - 1) & (lat == 0))
        def _():
            top_copy.wait()

        @pl.when((chunk == CHUNKS - 1) & (lat < lat_count - 1))
        def _():
            send_up.wait_recv()

        @pl.when((chunk == CHUNKS - 1) & (lat == lat_count - 1))
        def _():
            bottom_copy.wait()

        @pl.when(chunk < CHUNKS - 1)
        def _():
            pack(chunk + 1)

        forecast(chunk, 0, MINE, 'all')
        return carry

    lax.fori_loop(1, CHUNKS, forecast_chunk, 0)

    chan_id = lax.broadcasted_iota(jnp.int32, (CHANS, 8 * CHANS), 0)
    slot_id = lax.broadcasted_iota(jnp.int32, (CHANS, 8 * CHANS), 1)
    repeat = jnp.where(chan_id == slot_id % CHANS, 1.0, 0.0).astype(BF16)
    wide = jnp.broadcast_to(dot(op_ref[...], repeat)[:, None, :], (OBS, 8, 8 * CHANS))
    copy_id = lax.broadcasted_iota(jnp.int32, (OBS, 8, 8 * CHANS), 1)
    place_id = lax.broadcasted_iota(jnp.int32, (OBS, 8, 8 * CHANS), 2)
    bd_ref[...] = jnp.where(copy_id == place_id // CHANS, wide, 0.0).reshape(8 * OBS, 8 * CHANS).astype(BF16)
    row_id = lax.broadcasted_iota(jnp.int32, (MEMBERS, MEMBERS), 0)
    col_id = lax.broadcasted_iota(jnp.int32, (MEMBERS, MEMBERS), 1)
    perm_ref[...] = jnp.where((row_id // 16 == col_id % 16) & (row_id % 16 == col_id // 16), 1.0, 0.0).astype(BF16)
    for t in range(1, OWNERS):
        pl.semaphore_signal(ready, inc=1, device_id={'ens': (me + t) % OWNERS}, device_id_type=MESH)
    for copy in obs_copies:
        copy.wait()

    def place(chunk, owner):
        return chunk_row(chunk, owner // 2) + 1, pl.ds(pl.multiple_of((owner % 2) * PATCH, PATCH), PATCH)

    def r_copy(chunk, t, source):
        row, span = place(chunk, source)
        return pltpu.make_async_remote_copy(
            buf.at[STAGE + 3 * chunk + t - 1, 0:MAIN], xbuf.at[0:MAIN, row, :, span],
            r_send.at[chunk, t - 1], r_recv.at[chunk, source],
            device_id={'ens': (me + t) % OWNERS}, device_id_type=MESH)

    def last_copy(chunk, t, source):
        row, span = place(chunk, source)
        return pltpu.make_async_remote_copy(
            buf.at[STAGE + 3 * chunk + t - 1, MAIN:MINE], xbuf.at[MAIN:MINE, row, :, span],
            last_send.at[chunk, t - 1], last_recv.at[chunk, source],
            device_id={'ens': (me + t) % OWNERS}, device_id_type=MESH)

    def analyse(chunk, carry):
        for t in range(1, OWNERS):
            source = (me + t) % OWNERS
            pltpu.make_async_remote_copy(
                buf.at[STAGE], buf.at[OWNERS * chunk + source], f_send.at[chunk, 0], f_recv.at[chunk, source],
                device_id={'ens': source}, device_id_type=MESH).wait_recv()
        row = chunk_row(chunk, my_row)

        def block(group):
            return buf[OWNERS * chunk + group // SUBS, pl.ds((group % SUBS) * GROUP, GROUP)]

        def sums(group, acc):
            x_sum, y_sum = acc
            states = block(group)
            x_sum = x_sum + jnp.sum(states.astype(F32), axis=0)
            for part in range(2):
                y_sum = y_sum + dot(bd_ref[...], states[part * 8:part * 8 + 8].reshape(8 * CHANS, PATCH))
            return x_sum, y_sum

        x_sum, y_sum = lax.fori_loop(0, MEMBERS // GROUP, sums,
                                     (jnp.zeros((CHANS, PATCH), F32), jnp.zeros((8 * OBS, PATCH), F32)))
        xbar[...] = x_sum * (1.0 / MEMBERS)
        y_mean = jnp.sum(y_sum.reshape(OBS, 8, PATCH), axis=1) * (1.0 / MEMBERS)
        ybar[...] = y_mean
        root_wt = jnp.sqrt(wt_ref[row, my_half])
        sw_ref[...] = root_wt
        sd_ref[...] = root_wt * (yo_ref[row, my_half] - y_mean)

        def anomalies(group, carry):
            states = block(group)
            y_parts = [dot(bd_ref[...], states[part * 8:part * 8 + 8].reshape(8 * CHANS, PATCH)) for part in range(2)]
            spot = pl.ds(pl.multiple_of(group * GROUP, GROUP), GROUP)
            c_innov = jnp.zeros((GROUP, PATCH), F32)
            for o in range(OBS):
                y = jnp.concatenate([y_parts[0][o * 8:o * 8 + 8], y_parts[1][o * 8:o * 8 + 8]], axis=0)
                scaled = (y - ybar[o:o + 1]) * sw_ref[o:o + 1]
                c_innov = c_innov + scaled * sd_ref[o:o + 1]
                high, mid, low = split3(scaled)
                work[o, spot] = high
                work[OBS + o, spot] = mid
                work[2 * OBS + o, spot] = low
            cif[spot] = c_innov
            return carry

        lax.fori_loop(0, MEMBERS // GROUP, anomalies, 0)

        am[...] = jnp.zeros((MEMBERS, MEMBERS), F32)
        pm[...] = jnp.zeros((MEMBERS, MEMBERS), F32)

        def gram(o, carry):
            high = work[o]
            mid = work[OBS + o]
            pm[...] += dot_t(high, mid) + dot_t(high, work[2 * OBS + o])
            am[...] += dot_t(mid, mid) + dot_t(high, high)
            return carry

        lax.fori_loop(0, OBS, gram, 0)
        eye = jnp.where(row_id == col_id, 1.0, 0.0).astype(F32)
        cross = pm[...]
        a_mat = (MEMBERS - 1) * eye + (am[...] + (cross + cross.T))
        scale = jnp.sqrt(jnp.sum(jnp.sum(a_mat * a_mat, axis=0, keepdims=True), axis=1, keepdims=True))

        def put(refs, value):
            for index, part in enumerate(split3(value)):
                refs[index] = part

        def parts(refs):
            return [refs.at[index] for index in range(3)]

        put(sy, a_mat / scale)
        put(sz, eye)

        def newton(step, carry):
            unit = jnp.where(row_id == col_id, 1.5, 0.0).astype(F32)
            put(st, unit - 0.5 * dot6(parts(sz), parts(sy)))
            put(sy, dot6(parts(sy), parts(st)))
            z_next = dot6(parts(st), parts(sz))
            zm[...] = z_next
            put(sz, z_next)
            return carry

        lax.fori_loop(0, NS_STEPS, newton, 0)
        s_mat = zm[...] / jnp.sqrt(scale)
        zm[...] = s_mat
        put(sz, s_mat)
        pa_mat = dot6(parts(sz), parts(sz))
        c_innov = jnp.sum(cif[...], axis=1, keepdims=True)
        w_mean = jnp.sum(pa_mat * c_innov, axis=0, keepdims=True)
        t_mat = math.sqrt(MEMBERS - 1) * zm[...] + w_mean
        put(st, t_mat)
        rest = 1.0 - jnp.sum(t_mat, axis=1, keepdims=True)

        def by_channel(group, carry):
            spot = pl.ds(pl.multiple_of(group * GROUP, GROUP), GROUP)
            for part in range(2):
                piece = buf[OWNERS * chunk + group // SUBS, pl.ds((group % SUBS) * GROUP, GROUP), part * 16:part * 16 + 16]
                moved = dot(perm_ref[...], piece.reshape(256, PATCH)).astype(BF16)
                work[part * 16:part * 16 + 16, spot] = moved.reshape(16, 16, PATCH)
            return carry

        lax.fori_loop(0, MEMBERS // GROUP, by_channel, 0)

        def transform(c, carry):
            states = work[c]
            moved = dot(st[2], states) + dot(st[1], states) + dot(st[0], states)
            work[c] = (moved + rest * xbar[pl.ds(c, 1)]).astype(BF16)
            return carry

        lax.fori_loop(0, CHANS, transform, 0)

        for t in range(1, OWNERS):
            f_copy(chunk, t, 0, MINE).wait_send()

        @pl.when(chunk == 0)
        def _():
            pl.semaphore_wait(ready, OWNERS - 1)

        for t in (2, 1, 3, 0):
            def by_member(index, carry):
                spot = pl.ds(pl.multiple_of(((me + t) % OWNERS) * MINE + index * GROUP, GROUP), GROUP)
                for part in range(2):
                    piece = work[part * 16:part * 16 + 16, spot]
                    moved = dot(perm_ref[...], piece.reshape(256, PATCH)).astype(BF16).reshape(16, 16, PATCH)
                    if t == 0:
                        own_row, own_span = place(chunk, me)
                        xbuf[pl.ds(index * GROUP, GROUP), own_row, part * 16:part * 16 + 16, own_span] = moved
                    else:
                        buf[STAGE + 3 * chunk + t - 1, pl.ds(index * GROUP, GROUP), part * 16:part * 16 + 16] = moved

                        if t == 2:
                            @pl.when((index == SUBS - 1) & (chunk == CHUNKS - 1))
                            def _():
                                tail_ref[:, part * 16:part * 16 + 16] = moved
                return carry

            lax.fori_loop(0, SUBS, by_member, 0)
            if t:
                r_copy(chunk, t, me).start()

                @pl.when(chunk < LAST_CHUNK[t])
                def _():
                    last_copy(chunk, t, me).start()
        return carry

    lax.fori_loop(0, CHUNKS, analyse, 0)

    def finish(chunk, carry):
        for t in range(1, OWNERS):
            r_copy(chunk, t, (me + t) % OWNERS).wait_recv()
            r_copy(chunk, t, me).wait_send()

            @pl.when(chunk < LAST_CHUNK[t])
            def _():
                last_copy(chunk, t, (me + t) % OWNERS).wait_recv()
                last_copy(chunk, t, me).wait_send()
        edge_copy(chunk).wait_send()
        return carry

    lax.fori_loop(0, CHUNKS, finish, 0)

    @pl.when(lat > 0)
    def _():
        send_up.wait_send()

    @pl.when(lat < lat_count - 1)
    def _():
        send_down.wait_send()


def store_kernel(held, out_ref, sems):
    size = MINE // STORES
    copies = [pltpu.make_async_copy(held.at[part * size:part * size + size, 1:ROWS + 1], out_ref.at[part * size:part * size + size], sems.at[part])
              for part in range(STORES)]
    for copy in copies:
        copy.start()
    for copy in copies:
        copy.wait()


def join_kernel(whole, piece, out_ref, sem):
    source = (lax.axis_index('ens') + 2) % OWNERS
    span = pl.ds(pl.multiple_of((source % 2) * PATCH, PATCH), PATCH)
    copy = pltpu.make_async_copy(piece, out_ref.at[MAIN:MINE, chunk_row(CHUNKS - 1, source // 2), :, span], sem)
    copy.start()
    copy.wait()


def solution(mesh):
    lat_count = mesh.shape['lat']
    dom_count = mesh.shape['dom']

    def local_cycle(ens_block, w_in, w_out, obs_op, obs_val, obs_wt):
        state = jnp.transpose(ens_block, (0, 1, 3, 2))
        vmem = pl.BlockSpec(memory_space=pltpu.VMEM)
        hbm = pl.BlockSpec(memory_space=pl.ANY)
        tail = pltpu.VMEM((TAIL, CHANS, PATCH), BF16)
        held, tail_piece = pl.pallas_call(
            functools.partial(kernel, lat_count, dom_count),
            out_shape=(pltpu.VMEM((MINE, ROWS + 2, CHANS, COLS), BF16), tail),
            in_specs=[hbm] * 6,
            out_specs=(vmem, vmem),
            scratch_shapes=[
                pltpu.VMEM((STAGE + 3 * CHUNKS, MINE, CHANS, PATCH), BF16),
                pltpu.VMEM((2 * CHANS, 128), BF16),
                pltpu.VMEM((CHANS, 128), BF16),
                pltpu.VMEM((OBS, CHANS), BF16),
                pltpu.VMEM((128, 2 * CHANS), BF16),
                pltpu.VMEM((8 * OBS, 8 * CHANS), BF16),
                pltpu.VMEM((256, 256), BF16),
                pltpu.VMEM((ROWS, 2, OBS, PATCH), F32),
                pltpu.VMEM((ROWS, 2, OBS, PATCH), F32),
                pltpu.VMEM((CHUNKS, 2, CHANS, 128), BF16),
                pltpu.VMEM((CHUNKS, 2, CHANS, 128), BF16),
                pltpu.VMEM((3 * OBS, MEMBERS, PATCH), BF16),
                pltpu.VMEM((MEMBERS, MEMBERS), F32),
                pltpu.VMEM((MEMBERS, MEMBERS), F32),
                pltpu.VMEM((MEMBERS, MEMBERS), F32),
                pltpu.VMEM((MEMBERS, MEMBERS), F32),
                pltpu.VMEM((3, MEMBERS, MEMBERS), BF16),
                pltpu.VMEM((3, MEMBERS, MEMBERS), BF16),
                pltpu.VMEM((3, MEMBERS, MEMBERS), BF16),
                pltpu.VMEM((CHANS, PATCH), F32),
                pltpu.VMEM((OBS, PATCH), F32),
                pltpu.VMEM((OBS, PATCH), F32),
                pltpu.VMEM((OBS, PATCH), F32),
                pltpu.SemaphoreType.DMA((FIRST // BATCH,)),
                pltpu.SemaphoreType.DMA((4,)),
                pltpu.SemaphoreType.DMA((4,)),
                pltpu.SemaphoreType.DMA((3,)),
                pltpu.SemaphoreType.DMA((2,)),
                pltpu.SemaphoreType.DMA((2,)),
                pltpu.SemaphoreType.DMA((2,)),
                pltpu.SemaphoreType.DMA((CHUNKS,)),
                pltpu.SemaphoreType.DMA((CHUNKS,)),
                pltpu.SemaphoreType.DMA((CHUNKS, 3)),
                pltpu.SemaphoreType.DMA((CHUNKS, OWNERS)),
                pltpu.SemaphoreType.DMA((CHUNKS, 3)),
                pltpu.SemaphoreType.DMA((CHUNKS, OWNERS)),
                pltpu.SemaphoreType.DMA((CHUNKS, 3)),
                pltpu.SemaphoreType.DMA((CHUNKS, OWNERS)),
                pltpu.SemaphoreType.DMA((2,)),
                pltpu.SemaphoreType.REGULAR,
            ],
            compiler_params=pltpu.CompilerParams(collective_id=0, has_side_effects=True, vmem_limit_bytes=43 * 2 ** 20),
        )(w_in, jnp.transpose(w_out), jnp.transpose(obs_op),
          jnp.transpose(obs_val, (0, 1, 3, 2)), jnp.transpose(obs_wt, (0, 1, 3, 2)), state)
        tail_piece = lax.ppermute(tail_piece, 'ens', [(i, (i + 2) % OWNERS) for i in range(OWNERS)])
        result = pl.pallas_call(
            store_kernel,
            out_shape=jax.ShapeDtypeStruct(state.shape, BF16),
            in_specs=[vmem],
            out_specs=hbm,
            scratch_shapes=[pltpu.SemaphoreType.DMA((STORES,))],
            compiler_params=pltpu.CompilerParams(vmem_limit_bytes=2 ** 20),
            cost_estimate=pl.CostEstimate(flops=0, bytes_accessed=2 * state.size, transcendentals=0),
        )(pltpu.with_memory_space_constraint(held, pltpu.VMEM))
        result = pl.pallas_call(
            join_kernel,
            out_shape=jax.ShapeDtypeStruct(state.shape, BF16),
            in_specs=[hbm, vmem],
            out_specs=hbm,
            scratch_shapes=[pltpu.SemaphoreType.DMA],
            input_output_aliases={0: 0},
            compiler_params=pltpu.CompilerParams(vmem_limit_bytes=2 ** 20),
        )(result, tail_piece)
        return jnp.transpose(result, (0, 1, 3, 2))

    state_spec = P('ens', 'lat', 'dom', None)
    obs_spec = P('lat', 'dom', None, None)
    return jax.shard_map(local_cycle, mesh=mesh, in_specs=(state_spec, P(), P(), P(), obs_spec, obs_spec), out_specs=state_spec, check_vma=False)
```

```python
import functools
import math

import jax
import jax.numpy as jnp
from jax import lax
from jax.experimental import pallas as pl
from jax.experimental.pallas import tpu as pltpu
from jax.sharding import PartitionSpec as P

NS_STEPS = 12
MESH = pl.DeviceIdType.MESH
F32 = jnp.float32
BF16 = jnp.bfloat16
MEMBERS = 256
MINE = 64
ROWS = 8
COLS = 512
CHANS = 32
PATCH = 256
OBS = 16
CHUNKS = 4
OWNERS = 4
GROUP = 16
BATCH = 4
PACK = 8
STORES = 8
TAIL = 10
MAIN = MINE - TAIL
SUBS = MINE // GROUP
FIRST = 16
INNER = 32
STAGE = CHUNKS * OWNERS


def split3(value):
    high = value.astype(BF16)
    rest = value - high.astype(F32)
    mid = rest.astype(BF16)
    low = (rest - mid.astype(F32)).astype(BF16)
    return high, mid, low


def dot(a, b):
    return jnp.dot(a, b, preferred_element_type=F32)


def dot_t(a, b):
    return lax.dot_general(a, b, (((1,), (1,)), ((), ())), preferred_element_type=F32)


def dot6(a, b):
    small = dot(a[2][...], b[0][...]) + dot(a[0][...], b[2][...]) + dot(a[1][...], b[1][...])
    return small + dot(a[1][...], b[0][...]) + dot(a[0][...], b[1][...]) + dot(a[0][...], b[0][...])


def chunk_row(chunk, which):
    last = chunk // (CHUNKS - 1)
    return (1 - last) * (1 + 2 * chunk + which) + last * (ROWS - 1) * which


def kernel(lat_count, dom_count, w_in_hbm, w_out_hbm, op_hbm, yo_hbm, wt_hbm, x_ref, xbuf, tail_a, tail_b,
           buf, w_in_ref, w2_ref, op_ref, w1_ref, bd_ref, perm_ref, yo_ref, wt_ref, edge_out, edge_in, work, am, pm, zm, cif, sy, sz, st, xbar, ybar, sw_ref, sd_ref,
           first_sem, upper_sem, lower_sem, small_sem, halo_send, halo_recv, halo_local, edge_send, edge_recv, f_send, f_recv, r_send, r_recv, last_send, last_recv, obs_sem, ready):
    me = lax.axis_index('ens')
    lat = lax.axis_index('lat')
    dom = lax.axis_index('dom')
    my_row = me // 2
    my_half = me % 2
    lat_up = (lat + lat_count - 1) % lat_count
    lat_down = (lat + 1) % lat_count
    dom_other = (dom + 1) % dom_count

    def first_copy(index):
        some = pl.ds(index * BATCH, BATCH)
        return pltpu.make_async_copy(x_ref.at[some, 0:4], xbuf.at[some, 1:5], first_sem.at[index])

    def block_copies(start, first_row, sems):
        size = (MINE - start) // 4
        return [pltpu.make_async_copy(x_ref.at[start + size * part:start + size * part + size, first_row:first_row + 4],
                                      xbuf.at[start + size * part:start + size * part + size, first_row + 1:first_row + 5],
                                      sems.at[part]) for part in range(4)]

    upper_copies = block_copies(FIRST, 0, upper_sem)
    lower_copies = block_copies(0, 4, lower_sem)
    small_copies = [pltpu.make_async_copy(source, target, small_sem.at[index]) for index, (source, target) in enumerate(
        ((w_in_hbm, w_in_ref), (w_out_hbm, w2_ref), (op_hbm, op_ref)))]
    obs_copies = [pltpu.make_async_copy(yo_hbm, yo_ref, obs_sem.at[0]), pltpu.make_async_copy(wt_hbm, wt_ref, obs_sem.at[1])]
    first_copy(0).start()
    for copy in small_copies:
        copy.start()
    for index in range(1, FIRST // BATCH):
        first_copy(index).start()

    barrier = pltpu.get_barrier_semaphore()
    for t in range(1, OWNERS):
        pl.semaphore_signal(barrier, inc=1, device_id={'ens': (me + t) % OWNERS}, device_id_type=MESH)
    pl.semaphore_signal(barrier, inc=1, device_id={'lat': lat_up}, device_id_type=MESH)
    pl.semaphore_signal(barrier, inc=1, device_id={'lat': lat_down}, device_id_type=MESH)
    pl.semaphore_signal(barrier, inc=1, device_id={'dom': dom_other}, device_id_type=MESH)

    for copy in small_copies:
        copy.wait()
    w1_ref[...] = w_in_ref[...].astype(F32).T.astype(BF16)

    send_up = pltpu.make_async_remote_copy(x_ref.at[:, 0], xbuf.at[:, ROWS + 1], halo_send.at[0], halo_recv.at[1],
                                           device_id={'lat': lat_up}, device_id_type=MESH)
    send_down = pltpu.make_async_remote_copy(x_ref.at[:, ROWS - 1], xbuf.at[:, 0], halo_send.at[1], halo_recv.at[0],
                                             device_id={'lat': lat_down}, device_id_type=MESH)
    top_copy = pltpu.make_async_copy(x_ref.at[:, 0], xbuf.at[:, 0], halo_local.at[0])
    bottom_copy = pltpu.make_async_copy(x_ref.at[:, ROWS - 1], xbuf.at[:, ROWS + 1], halo_local.at[1])

    lane = lax.broadcasted_iota(jnp.int32, (CHANS, 128), 1)

    def edge_copy(chunk):
        return pltpu.make_async_remote_copy(edge_out.at[chunk], edge_in.at[chunk], edge_send.at[chunk], edge_recv.at[chunk],
                                            device_id={'dom': dom_other}, device_id_type=MESH)

    def pack(chunk):
        def members(index, acc):
            first, last = acc
            for offset in range(PACK):
                m = index * PACK + offset
                for which in range(2):
                    row = chunk_row(chunk, which) + 1
                    spot = lane == which * MINE + m
                    west = xbuf[m, row, :, 0:128].astype(F32)
                    east = xbuf[m, row, :, COLS - 128:COLS].astype(F32)
                    first = jnp.where(spot, west[:, 0:1], first)
                    last = jnp.where(spot, east[:, 127:128], last)
            return first, last

        zero = jnp.zeros((CHANS, 128), F32)
        first, last = lax.fori_loop(0, MINE // PACK, members, (zero, zero))
        edge_out[chunk, 0] = first.astype(BF16)
        edge_out[chunk, 1] = last.astype(BF16)
        edge_copy(chunk).start()

    def f_copy(chunk, t, start, size, kind='all'):
        owner = (me + t) % OWNERS
        source = buf.at[STAGE + 3 * chunk + t - 1, pl.ds(start, size)]
        target = buf.at[OWNERS * chunk + me, pl.ds(start, size)]
        if kind != 'all':
            half = owner % 2 if kind == 'outer' else 1 - owner % 2
            span = pl.ds(pl.multiple_of(half * 128, 128), 128)
            source = source.at[:, :, span]
            target = target.at[:, :, span]
        return pltpu.make_async_remote_copy(source, target, f_send.at[chunk, t - 1], f_recv.at[chunk, me],
                                            device_id={'ens': owner}, device_id_type=MESH)

    def slots_of(chunk):
        slots = []
        for owner in range(OWNERS):
            ahead = (owner - me + OWNERS) % OWNERS
            own = 1 - (ahead + OWNERS - 1) // OWNERS
            slots.append(own * (OWNERS * chunk + me) + (1 - own) * (STAGE + 3 * chunk + ahead - 1))
        return slots

    pieces_of = {'all': (PATCH, ((0, 0, 0), (PATCH, 0, 1))),
                 'inner': (128, ((128, 128, 0), (PATCH, 0, 1))),
                 'outer': (128, ((0, 0, 0), (PATCH + 128, 128, 1)))}

    def members(chunk, start, size, kind):
        width, pieces = pieces_of[kind]
        slots = slots_of(chunk)
        if kind != 'inner':
            from_east = edge_in[chunk, 0].astype(F32)
            from_west = edge_in[chunk, 1].astype(F32)
        places, features = [], []
        for m in [start + offset for offset in range(size)]:
            for which in range(2):
                row = chunk_row(chunk, which) + 1
                spot = which * MINE + m
                here = xbuf[m, row]
                mid = here.astype(F32)
                above = xbuf[m, row - 1].astype(F32)
                below = xbuf[m, row + 1].astype(F32)
                west = pltpu.roll(mid, 1, 1)
                east = pltpu.roll(mid, COLS - 1, 1)
                if kind != 'inner':
                    halo_west = pltpu.roll(from_west, (128 - spot) % 128, 1)
                    halo_east = pltpu.roll(from_east, 127 - spot, 1)
                    west = jnp.concatenate([jnp.where(lane == 0, halo_west, west[:, :128]), west[:, 128:]], axis=1)
                    east = jnp.concatenate([east[:, :COLS - 128], jnp.where(lane == 127, halo_east, east[:, COLS - 128:])], axis=1)
                laplace = (above + below + west + east - 4.0 * mid).astype(BF16)
                for column, first_lane, half in pieces:
                    span = slice(column, column + width)
                    features.append(jnp.concatenate([here[:, span], laplace[:, span]], axis=0))
                    places.append((row, m, span, slice(first_lane, first_lane + width), slots[2 * which + half]))
        pre_act = dot(w1_ref[...], jnp.concatenate(features, axis=1))
        hidden = (0.5 * pre_act * (1.0 + lax.erf(pre_act * math.sqrt(0.5)))).astype(BF16)
        update = dot(w2_ref[...], hidden)
        for unit, (row, m, span, lanes, slot) in enumerate(places):
            part = update[:, unit * width:(unit + 1) * width]
            buf[slot, m, :, lanes] = (xbuf[m, row, :, span].astype(F32) + part).astype(BF16)

    def send(chunk, start, size, kind):
        for t in (2, 1, 3):
            f_copy(chunk, t, start, size, kind).start()

    def forecast(chunk, start, stop, kind, whole=False):
        def step(index, carry):
            if kind == 'inner' and start == BATCH:
                first_copy(index).wait()
            members(chunk, index * BATCH, BATCH, kind)
            if not whole:
                send(chunk, index * BATCH, BATCH, kind)
            return carry

        lax.fori_loop(start // BATCH, stop // BATCH, step, 0)
        if whole:
            send(chunk, start, stop - start, kind)

    first_copy(0).wait()
    members(0, 0, BATCH // 2, 'inner')
    pl.semaphore_wait(barrier, OWNERS + 2)
    send(0, 0, BATCH // 2, 'inner')
    for copy in upper_copies:
        copy.start()
    members(0, BATCH // 2, BATCH // 2, 'inner')
    send(0, BATCH // 2, BATCH // 2, 'inner')
    forecast(0, BATCH, FIRST, 'inner')
    for copy in upper_copies:
        copy.wait()
    for copy in lower_copies:
        copy.start()
    for copy in obs_copies:
        copy.start()
    pack(0)

    @pl.when(lat > 0)
    def _():
        send_up.start()

    @pl.when(lat < lat_count - 1)
    def _():
        send_down.start()

    @pl.when(lat == 0)
    def _():
        top_copy.start()

    @pl.when(lat == lat_count - 1)
    def _():
        bottom_copy.start()

    forecast(0, FIRST, INNER, 'inner')
    edge_copy(0).wait_recv()
    forecast(0, 0, INNER, 'outer')
    forecast(0, INNER, MINE, 'all')
    for copy in lower_copies:
        copy.wait()
    pack(1)

    def forecast_chunk(chunk, carry):
        edge_copy(chunk).wait_recv()

        @pl.when((chunk == CHUNKS - 1) & (lat > 0))
        def _():
            send_down.wait_recv()

        @pl.when((chunk == CHUNKS - 1) & (lat == 0))
        def _():
            top_copy.wait()

        @pl.when((chunk == CHUNKS - 1) & (lat < lat_count - 1))
        def _():
            send_up.wait_recv()

        @pl.when((chunk == CHUNKS - 1) & (lat == lat_count - 1))
        def _():
            bottom_copy.wait()

        @pl.when(chunk < CHUNKS - 1)
        def _():
            pack(chunk + 1)

        forecast(chunk, 0, MINE, 'all', whole=True)
        return carry

    lax.fori_loop(1, CHUNKS, forecast_chunk, 0)

    chan_id = lax.broadcasted_iota(jnp.int32, (CHANS, 8 * CHANS), 0)
    slot_id = lax.broadcasted_iota(jnp.int32, (CHANS, 8 * CHANS), 1)
    repeat = jnp.where(chan_id == slot_id % CHANS, 1.0, 0.0).astype(BF16)
    wide = jnp.broadcast_to(dot(op_ref[...], repeat)[:, None, :], (OBS, 8, 8 * CHANS))
    copy_id = lax.broadcasted_iota(jnp.int32, (OBS, 8, 8 * CHANS), 1)
    place_id = lax.broadcasted_iota(jnp.int32, (OBS, 8, 8 * CHANS), 2)
    bd_ref[...] = jnp.where(copy_id == place_id // CHANS, wide, 0.0).reshape(8 * OBS, 8 * CHANS).astype(BF16)
    row_id = lax.broadcasted_iota(jnp.int32, (MEMBERS, MEMBERS), 0)
    col_id = lax.broadcasted_iota(jnp.int32, (MEMBERS, MEMBERS), 1)
    perm_ref[...] = jnp.where((row_id // 16 == col_id % 16) & (row_id % 16 == col_id // 16), 1.0, 0.0).astype(BF16)
    for t in range(1, OWNERS):
        pl.semaphore_signal(ready, inc=1, device_id={'ens': (me + t) % OWNERS}, device_id_type=MESH)
    for copy in obs_copies:
        copy.wait()

    def place(chunk, owner):
        return chunk_row(chunk, owner // 2) + 1, pl.ds(pl.multiple_of((owner % 2) * PATCH, PATCH), PATCH)

    def r_copy(chunk, t, source):
        row, span = place(chunk, source)
        return pltpu.make_async_remote_copy(
            buf.at[STAGE + 3 * chunk + t - 1, 0:MAIN], xbuf.at[0:MAIN, row, :, span],
            r_send.at[chunk, t - 1], r_recv.at[chunk, source],
            device_id={'ens': (me + t) % OWNERS}, device_id_type=MESH)

    def last_copy(chunk, t, source):
        row, span = place(chunk, source)
        return pltpu.make_async_remote_copy(
            buf.at[STAGE + 3 * chunk + t - 1, MAIN:MINE], xbuf.at[MAIN:MINE, row, :, span],
            last_send.at[chunk, t - 1], last_recv.at[chunk, source],
            device_id={'ens': (me + t) % OWNERS}, device_id_type=MESH)

    def leaves(chunk, t):
        crosses = {1: me % 2, 2: 1, 3: 1 - me % 2}[t]
        return (chunk // (CHUNKS - 1)) * crosses == 1

    def analyse(chunk, carry):
        for t in range(1, OWNERS):
            source = (me + t) % OWNERS
            pltpu.make_async_remote_copy(
                buf.at[STAGE], buf.at[OWNERS * chunk + source], f_send.at[chunk, 0], f_recv.at[chunk, source],
                device_id={'ens': source}, device_id_type=MESH).wait_recv()
        row = chunk_row(chunk, my_row)

        def block(group):
            return buf[OWNERS * chunk + group // SUBS, pl.ds((group % SUBS) * GROUP, GROUP)]

        def sums(group, acc):
            x_sum, y_sum = acc
            states = block(group)
            x_sum = x_sum + jnp.sum(states.astype(F32), axis=0)
            for part in range(2):
                y_sum = y_sum + dot(bd_ref[...], states[part * 8:part * 8 + 8].reshape(8 * CHANS, PATCH))
            return x_sum, y_sum

        x_sum, y_sum = lax.fori_loop(0, MEMBERS // GROUP, sums,
                                     (jnp.zeros((CHANS, PATCH), F32), jnp.zeros((8 * OBS, PATCH), F32)))
        xbar[...] = x_sum * (1.0 / MEMBERS)
        y_mean = jnp.sum(y_sum.reshape(OBS, 8, PATCH), axis=1) * (1.0 / MEMBERS)
        ybar[...] = y_mean
        root_wt = jnp.sqrt(wt_ref[row, my_half])
        sw_ref[...] = root_wt
        sd_ref[...] = root_wt * (yo_ref[row, my_half] - y_mean)

        def anomalies(group, carry):
            states = block(group)
            y_parts = [dot(bd_ref[...], states[part * 8:part * 8 + 8].reshape(8 * CHANS, PATCH)) for part in range(2)]
            spot = pl.ds(pl.multiple_of(group * GROUP, GROUP), GROUP)
            c_innov = jnp.zeros((GROUP, PATCH), F32)
            for o in range(OBS):
                y = jnp.concatenate([y_parts[0][o * 8:o * 8 + 8], y_parts[1][o * 8:o * 8 + 8]], axis=0)
                scaled = (y - ybar[o:o + 1]) * sw_ref[o:o + 1]
                c_innov = c_innov + scaled * sd_ref[o:o + 1]
                high, mid, low = split3(scaled)
                work[o, spot] = high
                work[OBS + o, spot] = mid
                work[2 * OBS + o, spot] = low
            cif[spot] = c_innov
            return carry

        lax.fori_loop(0, MEMBERS // GROUP, anomalies, 0)

        am[...] = jnp.zeros((MEMBERS, MEMBERS), F32)
        pm[...] = jnp.zeros((MEMBERS, MEMBERS), F32)

        def gram(o, carry):
            high = work[o]
            mid = work[OBS + o]
            pm[...] += dot_t(high, mid) + dot_t(high, work[2 * OBS + o])
            am[...] += dot_t(mid, mid) + dot_t(high, high)
            return carry

        lax.fori_loop(0, OBS, gram, 0)
        eye = jnp.where(row_id == col_id, 1.0, 0.0).astype(F32)
        cross = pm[...]
        a_mat = (MEMBERS - 1) * eye + (am[...] + (cross + cross.T))
        scale = jnp.sqrt(jnp.sum(jnp.sum(a_mat * a_mat, axis=0, keepdims=True), axis=1, keepdims=True))

        def put(refs, value):
            for index, part in enumerate(split3(value)):
                refs[index] = part

        def parts(refs):
            return [refs.at[index] for index in range(3)]

        put(sy, a_mat / scale)
        put(sz, eye)

        def newton(step, carry):
            unit = jnp.where(row_id == col_id, 1.5, 0.0).astype(F32)
            put(st, unit - 0.5 * dot6(parts(sz), parts(sy)))
            put(sy, dot6(parts(sy), parts(st)))
            z_next = dot6(parts(st), parts(sz))
            zm[...] = z_next
            put(sz, z_next)
            return carry

        lax.fori_loop(0, NS_STEPS, newton, 0)
        s_mat = zm[...] / jnp.sqrt(scale)
        zm[...] = s_mat
        put(sz, s_mat)
        pa_mat = dot6(parts(sz), parts(sz))
        c_innov = jnp.sum(cif[...], axis=1, keepdims=True)
        w_mean = jnp.sum(pa_mat * c_innov, axis=0, keepdims=True)
        t_mat = math.sqrt(MEMBERS - 1) * zm[...] + w_mean
        put(st, t_mat)
        rest = 1.0 - jnp.sum(t_mat, axis=1, keepdims=True)

        def by_channel(group, carry):
            spot = pl.ds(pl.multiple_of(group * GROUP, GROUP), GROUP)
            for part in range(2):
                piece = buf[OWNERS * chunk + group // SUBS, pl.ds((group % SUBS) * GROUP, GROUP), part * 16:part * 16 + 16]
                moved = dot(perm_ref[...], piece.reshape(256, PATCH)).astype(BF16)
                work[part * 16:part * 16 + 16, spot] = moved.reshape(16, 16, PATCH)
            return carry

        lax.fori_loop(0, MEMBERS // GROUP, by_channel, 0)

        def transform(c, carry):
            states = work[c]
            moved = dot(st[2], states) + dot(st[1], states) + dot(st[0], states)
            work[c] = (moved + rest * xbar[pl.ds(c, 1)]).astype(BF16)
            return carry

        lax.fori_loop(0, CHANS, transform, 0)

        for t in range(1, OWNERS):
            f_copy(chunk, t, 0, MINE).wait_send()

        @pl.when(chunk == 0)
        def _():
            pl.semaphore_wait(ready, OWNERS - 1)

        for t in (2, 1, 3, 0):
            def by_member(index, carry):
                spot = pl.ds(pl.multiple_of(((me + t) % OWNERS) * MINE + index * GROUP, GROUP), GROUP)
                for part in range(2):
                    piece = work[part * 16:part * 16 + 16, spot]
                    moved = dot(perm_ref[...], piece.reshape(256, PATCH)).astype(BF16).reshape(16, 16, PATCH)
                    if t == 0:
                        own_row, own_span = place(chunk, me)
                        xbuf[pl.ds(index * GROUP, GROUP), own_row, part * 16:part * 16 + 16, own_span] = moved
                    else:
                        buf[STAGE + 3 * chunk + t - 1, pl.ds(index * GROUP, GROUP), part * 16:part * 16 + 16] = moved

                        @pl.when((index == SUBS - 1) & leaves(chunk, t))
                        def _():
                            tail_ref = tail_a if t == 2 else tail_b
                            tail_ref[:, part * 16:part * 16 + 16] = moved[GROUP - TAIL:]
                return carry

            lax.fori_loop(0, SUBS, by_member, 0)
            if t:
                r_copy(chunk, t, me).start()

                @pl.when(jnp.logical_not(leaves(chunk, t)))
                def _():
                    last_copy(chunk, t, me).start()
        return carry

    lax.fori_loop(0, CHUNKS, analyse, 0)

    def finish(chunk, carry):
        for t in range(1, OWNERS):
            r_copy(chunk, t, (me + t) % OWNERS).wait_recv()
            r_copy(chunk, t, me).wait_send()

            @pl.when(jnp.logical_not(leaves(chunk, t)))
            def _():
                last_copy(chunk, t, (me + t) % OWNERS).wait_recv()
                last_copy(chunk, t, me).wait_send()
        edge_copy(chunk).wait_send()
        return carry

    lax.fori_loop(0, CHUNKS, finish, 0)

    @pl.when(lat > 0)
    def _():
        send_up.wait_send()

    @pl.when(lat < lat_count - 1)
    def _():
        send_down.wait_send()


def store_kernel(held, out_ref, sems):
    size = MINE // STORES
    copies = [pltpu.make_async_copy(held.at[part * size:part * size + size, 1:ROWS + 1], out_ref.at[part * size:part * size + size], sems.at[part])
              for part in range(STORES)]
    for copy in copies:
        copy.start()
    for copy in copies:
        copy.wait()


def join_kernel(whole, piece_a, piece_b, out_ref, sems):
    me = lax.axis_index('ens')
    copies = []
    for index, (piece, source) in enumerate(((piece_a, (me + 2) % OWNERS), (piece_b, OWNERS - 1 - me))):
        span = pl.ds(pl.multiple_of((source % 2) * PATCH, PATCH), PATCH)
        row = chunk_row(CHUNKS - 1, source // 2)
        copies.append(pltpu.make_async_copy(piece, out_ref.at[MAIN:MINE, row, :, span], sems.at[index]))
    for copy in copies:
        copy.start()
    for copy in copies:
        copy.wait()


def solution(mesh):
    lat_count = mesh.shape['lat']
    dom_count = mesh.shape['dom']

    def local_cycle(ens_block, w_in, w_out, obs_op, obs_val, obs_wt):
        state = jnp.transpose(ens_block, (0, 1, 3, 2))
        vmem = pl.BlockSpec(memory_space=pltpu.VMEM)
        hbm = pl.BlockSpec(memory_space=pl.ANY)
        tail = pltpu.VMEM((TAIL, CHANS, PATCH), BF16)
        held, tail_a, tail_b = pl.pallas_call(
            functools.partial(kernel, lat_count, dom_count),
            out_shape=(pltpu.VMEM((MINE, ROWS + 2, CHANS, COLS), BF16), tail, tail),
            in_specs=[hbm] * 6,
            out_specs=(vmem, vmem, vmem),
            scratch_shapes=[
                pltpu.VMEM((STAGE + 3 * CHUNKS, MINE, CHANS, PATCH), BF16),
                pltpu.VMEM((2 * CHANS, 128), BF16),
                pltpu.VMEM((CHANS, 128), BF16),
                pltpu.VMEM((OBS, CHANS), BF16),
                pltpu.VMEM((128, 2 * CHANS), BF16),
                pltpu.VMEM((8 * OBS, 8 * CHANS), BF16),
                pltpu.VMEM((256, 256), BF16),
                pltpu.VMEM((ROWS, 2, OBS, PATCH), F32),
                pltpu.VMEM((ROWS, 2, OBS, PATCH), F32),
                pltpu.VMEM((CHUNKS, 2, CHANS, 128), BF16),
                pltpu.VMEM((CHUNKS, 2, CHANS, 128), BF16),
                pltpu.VMEM((3 * OBS, MEMBERS, PATCH), BF16),
                pltpu.VMEM((MEMBERS, MEMBERS), F32),
                pltpu.VMEM((MEMBERS, MEMBERS), F32),
                pltpu.VMEM((MEMBERS, MEMBERS), F32),
                pltpu.VMEM((MEMBERS, MEMBERS), F32),
                pltpu.VMEM((3, MEMBERS, MEMBERS), BF16),
                pltpu.VMEM((3, MEMBERS, MEMBERS), BF16),
                pltpu.VMEM((3, MEMBERS, MEMBERS), BF16),
                pltpu.VMEM((CHANS, PATCH), F32),
                pltpu.VMEM((OBS, PATCH), F32),
                pltpu.VMEM((OBS, PATCH), F32),
                pltpu.VMEM((OBS, PATCH), F32),
                pltpu.SemaphoreType.DMA((FIRST // BATCH,)),
                pltpu.SemaphoreType.DMA((4,)),
                pltpu.SemaphoreType.DMA((4,)),
                pltpu.SemaphoreType.DMA((3,)),
                pltpu.SemaphoreType.DMA((2,)),
                pltpu.SemaphoreType.DMA((2,)),
                pltpu.SemaphoreType.DMA((2,)),
                pltpu.SemaphoreType.DMA((CHUNKS,)),
                pltpu.SemaphoreType.DMA((CHUNKS,)),
                pltpu.SemaphoreType.DMA((CHUNKS, 3)),
                pltpu.SemaphoreType.DMA((CHUNKS, OWNERS)),
                pltpu.SemaphoreType.DMA((CHUNKS, 3)),
                pltpu.SemaphoreType.DMA((CHUNKS, OWNERS)),
                pltpu.SemaphoreType.DMA((CHUNKS, 3)),
                pltpu.SemaphoreType.DMA((CHUNKS, OWNERS)),
                pltpu.SemaphoreType.DMA((2,)),
                pltpu.SemaphoreType.REGULAR,
            ],
            compiler_params=pltpu.CompilerParams(collective_id=0, has_side_effects=True, vmem_limit_bytes=43 * 2 ** 20),
        )(w_in, jnp.transpose(w_out), jnp.transpose(obs_op),
          jnp.transpose(obs_val, (0, 1, 3, 2)), jnp.transpose(obs_wt, (0, 1, 3, 2)), state)
        tail_a = lax.ppermute(tail_a, 'ens', [(i, (i + 2) % OWNERS) for i in range(OWNERS)])
        tail_b = lax.ppermute(tail_b, 'ens', [(i, OWNERS - 1 - i) for i in range(OWNERS)])
        result = pl.pallas_call(
            store_kernel,
            out_shape=jax.ShapeDtypeStruct(state.shape, BF16),
            in_specs=[vmem],
            out_specs=hbm,
            scratch_shapes=[pltpu.SemaphoreType.DMA((STORES,))],
            compiler_params=pltpu.CompilerParams(vmem_limit_bytes=2 ** 20),
            cost_estimate=pl.CostEstimate(flops=0, bytes_accessed=2 * state.size, transcendentals=0),
        )(pltpu.with_memory_space_constraint(held, pltpu.VMEM))
        result = pl.pallas_call(
            join_kernel,
            out_shape=jax.ShapeDtypeStruct(state.shape, BF16),
            in_specs=[hbm, vmem, vmem],
            out_specs=hbm,
            scratch_shapes=[pltpu.SemaphoreType.DMA((2,))],
            input_output_aliases={0: 0},
            compiler_params=pltpu.CompilerParams(vmem_limit_bytes=2 ** 20),
        )(result, tail_a, tail_b)
        return jnp.transpose(result, (0, 1, 3, 2))

    state_spec = P('ens', 'lat', 'dom', None)
    obs_spec = P('lat', 'dom', None, None)
    return jax.shard_map(local_cycle, mesh=mesh, in_specs=(state_spec, P(), P(), P(), obs_spec, obs_spec), out_specs=state_spec, check_vma=False)
```
